32 devices in a mesh: rep: 8 (over z, core), shard: 4 (over y, x).
Axes of the slice: x: 2, y: 2, z: 4, core: 2. Of those that a mesh axis runs over, the one named last changes fastest.
Arguments:
- block_in: bfloat16 [4096, 2048], P(('rep', 'shard')), may hold values from -6 to 6
- segments: int32 [4096], P('rep'), may hold values from 0 to 15, never falling along the last dimension, each value on 1 to 512 neighbouring positions
- routes: int32 [4096, 8], P(('rep', 'shard')), may hold values from 0 to 31, all different within a row; in each aligned block of 128 rows (0 to 127, 128 to 255, ...) at most 64 rows name the same one
- attn_gain: float32 [2048], replicated, may hold values from 0.25 to 1.75
- query_key_value_weight: bfloat16 [2048, 5120], P('shard'), may hold values from -0.125 to 0.125
- q_gain: float32 [128], replicated, may hold values from 0.25 to 1.75
- k_gain: float32 [128], replicated, may hold values from 0.25 to 1.75
- w_out: bfloat16 [4096, 2048], P('shard'), may hold values from -1.5 to 1.5
- ffn_gain: float32 [2048], replicated, may hold values from 0.25 to 1.75
- router: bfloat16 [2048, 32], replicated, may hold values from -0.09375 to 0.09375
- expert_weights: bfloat16 [32, 3, 2048, 768], P(('rep', 'shard')), may hold values from -0.125 to 0.125
- cotangent: bfloat16 [4096, 2048], P(('rep', 'shard')), may hold values from -6 to 6
Outputs:
- block_out: bfloat16 [4096, 2048], P(('rep', 'shard'))
- grad_input: bfloat16 [4096, 2048], P(('rep', 'shard'))
- grad_attn_gain: float32 [2048], replicated
- grad_qkv: float32 [2048, 5120], P('shard')
- grad_q_gain: float32 [128], replicated
- grad_k_gain: float32 [128], replicated
- grad_out: float32 [4096, 2048], P('shard')
- grad_ffn_gain: float32 [2048], replicated
- grad_router: float32 [2048, 32], replicated
- grad_experts: float32 [32, 3, 2048, 768], P(('rep', 'shard'))
The draws below stay inside these ranges and needn't reach their ends.
Inputs may be any that keep to these rules, and one draw needn't show every extreme that they name: `segments`: document numbers never fall along the tokens; a document has 1 to 512 tokens and one has exactly 512. `routes`: each row names 8 different experts; among the 128 rows of one device no expert is named more than 64 times, and in every draw some device names some expert exactly 64 times.
All inputs are finite; a program needn't handle non-finite values.
Results may differ from the reference program's by a relative error of at most 0.02.
Values may be sent and summed in bfloat16 or wider, within the bound.
A program may use at most 384 MiB of HBM per device.

```python
import math
import jax
import jax.numpy as jnp
import numpy as np
from jax import lax

MODEL_WIDTH = 2048
QUERY_HEADS = 32
KEY_VALUE_HEADS = 4
HEAD_SIZE = 128
FF = 768
TOP = 8
TOK_DEV = 128
EXPERTS = 32
SEQ = 512
TOKENS = 4096
CAP = 64
DOCS = 16
N_SHARD = 4


def levels(stream_key, extent, cuts, least, top_value):
    def one(dim, shards_of):
        draws = jax.random.uniform(jax.random.fold_in(jax.random.fold_in(stream_key, 6), dim), (shards_of,), jnp.float32, least / len(cuts), top_value / len(cuts))
        return jnp.repeat(jnp.exp(draws), extent[dim] // shards_of).reshape((-1,) + (1,) * (len(extent) - dim - 1))

    factor_of = one(*cuts[0])
    for cut in cuts[1:]:
        factor_of = factor_of * one(*cut)
    return factor_of


def length_profile(number_of, total, bound, slope):
    portions = [(1 << 20) // math.isqrt(standing ** slope) + 1 for standing in range(2, number_of + 1)]
    surplus, given = total - bound - (number_of - 1), [1] * (number_of - 1)
    while surplus > 0:
        movable = [i for i in range(number_of - 1) if given[i] < bound]
        pool, remaining = sum([portions[i] for i in movable]), surplus
        for i in movable:
            extra = min(bound - given[i], max(1, remaining * portions[i] // pool), surplus)
            given[i] = given[i] + extra
            surplus = surplus - extra
    return np.array([bound] + given)


def uneven(rng, number_of, total, reach, lean):
    if number_of == 2:
        one = jax.random.randint(rng, (), max(1, total - reach), min(reach, total - 1) + 1)
        return jnp.stack([one, total - one])
    sizes = jnp.asarray(length_profile(number_of, total, reach, lean), jnp.int32)
    couples = (number_of - 1) // 2
    donor, sink = sizes[1:1 + 2 * couples:2], sizes[2:2 + 2 * couples:2]
    slack = jnp.minimum(donor - 1, reach - sink)
    passed = jax.random.randint(jax.random.fold_in(rng, 1), (couples,), 0, 1 << 20) % (slack + 1)
    sizes = sizes.at[1:1 + 2 * couples:2].set(donor - passed).at[2:2 + 2 * couples:2].set(sink + passed)
    return sizes[jax.random.permutation(jax.random.fold_in(rng, 2), number_of)]


def routed_block(stream_key, own, number, rows, number_of, top, most, skew):
    ranking = jax.random.permutation(stream_key, number_of)
    packed, common = shares(number_of, rows * top, most, skew, True), shares(number_of, rows * top, most, skew, False)
    places = jnp.arange(number_of)

    def named(sizes, offset_by):
        used = int((sizes > 0).sum())
        fixed = max(1, used // 4)
        shifted = fixed + (places - fixed + offset_by * (used - fixed)) % max(1, number_of - fixed)
        return jnp.zeros((number_of,), jnp.int32).at[ranking[jnp.where(places < fixed, places, shifted)]].set(jnp.asarray(sizes, jnp.int32))

    sizes = jnp.where(number % 4 == 0, named(packed, number // 4), named(common, number - number // 4 - 1))
    mixed = jax.random.permutation(jax.random.fold_in(own, 3), number_of)
    giver, taker = mixed[0:number_of // 2 * 2:2], mixed[1:number_of // 2 * 2:2]
    slack = jnp.minimum(sizes[giver] - 1, most - sizes[taker]) // 2
    slack = jnp.where((giver == ranking[0]) | (taker == ranking[0]) | (sizes[taker] == 0), 0, jnp.maximum(slack, 0))
    shifted = jax.random.randint(jax.random.fold_in(own, 4), (number_of // 2,), 0, 1 << 20) % (slack + 1)
    sizes = sizes.at[giver].add(-shifted).at[taker].add(shifted)
    labels = jnp.searchsorted(jnp.cumsum(sizes), jnp.arange(rows * top), side="right").astype(jnp.int32)
    table = labels.reshape(top, rows).T
    table = table[jax.random.permutation(jax.random.fold_in(own, 1), rows)]
    offset_by = jax.random.randint(jax.random.fold_in(own, 2), (rows, 1), 0, top)
    return jnp.take_along_axis(table, (jnp.arange(top)[None, :] + offset_by) % top, axis=1)


def shares(amount, total, bound, slope, full):
    weights = [(1 << 20) // math.isqrt(rank ** slope) + 1 for rank in range(1, amount + 1)]
    largest = bound if full else min(bound, max(-(-total // amount), total * weights[0] // sum(weights)))
    least = 1 if total - largest >= amount - 1 else 0
    holding, rest = [largest] + [least] * (amount - 1), total - largest - least * (amount - 1)
    while rest > 0:
        candidates = [i for i in range(1, amount) if holding[i] < largest] or [i for i in range(1, amount) if holding[i] < bound]
        whole, left = sum([weights[i] for i in candidates]), rest
        for i in candidates:
            more = min(bound - holding[i], max(1, left * weights[i] // whole), rest)
            holding[i] = holding[i] + more
            rest = rest - more
    return np.array(holding)


def normal_values(key, dims, spread, reach, cuts=(), kind=jnp.bfloat16):
    drawn = spread * jax.random.normal(key, dims, jnp.float32)
    if cuts:
        drawn = drawn * levels(key, dims, cuts, -0.22, 0.18)
    return jnp.clip(drawn, -reach, reach).astype(kind)


def setup_inputs(seed: int = 0) -> dict:
    key_list = jax.random.split(jax.random.key(seed), 13)
    block_in = normal_values(key_list[0], (TOKENS, MODEL_WIDTH), 1.0, 6.0, ((0, 32),))
    segments = jnp.searchsorted(jnp.cumsum(uneven(key_list[1], DOCS, TOKENS, SEQ, 2)), jnp.arange(TOKENS), side="right").astype(jnp.int32)
    routes_keys = jax.random.split(jax.random.fold_in(key_list[2], 1), TOKENS // TOK_DEV)
    routes_turns = jax.random.permutation(jax.random.fold_in(key_list[2], 3), TOKENS // TOK_DEV)
    routes = jax.vmap(lambda own, number: routed_block(jax.random.fold_in(key_list[2], 2), own, number, TOK_DEV, EXPERTS, TOP, CAP, 2))(routes_keys, routes_turns).reshape((TOKENS, TOP))
    attn_gain = jnp.clip(1.0 + 0.15 * jax.random.normal(key_list[3], (MODEL_WIDTH,), jnp.float32), 0.25, 1.75)
    query_key_value_weight = normal_values(key_list[4], (MODEL_WIDTH, (QUERY_HEADS + 2 * KEY_VALUE_HEADS) * HEAD_SIZE), MODEL_WIDTH ** -0.5, 0.125, ((0, 4),))
    q_gain = jnp.clip(1.0 + 0.15 * jax.random.normal(key_list[5], (HEAD_SIZE,), jnp.float32), 0.25, 1.75)
    k_gain = jnp.clip(1.0 + 0.15 * jax.random.normal(key_list[6], (HEAD_SIZE,), jnp.float32), 0.25, 1.75)
    w_out = normal_values(key_list[7], (QUERY_HEADS * HEAD_SIZE, MODEL_WIDTH), (max(QUERY_HEADS * HEAD_SIZE // 256, 1)) ** -0.5, 1.5, ((0, 4),))
    ffn_gain = jnp.clip(1.0 + 0.15 * jax.random.normal(key_list[8], (MODEL_WIDTH,), jnp.float32), 0.25, 1.75)
    router = normal_values(key_list[9], (MODEL_WIDTH, EXPERTS), (2 * MODEL_WIDTH) ** -0.5, 0.09375)
    expert_weights = normal_values(key_list[10], (EXPERTS, 3, MODEL_WIDTH, FF), MODEL_WIDTH ** -0.5, 0.125, ((0, 32),))
    cotangent = normal_values(key_list[11], (TOKENS, MODEL_WIDTH), 1.0, 6.0, ((0, 32),))
    return dict(block_in=block_in, segments=segments, routes=routes, attn_gain=attn_gain, query_key_value_weight=query_key_value_weight, q_gain=q_gain, k_gain=k_gain, w_out=w_out, ffn_gain=ffn_gain, router=router, expert_weights=expert_weights, cotangent=cotangent)


epsilon = 1e-06
rope_base = 1000000.0

def product(form, left, right):
    return jnp.einsum(form, left.astype(jnp.float32), right.astype(jnp.float32), precision=lax.Precision.HIGHEST)

def rms_scale(values):
    return lax.rsqrt(lax.optimization_barrier(jnp.mean(values * values, axis=-1, keepdims=True)) + epsilon)

def rms_back(values, scale, gain, upstream):
    scaled = upstream * gain
    cube = scale * scale * scale
    grad_values = scale * scaled - values * cube * lax.optimization_barrier(jnp.mean(scaled * values, axis=-1, keepdims=True))
    grad_gain = lax.optimization_barrier(jnp.sum((upstream * values * scale).reshape(-1, values.shape[-1]), axis=0))
    return (grad_values, grad_gain)

def rope_tables(positions):
    half = HEAD_SIZE // 2
    freq = rope_base ** (-jnp.arange(half).astype(jnp.float32) * 2.0 / HEAD_SIZE)
    angles = positions.astype(jnp.float32)[:, None] * freq[None, :]
    cosine = jnp.concatenate([jnp.cos(angles), jnp.cos(angles)], axis=-1)
    sine = jnp.concatenate([jnp.sin(angles), jnp.sin(angles)], axis=-1)
    return (cosine[:, None, :], sine[:, None, :])

def rotate(values):
    half = values.shape[-1] // 2
    return jnp.concatenate([-values[..., half:], values[..., :half]], axis=-1)

def rotate_back(values):
    half = values.shape[-1] // 2
    return jnp.concatenate([values[..., half:], -values[..., :half]], axis=-1)

def split_heads(query_key_value):
    token_rows = query_key_value.shape[0]
    q_raw = query_key_value[:, :QUERY_HEADS * HEAD_SIZE].reshape(token_rows, QUERY_HEADS, HEAD_SIZE)
    unrotated_key = query_key_value[:, QUERY_HEADS * HEAD_SIZE:(QUERY_HEADS + KEY_VALUE_HEADS) * HEAD_SIZE].reshape(token_rows, KEY_VALUE_HEADS, HEAD_SIZE)
    projected_value = query_key_value[:, (QUERY_HEADS + KEY_VALUE_HEADS) * HEAD_SIZE:].reshape(token_rows, KEY_VALUE_HEADS, HEAD_SIZE)
    return (q_raw, unrotated_key, projected_value)

def norm_rope(raw, gain, cosine, sine):
    scale = rms_scale(raw)
    normed = raw * scale * gain
    return (scale, (normed * cosine + rotate(normed) * sine).astype(jnp.bfloat16))

def norm_rope_back(raw, scale, gain, cosine, sine, grad_rot):
    grad_normed = grad_rot * cosine + rotate_back(grad_rot * sine)
    return rms_back(raw, scale, gain, grad_normed)

def split_groups(values, groups):
    token_rows, heads, width = values.shape
    return values.reshape(token_rows, groups, heads // groups, width).transpose(1, 0, 2, 3)

def attend_forward(queries, keys, values, allowed):
    groups = keys.shape[1]
    token_rows = queries.shape[0]
    scale = queries.shape[2] ** (-0.5)

    def one_group(operands):
        q_part, k_part, v_part = operands
        scores = jnp.where(allowed[None], product('tpd,sd->pts', q_part, k_part) * scale, -1e+30)
        highest = lax.optimization_barrier(jnp.max(scores, axis=2, keepdims=True))
        lse = highest + jnp.log(lax.optimization_barrier(jnp.sum(jnp.exp(scores - highest), axis=2, keepdims=True)))
        probs = jnp.exp(scores - lse).astype(jnp.bfloat16)
        return (product('pts,sd->tpd', probs, v_part), lse[:, :, 0])
    outputs, lse = lax.map(one_group, (split_groups(queries, groups), keys.transpose(1, 0, 2), values.transpose(1, 0, 2)))
    return (outputs.transpose(1, 0, 2, 3).reshape(token_rows, -1), lse)

def attend_backward(queries, keys, values, allowed, lse, attended, grad_attended):
    groups = keys.shape[1]
    token_rows, heads, width = queries.shape
    scale = width ** (-0.5)

    def one_group(operands):
        q_part, k_part, v_part, lse_part, out_part, grad_part = operands
        scores = jnp.where(allowed[None], product('tpd,sd->pts', q_part, k_part) * scale, -1e+30)
        probs = jnp.exp(scores - lse_part[:, :, None])
        grad_v = product('pts,tpd->sd', probs.astype(jnp.bfloat16), grad_part)
        grad_p = product('tpd,sd->pts', grad_part, v_part)
        delta = lax.optimization_barrier(jnp.sum(out_part.astype(jnp.float32) * grad_part.astype(jnp.float32), axis=2)).transpose(1, 0)
        grad_score = (probs * (grad_p - delta[:, :, None]) * scale).astype(jnp.bfloat16)
        return (product('pts,sd->tpd', grad_score, k_part), product('pts,tpd->sd', grad_score, q_part), grad_v)
    shaped_out = split_groups(attended.reshape(token_rows, heads, width), groups)
    shaped_grad = split_groups(grad_attended.reshape(token_rows, heads, width), groups)
    grad_q, grad_k, grad_v = lax.map(one_group, (split_groups(queries, groups), keys.transpose(1, 0, 2), values.transpose(1, 0, 2), lse, shaped_out, shaped_grad))
    return (grad_q.transpose(1, 0, 2, 3).reshape(token_rows, heads, width), grad_k.transpose(1, 0, 2), grad_v.transpose(1, 0, 2))

def route_gates(normed, router, routes):
    logits = jnp.dot(normed, router, preferred_element_type=jnp.float32)
    weights = jax.nn.softmax(logits, axis=-1)
    chosen = (routes[:, :, None] == jnp.arange(router.shape[1], dtype=jnp.int32)[None, None, :]).astype(jnp.float32)
    picked = lax.optimization_barrier(jnp.sum(chosen * weights[:, None, :], axis=2))
    total = lax.optimization_barrier(jnp.sum(picked, axis=1, keepdims=True))
    return (weights, chosen, picked, total, picked / total)

def route_gates_back(normed, router, weights, chosen, picked, total, grad_gates):
    grad_picked = grad_gates / total - lax.optimization_barrier(jnp.sum(grad_gates * picked, axis=1, keepdims=True)) / (total * total)
    grad_weights = lax.optimization_barrier(jnp.sum(chosen * grad_picked[:, :, None], axis=1))
    grad_logits = weights * (grad_weights - lax.optimization_barrier(jnp.sum(grad_weights * weights, axis=1, keepdims=True)))
    grad_normed = jnp.dot(grad_logits, router.astype(jnp.float32).T, precision=lax.Precision.HIGHEST)
    grad_router = jnp.dot(normed.astype(jnp.float32).T, grad_logits, precision=lax.Precision.HIGHEST)
    return (grad_normed, grad_router)

def route_index(routes, experts, capacity):
    flat = routes.reshape(-1)
    onehot = (flat[:, None] == jnp.arange(experts, dtype=jnp.int32)[None, :]).astype(jnp.int32)
    before = jnp.cumsum(onehot, axis=0) - onehot
    return flat * capacity + lax.optimization_barrier(jnp.sum(before * onehot, axis=1))

def dispatch(rows_per_route, index, experts, capacity):
    width = rows_per_route.shape[1]
    empty = jnp.zeros((experts * capacity, width), rows_per_route.dtype)
    return empty.at[index].set(rows_per_route).reshape(experts, capacity, width)

def collect(buffer, index):
    return buffer.reshape(-1, buffer.shape[-1])[index]

def expert_forward(inputs, weights):
    gate_pre = product('ecd,edf->ecf', inputs, weights[:, 0])
    up_pre = product('ecd,edf->ecf', inputs, weights[:, 1])
    hidden = (jax.nn.silu(gate_pre) * up_pre).astype(jnp.bfloat16)
    result = product('ecf,edf->ecd', hidden, weights[:, 2]).astype(jnp.bfloat16)
    return (gate_pre, up_pre, hidden, result)

def expert_backward(inputs, weights, gate_pre, up_pre, grad_result):
    grad_hidden = product('ecd,edf->ecf', grad_result, weights[:, 2])
    sig = jax.nn.sigmoid(gate_pre)
    grad_gate = (grad_hidden * up_pre * sig * (1.0 + gate_pre * (1.0 - sig))).astype(jnp.bfloat16)
    grad_up = (grad_hidden * gate_pre * sig).astype(jnp.bfloat16)
    grad_inputs = product('ecf,edf->ecd', grad_gate, weights[:, 0]) + product('ecf,edf->ecd', grad_up, weights[:, 1])
    return (grad_gate, grad_up, grad_inputs.astype(jnp.bfloat16))

def expert_weight_grads(inputs, hidden, grad_gate, grad_up, grad_result):
    return jnp.stack([product('ecd,ecf->edf', inputs, grad_gate), product('ecd,ecf->edf', inputs, grad_up), product('ecd,ecf->edf', grad_result, hidden)], axis=1)

def reference(block_in, segments, routes, attn_gain, query_key_value_weight, q_gain, k_gain, w_out, ffn_gain, router, expert_weights, cotangent):
    experts = EXPERTS
    blocks = N_SHARD
    tok = SEQ // blocks
    positions = jnp.arange(SEQ, dtype=jnp.int32)
    cosine, sine = rope_tables(positions)

    def front(x_seq, seg_seq, route_seq, cot_seq):
        inputs = x_seq.astype(jnp.float32)
        scale_one = rms_scale(inputs)
        normed_one = (inputs * scale_one * attn_gain).astype(jnp.bfloat16)
        query_key_value = jnp.dot(normed_one, query_key_value_weight, preferred_element_type=jnp.float32)
        q_raw, unrotated_key, projected_value = split_heads(query_key_value)
        q_scale, q_rot = norm_rope(q_raw, q_gain, cosine, sine)
        k_scale, k_rot = norm_rope(unrotated_key, k_gain, cosine, sine)
        v_b = projected_value.astype(jnp.bfloat16)
        allowed = (seg_seq[:, None] == seg_seq[None, :]) & (positions[None, :] <= positions[:, None])
        attended_f, lse = attend_forward(q_rot, k_rot, v_b, allowed)
        attended = attended_f.astype(jnp.bfloat16)
        middle = inputs + jnp.dot(attended, w_out, preferred_element_type=jnp.float32)
        scale_two = rms_scale(middle)
        normed_two = (middle * scale_two * ffn_gain).astype(jnp.bfloat16)
        weights, chosen, picked, total, gates = route_gates(normed_two, router, route_seq)
        index = jax.vmap(lambda r: route_index(r, experts, CAP))(route_seq.reshape(blocks, tok, TOP))
        upstream = cot_seq.astype(jnp.float32)
        grad_rows = (gates[:, :, None] * upstream[:, None, :]).astype(jnp.bfloat16).reshape(SEQ * TOP, MODEL_WIDTH)
        paired = jnp.concatenate([jnp.repeat(normed_two, TOP, axis=0), grad_rows], axis=1).reshape(blocks, tok * TOP, 2 * MODEL_WIDTH)
        buffer = jax.vmap(lambda r, i: dispatch(r, i, experts, CAP))(paired, index)
        kept = (inputs, scale_one, normed_one, q_raw, q_scale, q_rot, unrotated_key, k_scale, k_rot, v_b, allowed, lse, attended, middle, scale_two, normed_two, weights, chosen, picked, total, gates, index, upstream)
        return (kept, buffer)

    def first_pass(carry, operands):
        kept, buffer = front(*operands)
        return (carry, buffer)
    sequences = block_in.shape[0] // SEQ
    operands = (block_in.reshape(sequences, SEQ, MODEL_WIDTH), segments.reshape(sequences, SEQ), routes.reshape(sequences, SEQ, TOP), cotangent.reshape(sequences, SEQ, MODEL_WIDTH))
    _, buffers = lax.scan(first_pass, jnp.zeros((), jnp.float32), operands)
    buffers = buffers.reshape(sequences * blocks, experts, CAP, 2 * MODEL_WIDTH)
    slots = sequences * blocks * CAP

    def one_expert(expert):
        slab = lax.dynamic_index_in_dim(buffers, expert, 1, keepdims=False).reshape(1, slots, 2 * MODEL_WIDTH)
        token_rows = slab[:, :, :MODEL_WIDTH]
        grads = slab[:, :, MODEL_WIDTH:]
        own = lax.dynamic_index_in_dim(expert_weights, expert, 0, keepdims=True)
        gate_pre, up_pre, hidden, result = expert_forward(token_rows, own)
        grad_gate, grad_up, grad_inner = expert_backward(token_rows, own, gate_pre, up_pre, grads)
        grad_own = expert_weight_grads(token_rows, hidden, grad_gate, grad_up, grads)
        return (jnp.concatenate([result, grad_inner], axis=2)[0], grad_own[0])
    backs, grad_exp = lax.map(one_expert, jnp.arange(experts, dtype=jnp.int32))
    backs = backs.reshape(experts, sequences, blocks, CAP, 2 * MODEL_WIDTH).transpose(1, 2, 0, 3, 4)

    def second_pass(carry, operands):
        x_seq, seg_seq, route_seq, cot_seq, back_seq = operands
        kept, buffer = front(x_seq, seg_seq, route_seq, cot_seq)
        inputs, scale_one, normed_one, q_raw, q_scale, q_rot, unrotated_key, k_scale, k_rot, v_b, allowed, lse, attended, middle, scale_two, normed_two, weights, chosen, picked, total, gates, index, upstream = kept
        fetched = jax.vmap(collect)(back_seq, index).reshape(SEQ, TOP, 2 * MODEL_WIDTH)
        expert_rows = fetched[:, :, :MODEL_WIDTH].astype(jnp.float32)
        grad_from_experts = lax.optimization_barrier(jnp.sum(fetched[:, :, MODEL_WIDTH:].astype(jnp.float32), axis=1))
        block_out = (middle + lax.optimization_barrier(jnp.sum(gates[:, :, None] * expert_rows, axis=1))).astype(jnp.bfloat16)
        grad_gates = lax.optimization_barrier(jnp.sum(expert_rows * upstream[:, None, :], axis=2))
        grad_from_router, grad_rt = route_gates_back(normed_two, router, weights, chosen, picked, total, grad_gates)
        grad_norm_two, grad_fg = rms_back(middle, scale_two, ffn_gain, grad_from_experts + grad_from_router)
        grad_middle = upstream + grad_norm_two
        grad_middle_b = grad_middle.astype(jnp.bfloat16)
        grad_o = jnp.dot(attended.T, grad_middle_b, preferred_element_type=jnp.float32)
        grad_attended = jnp.dot(grad_middle_b, w_out.T, preferred_element_type=jnp.float32).astype(jnp.bfloat16)
        grad_q_rot, grad_k_rot, grad_v = attend_backward(q_rot, k_rot, v_b, allowed, lse, attended, grad_attended)
        grad_q_raw, grad_qg = norm_rope_back(q_raw, q_scale, q_gain, cosine, sine, grad_q_rot)
        grad_k_raw, grad_kg = norm_rope_back(unrotated_key, k_scale, k_gain, cosine, sine, grad_k_rot)
        grad_qkv_b = jnp.concatenate([grad_q_raw.reshape(SEQ, -1), grad_k_raw.reshape(SEQ, -1), grad_v.reshape(SEQ, -1)], axis=1).astype(jnp.bfloat16)
        grad_w = jnp.dot(normed_one.T, grad_qkv_b, preferred_element_type=jnp.float32)
        grad_norm_one = jnp.dot(grad_qkv_b, query_key_value_weight.T, preferred_element_type=jnp.float32)
        grad_inputs, grad_ag = rms_back(inputs, scale_one, attn_gain, grad_norm_one)
        grad_input = (grad_middle + grad_inputs).astype(jnp.bfloat16)
        updates = (grad_ag, grad_w, grad_qg, grad_kg, grad_o, grad_fg, grad_rt)
        carry = tuple((a + b for a, b in zip(carry, updates)))
        return (carry, (block_out, grad_input))
    zeros = (jnp.zeros((MODEL_WIDTH,), jnp.float32), jnp.zeros(query_key_value_weight.shape, jnp.float32), jnp.zeros((HEAD_SIZE,), jnp.float32), jnp.zeros((HEAD_SIZE,), jnp.float32), jnp.zeros(w_out.shape, jnp.float32), jnp.zeros((MODEL_WIDTH,), jnp.float32), jnp.zeros(router.shape, jnp.float32))
    sums, (outputs, grads_in) = lax.scan(second_pass, zeros, operands + (backs,))
    return (outputs.reshape(-1, MODEL_WIDTH), grads_in.reshape(-1, MODEL_WIDTH), sums[0], sums[1], sums[2], sums[3], sums[4], sums[5], sums[6], grad_exp)
```

```python
import functools

import jax
import jax.numpy as jnp
from jax import lax
from jax.experimental import pallas as pl
from jax.experimental.pallas import tpu as pltpu
from jax.sharding import PartitionSpec as P


QUERY_HEADS = 32
KEY_VALUE_HEADS = 4
HEAD_SIZE = 128


epsilon = 1e-06
rope_base = 1000000.0


def product(form, left, right):
    return jnp.einsum(form, left, right, preferred_element_type=jnp.float32)


def rms_scale(values):
    return lax.rsqrt(jnp.mean(values * values, axis=-1, keepdims=True) + epsilon)


def rms_back(values, scale, gain, upstream):
    scaled = upstream * gain
    cube = scale * scale * scale
    grad_values = scale * scaled - values * cube * jnp.mean(scaled * values, axis=-1, keepdims=True)
    grad_gain = jnp.sum((upstream * values * scale).reshape(-1, values.shape[-1]), axis=0)
    return (grad_values, grad_gain)


def rope_tables(positions):
    half = HEAD_SIZE // 2
    freq = rope_base ** (-jnp.arange(half).astype(jnp.float32) * 2.0 / HEAD_SIZE)
    angles = positions.astype(jnp.float32)[:, None] * freq[None, :]
    cosine = jnp.concatenate([jnp.cos(angles), jnp.cos(angles)], axis=-1)
    sine = jnp.concatenate([jnp.sin(angles), jnp.sin(angles)], axis=-1)
    return (cosine[:, None, :], sine[:, None, :])


def rotate(values):
    half = values.shape[-1] // 2
    return jnp.concatenate([-values[..., half:], values[..., :half]], axis=-1)


def rotate_back(values):
    half = values.shape[-1] // 2
    return jnp.concatenate([values[..., half:], -values[..., :half]], axis=-1)


def split_heads(query_key_value):
    token_rows = query_key_value.shape[0]
    q_raw = query_key_value[:, : QUERY_HEADS * HEAD_SIZE].reshape(
        token_rows, QUERY_HEADS, HEAD_SIZE
    )
    unrotated_key = query_key_value[
        :, QUERY_HEADS * HEAD_SIZE : (QUERY_HEADS + KEY_VALUE_HEADS) * HEAD_SIZE
    ].reshape(token_rows, KEY_VALUE_HEADS, HEAD_SIZE)
    projected_value = query_key_value[:, (QUERY_HEADS + KEY_VALUE_HEADS) * HEAD_SIZE :].reshape(
        token_rows, KEY_VALUE_HEADS, HEAD_SIZE
    )
    return (q_raw, unrotated_key, projected_value)


def norm_rope(raw, gain, cosine, sine):
    scale = rms_scale(raw)
    normed = raw * scale * gain
    return (scale, (normed * cosine + rotate(normed) * sine).astype(jnp.bfloat16))


def norm_rope_back(raw, scale, gain, cosine, sine, grad_rot):
    grad_normed = grad_rot * cosine + rotate_back(grad_rot * sine)
    return rms_back(raw, scale, gain, grad_normed)


def split_groups(values, groups):
    token_rows, heads, width = values.shape
    return values.reshape(token_rows, groups, heads // groups, width).transpose(1, 0, 2, 3)


def attend_forward(queries, keys, values, allowed):
    groups = keys.shape[1]
    token_rows = queries.shape[0]
    scale = queries.shape[2] ** (-0.5)

    def one_group(operands):
        q_part, k_part, v_part = operands
        scores = jnp.where(allowed[None], product("tpd,sd->pts", q_part, k_part) * scale, -1e30)
        highest = jnp.max(scores, axis=2, keepdims=True)
        lse = highest + jnp.log(jnp.sum(jnp.exp(scores - highest), axis=2, keepdims=True))
        probs = jnp.exp(scores - lse).astype(jnp.bfloat16)
        return (product("pts,sd->tpd", probs, v_part), lse[:, :, 0])

    outputs, lse = lax.map(
        one_group,
        (split_groups(queries, groups), keys.transpose(1, 0, 2), values.transpose(1, 0, 2)),
    )
    return (outputs.transpose(1, 0, 2, 3).reshape(token_rows, -1), lse)


def attend_backward(queries, keys, values, allowed, lse, attended, grad_attended):
    groups = keys.shape[1]
    token_rows, heads, width = queries.shape
    scale = width ** (-0.5)

    def one_group(operands):
        q_part, k_part, v_part, lse_part, out_part, grad_part = operands
        scores = jnp.where(allowed[None], product("tpd,sd->pts", q_part, k_part) * scale, -1e30)
        probs = jnp.exp(scores - lse_part[:, :, None])
        grad_v = product("pts,tpd->sd", probs.astype(jnp.bfloat16), grad_part)
        grad_p = product("tpd,sd->pts", grad_part, v_part)
        delta = jnp.sum(
            out_part.astype(jnp.float32) * grad_part.astype(jnp.float32), axis=2
        ).transpose(1, 0)
        grad_score = (probs * (grad_p - delta[:, :, None]) * scale).astype(jnp.bfloat16)
        return (
            product("pts,sd->tpd", grad_score, k_part),
            product("pts,tpd->sd", grad_score, q_part),
            grad_v,
        )

    shaped_out = split_groups(attended.reshape(token_rows, heads, width), groups)
    shaped_grad = split_groups(grad_attended.reshape(token_rows, heads, width), groups)
    grad_q, grad_k, grad_v = lax.map(
        one_group,
        (
            split_groups(queries, groups),
            keys.transpose(1, 0, 2),
            values.transpose(1, 0, 2),
            lse,
            shaped_out,
            shaped_grad,
        ),
    )
    return (
        grad_q.transpose(1, 0, 2, 3).reshape(token_rows, heads, width),
        grad_k.transpose(1, 0, 2),
        grad_v.transpose(1, 0, 2),
    )


def route_gates(normed, router, routes):
    logits = jnp.dot(normed, router, preferred_element_type=jnp.float32)
    weights = jax.nn.softmax(logits, axis=-1)
    chosen = (
        routes[:, :, None] == jnp.arange(router.shape[1], dtype=jnp.int32)[None, None, :]
    ).astype(jnp.float32)
    picked = jnp.sum(chosen * weights[:, None, :], axis=2)
    total = jnp.sum(picked, axis=1, keepdims=True)
    return (weights, chosen, picked, total, picked / total)


def route_gates_back(normed, router, weights, chosen, picked, total, grad_gates):
    grad_picked = grad_gates / total - jnp.sum(grad_gates * picked, axis=1, keepdims=True) / (
        total * total
    )
    grad_weights = jnp.sum(chosen * grad_picked[:, :, None], axis=1)
    grad_logits = weights * (grad_weights - jnp.sum(grad_weights * weights, axis=1, keepdims=True))
    grad_normed = jnp.dot(
        grad_logits, router.astype(jnp.float32).T, precision=lax.Precision.HIGHEST
    )
    grad_router = jnp.dot(
        normed.astype(jnp.float32).T, grad_logits, precision=lax.Precision.HIGHEST
    )
    return (grad_normed, grad_router)


def route_index(routes, experts, capacity):
    flat = routes.reshape(-1)
    onehot = (flat[:, None] == jnp.arange(experts, dtype=jnp.int32)[None, :]).astype(jnp.int32)
    before = jnp.cumsum(onehot, axis=0) - onehot
    return flat * capacity + jnp.sum(before * onehot, axis=1)


def dispatch(rows_per_route, index, experts, capacity):
    width = rows_per_route.shape[1]
    empty = jnp.zeros((experts * capacity, width), rows_per_route.dtype)
    return empty.at[index].set(rows_per_route).reshape(experts, capacity, width)


def collect(buffer, index):
    return buffer.reshape(-1, buffer.shape[-1])[index]


def expert_forward(inputs, weights):
    gate_pre = product("ecd,edf->ecf", inputs, weights[:, 0])
    up_pre = product("ecd,edf->ecf", inputs, weights[:, 1])
    hidden = (jax.nn.silu(gate_pre) * up_pre).astype(jnp.bfloat16)
    result = product("ecf,edf->ecd", hidden, weights[:, 2]).astype(jnp.bfloat16)
    return (gate_pre, up_pre, hidden, result)


def expert_backward(weights, gate_pre, up_pre, grad_result):
    grad_hidden = product("ecd,edf->ecf", grad_result, weights[:, 2])
    sig = jax.nn.sigmoid(gate_pre)
    grad_gate = (grad_hidden * up_pre * sig * (1.0 + gate_pre * (1.0 - sig))).astype(jnp.bfloat16)
    grad_up = (grad_hidden * gate_pre * sig).astype(jnp.bfloat16)
    grad_inputs = product("ecf,edf->ecd", grad_gate, weights[:, 0]) + product(
        "ecf,edf->ecd", grad_up, weights[:, 1]
    )
    return (grad_gate, grad_up, grad_inputs.astype(jnp.bfloat16))


def expert_weight_grads(inputs, hidden, grad_gate, grad_up, grad_result):
    return jnp.stack(
        [
            product("ecd,ecf->edf", inputs, grad_gate),
            product("ecd,ecf->edf", inputs, grad_up),
            product("ecd,ecf->edf", grad_result, hidden),
        ],
        axis=1,
    )


def plain_body(
    block_in,
    segments,
    routes,
    attn_gain,
    query_key_value_weight,
    q_gain,
    k_gain,
    w_out,
    ffn_gain,
    router,
    expert_weights,
    cotangent,
):
    tok = block_in.shape[0]
    width = block_in.shape[1]
    top = routes.shape[1]
    rep_count = lax.axis_size("rep")
    shard_count = lax.axis_size("shard")
    experts = expert_weights.shape[0] * rep_count * shard_count
    capacity = tok * top * 2 // experts
    shard_pos = lax.axis_index("shard")
    qkv_whole, out_whole = (
        lax.all_gather(query_key_value_weight, "shard", axis=0, tiled=True),
        lax.all_gather(w_out, "shard", axis=0, tiled=True),
    )
    inputs = block_in.astype(jnp.float32)
    scale_one = rms_scale(inputs)
    normed_one = (inputs * scale_one * attn_gain).astype(jnp.bfloat16)
    query_key_value = jnp.dot(normed_one, qkv_whole, preferred_element_type=jnp.float32)
    q_raw, unrotated_key, projected_value = split_heads(query_key_value)
    positions = shard_pos * tok + jnp.arange(tok, dtype=jnp.int32)
    cosine, sine = rope_tables(positions)
    q_scale, q_rot = norm_rope(q_raw, q_gain, cosine, sine)
    k_scale, k_rot = norm_rope(unrotated_key, k_gain, cosine, sine)
    keys_all, values_all = (
        lax.all_gather(k_rot, "shard", axis=0, tiled=True),
        lax.all_gather(projected_value.astype(jnp.bfloat16), "shard", axis=0, tiled=True),
    )
    query_seg = lax.dynamic_slice_in_dim(segments, shard_pos * tok, tok)
    key_pos = jnp.arange(segments.shape[0], dtype=jnp.int32)
    allowed = (query_seg[:, None] == segments[None, :]) & (key_pos[None, :] <= positions[:, None])
    attended_f, lse = attend_forward(q_rot, keys_all, values_all, allowed)
    attended = attended_f.astype(jnp.bfloat16)
    middle = inputs + jnp.dot(attended, out_whole, preferred_element_type=jnp.float32)
    scale_two = rms_scale(middle)
    normed_two = (middle * scale_two * ffn_gain).astype(jnp.bfloat16)
    weights, chosen, picked, total, gates = route_gates(normed_two, router, routes)
    index = route_index(routes, experts, capacity)
    upstream = cotangent.astype(jnp.float32)
    grad_rows = (
        (gates[:, :, None] * upstream[:, None, :]).astype(jnp.bfloat16).reshape(tok * top, width)
    )
    paired = jnp.concatenate([jnp.repeat(normed_two, top, axis=0), grad_rows], axis=1)
    buffer = dispatch(paired, index, experts, capacity)
    received = lax.all_to_all(buffer, ("rep", "shard"), split_axis=0, concat_axis=1, tiled=True)
    token_rows = received[:, :, :width]
    grads = received[:, :, width:]
    gate_pre, up_pre, hidden, result = expert_forward(token_rows, expert_weights)
    grad_gate, grad_up, grad_inner = expert_backward(expert_weights, gate_pre, up_pre, grads)
    grad_experts = expert_weight_grads(token_rows, hidden, grad_gate, grad_up, grads)
    outgoing = jnp.concatenate([result, grad_inner], axis=2)
    returned = lax.all_to_all(outgoing, ("rep", "shard"), split_axis=1, concat_axis=0, tiled=True)
    fetched = collect(returned, index).reshape(tok, top, 2 * width)
    expert_rows = fetched[:, :, :width].astype(jnp.float32)
    grad_from_experts = jnp.sum(fetched[:, :, width:].astype(jnp.float32), axis=1)
    block_out = (middle + jnp.sum(gates[:, :, None] * expert_rows, axis=1)).astype(jnp.bfloat16)
    grad_gates = jnp.sum(expert_rows * upstream[:, None, :], axis=2)
    grad_from_router, grad_router = route_gates_back(
        normed_two, router, weights, chosen, picked, total, grad_gates
    )
    grad_norm_two, grad_ffn_gain = rms_back(
        middle, scale_two, ffn_gain, grad_from_experts + grad_from_router
    )
    grad_middle = upstream + grad_norm_two
    grad_middle_b = grad_middle.astype(jnp.bfloat16)
    columns = attended
    grad_out = lax.psum_scatter(
        lax.dot_general(
            columns, grad_middle_b, (((0,), (0,)), ((), ())), preferred_element_type=jnp.float32
        ).astype(jnp.bfloat16),
        "shard",
        scatter_dimension=0,
        tiled=True,
    ).astype(jnp.float32)
    grad_attended = jnp.dot(grad_middle_b, out_whole.T, preferred_element_type=jnp.float32).astype(
        jnp.bfloat16
    )
    grad_q_rot, grad_k_all, grad_v_all = attend_backward(
        q_rot, keys_all, values_all, allowed, lse, attended, grad_attended
    )
    grad_k_rot, grad_v = (
        lax.psum_scatter(
            grad_k_all.astype(jnp.bfloat16), "shard", scatter_dimension=0, tiled=True
        ).astype(jnp.float32),
        lax.psum_scatter(
            grad_v_all.astype(jnp.bfloat16), "shard", scatter_dimension=0, tiled=True
        ).astype(jnp.float32),
    )
    grad_q_raw, grad_q_gain = norm_rope_back(q_raw, q_scale, q_gain, cosine, sine, grad_q_rot)
    grad_k_raw, grad_k_gain = norm_rope_back(
        unrotated_key, k_scale, k_gain, cosine, sine, grad_k_rot
    )
    grad_qkv_b = jnp.concatenate(
        [grad_q_raw.reshape(tok, -1), grad_k_raw.reshape(tok, -1), grad_v.reshape(tok, -1)], axis=1
    ).astype(jnp.bfloat16)
    columns = normed_one
    grad_qkv = lax.psum_scatter(
        lax.dot_general(
            columns, grad_qkv_b, (((0,), (0,)), ((), ())), preferred_element_type=jnp.float32
        ).astype(jnp.bfloat16),
        "shard",
        scatter_dimension=0,
        tiled=True,
    ).astype(jnp.float32)
    grad_norm_one = jnp.dot(grad_qkv_b, qkv_whole.T, preferred_element_type=jnp.float32)
    grad_inputs, grad_attn_gain = rms_back(inputs, scale_one, attn_gain, grad_norm_one)
    grad_input = (grad_middle + grad_inputs).astype(jnp.bfloat16)
    grad_attn_gain, grad_q_gain, grad_k_gain, grad_ffn_gain, grad_router = lax.psum(
        (grad_attn_gain, grad_q_gain, grad_k_gain, grad_ffn_gain, grad_router), ("rep", "shard")
    )
    grad_qkv, grad_out = (
        lax.psum(grad_qkv.astype(jnp.bfloat16), "rep").astype(jnp.float32),
        lax.psum(grad_out.astype(jnp.bfloat16), "rep").astype(jnp.float32),
    )
    return (
        block_out,
        grad_input,
        grad_attn_gain,
        grad_qkv,
        grad_q_gain,
        grad_k_gain,
        grad_out,
        grad_ffn_gain,
        grad_router,
        grad_experts,
    )


MESH_ID = pl.DeviceIdType.MESH
PLANES = 4


def place():
    rep, shard = lax.axis_index("rep"), lax.axis_index("shard")
    return rep // 2, rep % 2, shard // 2, shard % 2


def device(z, core, y, x):
    return (z * 2 + core, y * 2 + x)


def block_of(z, core, y, x):
    return (z * 2 + core) * 4 + y * 2 + x


def greet(targets):
    barrier = pltpu.get_barrier_semaphore()
    for condition, target in targets:
        if condition is None:
            pl.semaphore_signal(barrier, inc=1, device_id=target, device_id_type=MESH_ID)
        else:

            @pl.when(condition)
            def _():
                pl.semaphore_signal(barrier, inc=1, device_id=target, device_id_type=MESH_ID)

    peers = 0
    for condition, _ in targets:
        peers = peers + (1 if condition is None else condition.astype(jnp.int32))
    pl.semaphore_wait(barrier, peers)


def gather_kernel(rows, *refs):
    count = len(rows)
    ins, outs = refs[:count], refs[count : 2 * count]
    send_sem, recv_sem, own_sem = refs[2 * count :]
    z, core, y, x = place()
    partner = device(z, 1 - core, y, x)
    x_next, y_next = device(z, core, y, 1 - x), device(z, core, 1 - y, x)
    up, down = device(z + 1, core, y, x), device(z - 1, core, y, x)
    greet(
        [
            (None, partner),
            (None, x_next),
            (None, y_next),
            (z < PLANES - 1, up),
            (z > 0, down),
        ]
    )
    pending, used = [], [0]
    can_up, can_down = z < PLANES - 1, z > 0

    def region(array, block, part):
        size = rows[array]
        if part is None:
            return pl.ds(pl.multiple_of(block * size, size), size)
        return pl.ds(pl.multiple_of(block * size + part * (size // 2), size // 2), size // 2)

    def copy_of(array, block, part, target, index, own=False):
        where = region(array, block, part)
        source = ins[array] if own else outs[array].at[where]
        return pltpu.make_async_remote_copy(
            src_ref=source,
            dst_ref=outs[array].at[where],
            send_sem=send_sem.at[array, index],
            recv_sem=recv_sem.at[array, block * 2 + (part or 0)],
            device_id=target,
            device_id_type=MESH_ID,
        )

    def send(block, part, target, condition=None, own=False, guard=None):
        index = used[0]
        used[0] += 1

        def start():
            for array in range(count):
                copy_of(array, block, part, target, index, own).start()

        def finish():
            for array in range(count):
                copy_of(array, block, part, target, index, own).wait_send()

        if condition is None:
            start()
        else:
            pl.when(condition)(start)
        pending.append(([c for c in (guard, condition) if c is not None], finish))

    def arrived(block, part):
        for array in range(count):
            copy_of(array, block, part, partner, 0).wait_recv()

    own = block_of(z, core, y, x)
    send(own, None, up, can_up, own=True)
    send(own, None, down, can_down, own=True)
    send(own, None, x_next, own=True)
    send(own, None, y_next, own=True)
    send(own, None, partner, own=True)
    for array in range(count):
        pltpu.make_async_copy(
            ins[array], outs[array].at[region(array, own, None)], own_sem.at[array]
        ).start()

    def planes(step):
        if step == 0:
            return [(None, z)]
        return [(z >= step, z - step), (z + step < PLANES, z + step)]

    def under(condition, run):
        if condition is None:
            run()
        else:
            pl.when(condition)(run)

    def along_z(step):
        for side, (condition, plane) in enumerate(planes(step)):
            block = block_of(plane, core, y, x)

            def run():
                arrived(block, None)
                if side == 0:
                    send(block, None, up, can_up, guard=condition)
                else:
                    send(block, None, down, can_down, guard=condition)
                send(block, None, x_next, guard=condition)
                send(block, None, y_next, guard=condition)
                send(block, None, partner, guard=condition)

            under(condition, run)

    def across(step):
        for condition, plane in planes(step):
            from_x, from_y = block_of(plane, core, y, 1 - x), block_of(plane, core, 1 - y, x)

            def run():
                arrived(from_x, None)
                send(from_x, 1, y_next, guard=condition)
                send(from_x, None, partner, guard=condition)
                arrived(from_y, None)
                send(from_y, 0, x_next, guard=condition)
                send(from_y, None, partner, guard=condition)

            under(condition, run)

    def diagonal(step):
        for condition, plane in planes(step):
            block = block_of(plane, core, 1 - y, 1 - x)

            def run():
                for part in range(2):
                    arrived(block, part)
                    send(block, part, partner, guard=condition)

            under(condition, run)

    along_z(1)
    across(0)
    along_z(2)
    across(1)
    along_z(3)
    diagonal(0)
    across(2)
    diagonal(1)
    across(3)
    diagonal(2)
    diagonal(3)
    for plane in range(PLANES):
        for where_y, where_x in ((y, x), (y, 1 - x), (1 - y, x)):
            arrived(block_of(plane, 1 - core, where_y, where_x), None)
        for part in range(2):
            arrived(block_of(plane, 1 - core, 1 - y, 1 - x), part)
    for array in range(count):
        pltpu.make_async_copy(
            ins[array], outs[array].at[region(array, own, None)], own_sem.at[array]
        ).wait()
    for conditions, finish in pending:
        if len(conditions) == 2:
            under(jnp.logical_and(*conditions), finish)
        else:
            under(conditions[0] if conditions else None, finish)


def gather_all(arrays, collective_id):
    rows = tuple(array.shape[0] for array in arrays)
    count = len(arrays)
    return pl.pallas_call(
        functools.partial(gather_kernel, rows),
        out_shape=[
            jax.ShapeDtypeStruct((array.shape[0] * 32,) + array.shape[1:], array.dtype)
            for array in arrays
        ],
        in_specs=[pl.BlockSpec(memory_space=pltpu.VMEM)] * count,
        out_specs=[pl.BlockSpec(memory_space=pltpu.HBM)] * count,
        scratch_shapes=[
            pltpu.SemaphoreType.DMA((count, 72)),
            pltpu.SemaphoreType.DMA((count, 64)),
            pltpu.SemaphoreType.DMA((count,)),
        ],
        compiler_params=pltpu.CompilerParams(
            collective_id=collective_id, has_side_effects=True, vmem_limit_bytes=40 << 20
        ),
        name="gather_all",
    )(*arrays)


def add_rows(target, sources, rows=128, step=16):
    @pl.loop(0, rows // step)
    def _(i):
        where = pl.ds(pl.multiple_of(i * step, step), step)
        total = target[where].astype(jnp.float32)
        for source in sources:
            total += source[where].astype(jnp.float32)
        target[where] = total.astype(target.dtype)


def reduce_kernel(
    part_ref,
    out_ref,
    kept,
    paired,
    x_half,
    x_full,
    y_half,
    y_full,
    from_up,
    from_down,
    send_sem,
    pair_sem,
    x_sem,
    y_sem,
    z_sem,
    load_sem,
):
    rows = out_ref.shape[0]
    half = rows // 2
    z, core, y, x = place()
    partner = device(z, 1 - core, y, x)
    x_next, y_next = device(z, core, y, 1 - x), device(z, core, 1 - y, x)
    up, down = device(z + 1, core, y, x), device(z - 1, core, y, x)
    greet(
        [
            (None, partner),
            (None, x_next),
            (None, y_next),
            (z < PLANES - 1, up),
            (z > 0, down),
        ]
    )
    pending, used = [], [0]

    def send(source, landing, sem, target, condition=None):
        copy = pltpu.make_async_remote_copy(
            src_ref=source,
            dst_ref=landing,
            send_sem=send_sem.at[used[0]],
            recv_sem=sem,
            device_id=target,
            device_id_type=MESH_ID,
        )
        used[0] += 1
        if condition is None:
            copy.start()
        pending.append((condition, copy))
        return copy

    def arrived(landing, sem):
        pltpu.make_async_remote_copy(
            src_ref=landing,
            dst_ref=landing,
            send_sem=send_sem.at[0],
            recv_sem=sem,
            device_id=partner,
            device_id_type=MESH_ID,
        ).wait_recv()

    order = (0, 3, 1, 2)
    spots = ((1 - y, 1 - x), (y, 1 - x), (1 - y, x), (y, x))

    def slot(plane, spot):
        return plane * 4 + spots[spot][0] * 2 + spots[spot][1]

    def block(plane, which, spot):
        size = pl.multiple_of(block_of(plane, which, *spots[spot]) * rows, rows)
        return part_ref.at[pl.ds(size, rows)]

    def load(plane, spot):
        return pltpu.make_async_copy(
            block(plane, core, spot), kept.at[slot(plane, spot)], load_sem.at[spot * 4 + plane]
        )

    for spot in range(4):
        for plane in order:
            where = slot(plane, spot)
            send(block(plane, 1 - core, spot), paired.at[where], pair_sem.at[where], partner)
            load(plane, spot).start()

    def joined(plane, spot, more=()):
        where = slot(plane, spot)
        load(plane, spot).wait()
        arrived(paired.at[where], pair_sem.at[where])
        add_rows(kept.at[where], (paired.at[where],) + tuple(more), rows)

    for plane in order:
        joined(plane, 0)
        source = kept.at[slot(plane, 0)]
        send(source.at[pl.ds(0, half)], x_half.at[plane], x_sem.at[plane], x_next)
        send(source.at[pl.ds(half, half)], y_half.at[plane], y_sem.at[plane], y_next)
    for plane in order:
        joined(plane, 1)
        arrived(y_half.at[plane], y_sem.at[plane])
        add_rows(kept.at[slot(plane, 1)].at[pl.ds(half, half)], (y_half.at[plane],), half)
        send(kept.at[slot(plane, 1)], x_full.at[plane], x_sem.at[4 + plane], x_next)
        joined(plane, 2)
        arrived(x_half.at[plane], x_sem.at[plane])
        add_rows(kept.at[slot(plane, 2)].at[pl.ds(0, half)], (x_half.at[plane],), half)
        send(kept.at[slot(plane, 2)], y_full.at[plane], y_sem.at[4 + plane], y_next)
    for plane in order:
        arrived(x_full.at[plane], x_sem.at[4 + plane])
        arrived(y_full.at[plane], y_sem.at[4 + plane])
        joined(plane, 3, (x_full.at[plane], y_full.at[plane]))
        total = kept.at[slot(plane, 3)]
        if plane < PLANES - 1:
            copy = send(total, from_up.at[plane], z_sem.at[0, plane], down, z > plane)

            @pl.when(z > plane)
            def _():
                @pl.when(z < PLANES - 1)
                def _():
                    arrived(from_up.at[plane], z_sem.at[0, plane])
                    add_rows(total, (from_up.at[plane],), rows)

                copy.start()

        if plane > 0:
            climb = send(total, from_down.at[plane - 1], z_sem.at[1, plane - 1], up, z < plane)

            @pl.when(z < plane)
            def _():
                @pl.when(z > 0)
                def _():
                    arrived(from_down.at[plane - 1], z_sem.at[1, plane - 1])
                    add_rows(total, (from_down.at[plane - 1],), rows)

                climb.start()

    mine = kept.at[slot(z, 3)]

    @pl.when(z < PLANES - 1)
    def _():
        arrived(from_up.at[z], z_sem.at[0, z])
        add_rows(mine, (from_up.at[z],), rows)

    @pl.when(z > 0)
    def _():
        arrived(from_down.at[z - 1], z_sem.at[1, z - 1])
        add_rows(mine, (from_down.at[z - 1],), rows)

    out_ref[...] = mine[...]
    for condition, copy in pending:
        if condition is None:
            copy.wait_send()
        else:
            pl.when(condition)(copy.wait_send)


def reduce_all(part, collective_id):
    total, width = part.shape
    rows = total // 32
    half = rows // 2
    dtype = part.dtype
    return pl.pallas_call(
        reduce_kernel,
        out_shape=jax.ShapeDtypeStruct((rows, width), dtype),
        in_specs=[pl.BlockSpec(memory_space=pltpu.HBM)],
        out_specs=pl.BlockSpec(memory_space=pltpu.VMEM),
        scratch_shapes=[
            pltpu.VMEM((16, rows, width), dtype),
            pltpu.VMEM((16, rows, width), dtype),
            pltpu.VMEM((4, half, width), dtype),
            pltpu.VMEM((4, rows, width), dtype),
            pltpu.VMEM((4, half, width), dtype),
            pltpu.VMEM((4, rows, width), dtype),
            pltpu.VMEM((3, rows, width), dtype),
            pltpu.VMEM((3, rows, width), dtype),
            pltpu.SemaphoreType.DMA((48,)),
            pltpu.SemaphoreType.DMA((16,)),
            pltpu.SemaphoreType.DMA((8,)),
            pltpu.SemaphoreType.DMA((8,)),
            pltpu.SemaphoreType.DMA((2, 3)),
            pltpu.SemaphoreType.DMA((16,)),
        ],
        compiler_params=pltpu.CompilerParams(
            collective_id=collective_id, has_side_effects=True, vmem_limit_bytes=60 << 20
        ),
        name="reduce_all",
    )(part)


def others():
    z, core, y, x = place()
    return [
        (device(z, core, yy, xx), yy * 2 + xx)
        for yy, xx in ((y, 1 - x), (1 - y, x), (1 - y, 1 - x))
    ]


def remote(source, landing, send_sem, recv_sem, target):
    return pltpu.make_async_remote_copy(
        src_ref=source,
        dst_ref=landing,
        send_sem=send_sem,
        recv_sem=recv_sem,
        device_id=target,
        device_id_type=MESH_ID,
    )


def start_kernel(
    x_ref, w_ref, x_all, w_own, hold, send_sem, x_sem, w_sem, pair_sem, own_sem
):
    tok = x_ref.shape[0]
    depth = w_ref.shape[0]
    half = depth // 2
    z, core, y, x = place()
    me = y * 2 + x
    partner = device(z, 1 - core, y, x)
    near = others()
    greet([(None, target) for target, _ in near] + [(None, partner)])
    parts = QUERY_HEADS // 4 * HEAD_SIZE
    single = HEAD_SIZE
    widths = (
        (0, parts, 0),
        (QUERY_HEADS * HEAD_SIZE, single, parts),
        ((QUERY_HEADS + KEY_VALUE_HEADS) * HEAD_SIZE, single, parts + single),
    )

    def columns(piece, who):
        base, width, _ = widths[piece]
        return pl.ds(pl.multiple_of(base + who * width, 128), width)

    def landing(piece, who, part, ref=w_own):
        _, width, offset = widths[piece]
        rows = pl.ds(pl.multiple_of(who * depth + part * half, half), half)
        return ref.at[rows, pl.ds(offset, width)]

    sends = []
    for slot, (target, who) in enumerate(near):
        for piece in range(3):
            copy = remote(
                w_ref.at[pl.ds(pl.multiple_of(core * half, half), half), columns(piece, who)],
                landing(piece, me, core),
                send_sem.at[slot * 4 + piece],
                w_sem.at[slot * 3 + piece],
                target,
            )
            copy.start()
            sends.append(copy)
        copy = remote(
            x_ref,
            x_all.at[pl.ds(pl.multiple_of(me * tok, tok), tok)],
            send_sem.at[slot * 4 + 3],
            x_sem.at[slot],
            target,
        )
        copy.start()
        sends.append(copy)
    mine = pltpu.make_async_copy(
        x_ref, x_all.at[pl.ds(pl.multiple_of(me * tok, tok), tok)], own_sem.at[0]
    )
    mine.start()
    loads = []
    for piece in range(3):
        _, width, offset = widths[piece]
        loads.append(
            pltpu.make_async_copy(
                w_ref.at[:, columns(piece, me)], hold.at[:, pl.ds(offset, width)], own_sem.at[1 + piece]
            )
        )
        loads[-1].start()
    for copy in loads:
        copy.wait()
    keep = pltpu.make_async_copy(
        hold, w_own.at[pl.ds(pl.multiple_of(me * depth, depth), depth)], own_sem.at[4]
    )
    keep.start()
    for slot, (target, who) in enumerate(near):
        for piece in range(3):
            where = landing(piece, who, core)
            remote(where, where, send_sem.at[0], w_sem.at[slot * 3 + piece], partner).wait_recv()
        rows = w_own.at[pl.ds(pl.multiple_of(who * depth + core * half, half), half)]
        copy = remote(rows, rows, send_sem.at[12 + slot], pair_sem.at[slot], partner)
        copy.start()
        sends.append(copy)
    for slot, (target, who) in enumerate(near):
        rows = w_own.at[pl.ds(pl.multiple_of(who * depth + (1 - core) * half, half), half)]
        remote(rows, rows, send_sem.at[0], pair_sem.at[slot], partner).wait_recv()
        rows = x_all.at[pl.ds(pl.multiple_of(who * tok, tok), tok)]
        remote(rows, rows, send_sem.at[0], x_sem.at[slot], partner).wait_recv()
    mine.wait()
    keep.wait()
    for copy in sends:
        copy.wait_send()


def start_exchange(block_in, weight, collective_id):
    tok, width = block_in.shape
    depth, columns = weight.shape
    return pl.pallas_call(
        start_kernel,
        out_shape=[
            jax.ShapeDtypeStruct((tok * 4, width), block_in.dtype),
            jax.ShapeDtypeStruct((depth * 4, columns // 4), weight.dtype),
        ],
        in_specs=[
            pl.BlockSpec(memory_space=pltpu.VMEM),
            pl.BlockSpec(memory_space=pltpu.HBM),
        ],
        out_specs=[pl.BlockSpec(memory_space=pltpu.HBM)] * 2,
        scratch_shapes=[
            pltpu.VMEM((depth, columns // 4), weight.dtype),
            pltpu.SemaphoreType.DMA((16,)),
            pltpu.SemaphoreType.DMA((3,)),
            pltpu.SemaphoreType.DMA((9,)),
            pltpu.SemaphoreType.DMA((3,)),
            pltpu.SemaphoreType.DMA((5,)),
        ],
        compiler_params=pltpu.CompilerParams(
            collective_id=collective_id, has_side_effects=True, vmem_limit_bytes=40 << 20
        ),
        name="start_exchange",
    )(block_in, weight)


def spread_kernel(x_ref, x_all, send_sem, x_sem, own_sem):
    tok = x_ref.shape[0]
    z, core, y, x = place()
    me = y * 2 + x
    near = others()
    greet([(None, target) for target, _ in near])
    sends = []
    rows = x_all.at[pl.ds(pl.multiple_of(me * tok, tok), tok)]
    for slot, (target, _) in enumerate(near):
        copy = remote(x_ref, rows, send_sem.at[slot], x_sem.at[slot], target)
        copy.start()
        sends.append(copy)
    mine = pltpu.make_async_copy(x_ref, rows, own_sem)
    mine.start()
    for slot, (target, who) in enumerate(near):
        rows = x_all.at[pl.ds(pl.multiple_of(who * tok, tok), tok)]
        remote(rows, rows, send_sem.at[0], x_sem.at[slot], target).wait_recv()
    mine.wait()
    for copy in sends:
        copy.wait_send()


def spread_sequence(rows, collective_id):
    tok, width = rows.shape
    return pl.pallas_call(
        spread_kernel,
        out_shape=jax.ShapeDtypeStruct((tok * 4, width), rows.dtype),
        in_specs=[pl.BlockSpec(memory_space=pltpu.VMEM)],
        out_specs=pl.BlockSpec(memory_space=pltpu.HBM),
        scratch_shapes=[
            pltpu.SemaphoreType.DMA((3,)),
            pltpu.SemaphoreType.DMA((3,)),
            pltpu.SemaphoreType.DMA,
        ],
        compiler_params=pltpu.CompilerParams(
            collective_id=collective_id, has_side_effects=True, vmem_limit_bytes=40 << 20
        ),
        name="spread_sequence",
    )(rows)


def fold_kernel(part_ref, out_ref, landing, send_sem, recv_sem):
    tok = out_ref.shape[0]
    z, core, y, x = place()
    me = y * 2 + x
    near = others()
    greet([(None, target) for target, _ in near])
    sends = []
    for slot, (target, who) in enumerate(near):
        copy = remote(
            part_ref.at[pl.ds(pl.multiple_of(who * tok, tok), tok)],
            landing.at[slot],
            send_sem.at[slot],
            recv_sem.at[slot],
            target,
        )
        copy.start()
        sends.append(copy)
    for slot, (target, _) in enumerate(near):
        remote(
            landing.at[slot], landing.at[slot], send_sem.at[0], recv_sem.at[slot], target
        ).wait_recv()

    @pl.loop(0, tok // 16)
    def _(i):
        where = pl.ds(pl.multiple_of(i * 16, 16), 16)
        total = part_ref[pl.ds(pl.multiple_of(me * tok + i * 16, 16), 16)].astype(jnp.float32)
        for slot in range(3):
            total += landing[slot, where].astype(jnp.float32)
        out_ref[where] = total

    for copy in sends:
        copy.wait_send()


def fold_sequence(part, collective_id):
    total, width = part.shape
    tok = total // 4
    return pl.pallas_call(
        fold_kernel,
        out_shape=jax.ShapeDtypeStruct((tok, width), jnp.float32),
        in_specs=[pl.BlockSpec(memory_space=pltpu.VMEM)],
        out_specs=pl.BlockSpec(memory_space=pltpu.VMEM),
        scratch_shapes=[
            pltpu.VMEM((3, tok, width), part.dtype),
            pltpu.SemaphoreType.DMA((3,)),
            pltpu.SemaphoreType.DMA((3,)),
        ],
        compiler_params=pltpu.CompilerParams(
            collective_id=collective_id, has_side_effects=True, vmem_limit_bytes=40 << 20
        ),
        name="fold_sequence",
    )(part)


def expert_kernel(
    slots_ref,
    gates_ref,
    x_ref,
    g_ref,
    w_ref,
    out_ref,
    grad_ref,
    gg_ref,
    grad_w,
    xs,
    gs,
    weighted,
    sums,
    sem,
):
    step = pl.program_id(0)
    blocks = x_ref.shape[0] // 128
    cap = xs.shape[0] // blocks

    @pl.when(step == 0)
    def _():
        sums[...] = jnp.zeros_like(sums)

    def dot(left, right, dims):
        return lax.dot_general(
            left, right, ((dims[:1], dims[1:]), ((), ())), preferred_element_type=jnp.float32
        )

    chosen, gate_rows = [], []
    for pair in range(blocks // 2):
        slot_row = jnp.concatenate(
            [
                slots_ref[pl.ds(step * blocks + pair * 2, 1), :],
                slots_ref[pl.ds(step * blocks + pair * 2 + 1, 1), :] + float(cap),
            ],
            axis=1,
        )
        gate_row = jnp.concatenate(
            [gates_ref[pl.ds(step * blocks + pair * 2 + j, 1), :] for j in range(2)], axis=1
        )
        ids = lax.broadcasted_iota(jnp.int32, (2 * cap, 256), 0).astype(jnp.float32)
        mask = jnp.where(ids == slot_row, 1.0, 0.0)
        pick = mask.astype(jnp.bfloat16)
        rows = pl.ds(pair * 2 * cap, 2 * cap)
        tokens = pl.ds(pair * 256, 256)
        gate = jnp.sum(mask * gate_row, axis=1, keepdims=True)
        xs[rows] = dot(pick, x_ref[tokens], (1, 0)).astype(jnp.bfloat16)
        upstream = dot(pick, g_ref[tokens], (1, 0))
        gs[rows] = upstream.astype(jnp.bfloat16)
        weighted[rows] = (upstream * gate).astype(jnp.bfloat16)
        chosen.append(pick)
        gate_rows.append(gate)
    rows_x = xs[...]
    rows_g = weighted[...]
    gate_pre = dot(rows_x, w_ref[0], (1, 0))
    up_pre = dot(rows_x, w_ref[1], (1, 0))
    sig = jax.nn.sigmoid(gate_pre)
    silu = gate_pre * sig
    hidden = (silu * up_pre).astype(jnp.bfloat16)
    grad_hidden = dot(rows_g, w_ref[2], (1, 0))
    grad_gate = (grad_hidden * up_pre * sig * (1.0 + gate_pre * (1.0 - sig))).astype(jnp.bfloat16)
    grad_up = (grad_hidden * silu).astype(jnp.bfloat16)
    result = dot(hidden, w_ref[2], (1, 1)).astype(jnp.bfloat16)
    grad_in = (dot(grad_gate, w_ref[0], (1, 1)) + dot(grad_up, w_ref[1], (1, 1))).astype(
        jnp.bfloat16
    )
    sums[0] += dot(rows_x, grad_gate, (0, 0))
    sums[1] += dot(rows_x, grad_up, (0, 0))
    sums[2] += dot(rows_g, hidden, (0, 0))
    result_f = result.astype(jnp.float32)
    along = jnp.sum(gs[...].astype(jnp.float32) * result_f, axis=1, keepdims=True)
    for pair in range(blocks // 2):
        tokens = pl.ds(pair * 256, 256)
        low, high = pair * 2 * cap, (pair + 1) * 2 * cap
        pick = chosen[pair]
        scaled = (result_f[low:high] * gate_rows[pair]).astype(jnp.bfloat16)
        out_ref[tokens] = dot(pick, scaled, (0, 0)).astype(jnp.bfloat16)
        grad_ref[tokens] = dot(pick, grad_in[low:high], (0, 0)).astype(jnp.bfloat16)
        row = jnp.sum(pick.astype(jnp.float32) * along[low:high], axis=0, keepdims=True)
        for j in range(2):
            gg_ref[pl.ds(step * blocks + pair * 2 + j, 1), :] = row[:, j * 128 : (j + 1) * 128]

    @pl.when(step == pl.num_programs(0) - 1)
    def _():
        copy = pltpu.make_async_copy(sums, grad_w.at[0], sem)
        copy.start()
        copy.wait()


def run_expert(slots, gates, tokens, upstream, weights, cap):
    count, width = tokens.shape
    _, three, _, ff = weights.shape
    group = 512
    steps = count // group
    held = group // 128 * cap
    whole = lambda i: (0, 0)
    return pl.pallas_call(
        expert_kernel,
        grid=(steps,),
        out_shape=[
            jax.ShapeDtypeStruct((count, width), jnp.bfloat16),
            jax.ShapeDtypeStruct((count, width), jnp.bfloat16),
            jax.ShapeDtypeStruct(slots.shape, jnp.float32),
            jax.ShapeDtypeStruct(weights.shape, jnp.float32),
        ],
        in_specs=[
            pl.BlockSpec(slots.shape, whole),
            pl.BlockSpec(gates.shape, whole),
            pl.BlockSpec((group, width), lambda i: (i, 0)),
            pl.BlockSpec((group, width), lambda i: (i, 0)),
            pl.BlockSpec(
                (None, three, width, ff), lambda i: (0, 0, 0, 0), pipeline_mode=pl.Buffered(1)
            ),
        ],
        out_specs=[
            pl.BlockSpec((group, width), lambda i: (i, 0)),
            pl.BlockSpec((group, width), lambda i: (i, 0)),
            pl.BlockSpec(slots.shape, whole),
            pl.BlockSpec(memory_space=pltpu.HBM),
        ],
        scratch_shapes=[
            pltpu.VMEM((held, width), jnp.bfloat16),
            pltpu.VMEM((held, width), jnp.bfloat16),
            pltpu.VMEM((held, width), jnp.bfloat16),
            pltpu.VMEM((three, width, ff), jnp.float32),
            pltpu.SemaphoreType.DMA,
        ],
        compiler_params=pltpu.CompilerParams(vmem_limit_bytes=63 << 20),
        name="run_expert",
    )(slots, gates, tokens, upstream, weights)


def split_body(
    block_in,
    segments,
    routes,
    attn_gain,
    query_key_value_weight,
    q_gain,
    k_gain,
    w_out,
    ffn_gain,
    router,
    expert_weights,
    cotangent,
):
    tok, width = block_in.shape
    seq = segments.shape[0]
    experts = router.shape[1]
    capacity = tok * routes.shape[1] * 2 // experts
    heads = QUERY_HEADS // 4
    both = ("rep", "shard")
    upstream_all = lax.all_gather(cotangent, both, axis=0, tiled=True)
    x_all, weight = start_exchange(block_in, query_key_value_weight, 0)

    mask = jnp.any(
        routes[:, :, None] == jnp.arange(experts, dtype=jnp.int32)[None, None, :], axis=1
    )
    mask_f = mask.astype(jnp.float32)
    earlier = (jnp.arange(tok)[:, None] > jnp.arange(tok)[None, :]).astype(jnp.bfloat16)
    slot = jnp.dot(earlier, mask.astype(jnp.bfloat16), preferred_element_type=jnp.float32)
    slot_table = jnp.where(mask, slot, -4096.0).T

    inputs_all = x_all.astype(jnp.float32)
    normed_one = (inputs_all * rms_scale(inputs_all) * attn_gain).astype(jnp.bfloat16)
    query_key_value = jnp.dot(normed_one, weight, preferred_element_type=jnp.float32)
    q_raw = query_key_value[:, : heads * HEAD_SIZE].reshape(seq, heads, HEAD_SIZE)
    k_raw = query_key_value[:, heads * HEAD_SIZE : (heads + 1) * HEAD_SIZE].reshape(
        seq, 1, HEAD_SIZE
    )
    values = query_key_value[:, (heads + 1) * HEAD_SIZE :].reshape(seq, 1, HEAD_SIZE)
    values = values.astype(jnp.bfloat16)
    positions = jnp.arange(seq, dtype=jnp.int32)
    cosine, sine = rope_tables(positions)
    q_scale, q_rot = norm_rope(q_raw, q_gain, cosine, sine)
    k_scale, k_rot = norm_rope(k_raw, k_gain, cosine, sine)
    allowed = (segments[:, None] == segments[None, :]) & (positions[None, :] <= positions[:, None])
    attended_f, lse = attend_forward(q_rot, k_rot, values, allowed)
    attended = attended_f.astype(jnp.bfloat16)
    partial = jnp.dot(attended, w_out, preferred_element_type=jnp.float32).astype(jnp.bfloat16)
    inputs = block_in.astype(jnp.float32)
    middle = inputs + fold_sequence(partial, 1)
    scale_two = rms_scale(middle)
    normed_two = (middle * scale_two * ffn_gain).astype(jnp.bfloat16)
    logits = jnp.dot(normed_two, router, preferred_element_type=jnp.float32)
    weights = jax.nn.softmax(logits, axis=-1)
    picked = weights * mask_f
    total = jnp.sum(picked, axis=1, keepdims=True)
    gates = picked / total
    table = jnp.concatenate([gates.T, slot_table], axis=0)
    tokens_all, table_all = gather_all([normed_two, table], 2)
    expert = lax.axis_index(both)
    table_all = table_all.reshape(-1, 2, experts, tok)
    own = lax.dynamic_index_in_dim(table_all, expert, 2, keepdims=False)
    out_part, grad_part, gate_part, grad_experts = run_expert(
        own[:, 1], own[:, 0], tokens_all, upstream_all, expert_weights, capacity
    )
    grad_gates = lax.all_to_all(gate_part, both, split_axis=0, concat_axis=0, tiled=True).T
    grad_from_experts = reduce_all(grad_part, 3).astype(jnp.float32)
    expert_sum = reduce_all(out_part, 4).astype(jnp.float32)
    block_out = (middle + expert_sum).astype(jnp.bfloat16)

    upstream = cotangent.astype(jnp.float32)
    grad_picked = grad_gates / total - jnp.sum(grad_gates * picked, axis=1, keepdims=True) / (
        total * total
    )
    grad_weights = grad_picked * mask_f
    grad_logits = weights * (grad_weights - jnp.sum(grad_weights * weights, axis=1, keepdims=True))
    grad_from_router = jnp.dot(
        grad_logits, router.astype(jnp.float32).T, precision=lax.Precision.HIGHEST
    )
    grad_router = jnp.dot(
        normed_two.astype(jnp.float32).T, grad_logits, precision=lax.Precision.HIGHEST
    )
    grad_norm_two, grad_ffn_gain = rms_back(
        middle, scale_two, ffn_gain, grad_from_experts + grad_from_router
    )
    grad_middle = upstream + grad_norm_two
    grad_middle_all = spread_sequence(grad_middle.astype(jnp.bfloat16), 5)
    grad_out = lax.dot_general(
        attended, grad_middle_all, (((0,), (0,)), ((), ())), preferred_element_type=jnp.float32
    ).astype(jnp.bfloat16)
    grad_out = lax.psum(grad_out, "rep").astype(jnp.float32)
    grad_attended = jnp.dot(
        grad_middle_all, w_out.T, preferred_element_type=jnp.float32
    ).astype(jnp.bfloat16)
    grad_q_rot, grad_k_rot, grad_v = attend_backward(
        q_rot, k_rot, values, allowed, lse, attended, grad_attended
    )
    grad_q_raw, grad_q_gain = norm_rope_back(q_raw, q_scale, q_gain, cosine, sine, grad_q_rot)
    grad_k_raw, grad_k_gain = norm_rope_back(k_raw, k_scale, k_gain, cosine, sine, grad_k_rot)
    grad_qkv_b = jnp.concatenate(
        [grad_q_raw.reshape(seq, -1), grad_k_raw.reshape(seq, -1), grad_v.reshape(seq, -1)], axis=1
    ).astype(jnp.bfloat16)
    grad_norm_one = fold_sequence(
        jnp.dot(grad_qkv_b, weight.T, preferred_element_type=jnp.float32).astype(jnp.bfloat16), 6
    )
    grad_weight = lax.dot_general(
        normed_one, grad_qkv_b, (((0,), (0,)), ((), ())), preferred_element_type=jnp.float32
    ).astype(jnp.bfloat16)
    grad_weight = lax.all_to_all(
        grad_weight.reshape(4, -1, grad_weight.shape[1]), "shard", split_axis=0, concat_axis=0, tiled=True
    )
    grad_weight = lax.psum(grad_weight, "rep").astype(jnp.float32)
    cut = heads * HEAD_SIZE
    depth = grad_weight.shape[1]
    grad_qkv = jnp.concatenate(
        [
            grad_weight[:, :, low:high].transpose(1, 0, 2).reshape(depth, -1)
            for low, high in ((0, cut), (cut, cut + HEAD_SIZE), (cut + HEAD_SIZE, cut + 2 * HEAD_SIZE))
        ],
        axis=1,
    )
    grad_inputs, grad_attn_gain = rms_back(inputs, rms_scale(inputs), attn_gain, grad_norm_one)
    grad_input = (grad_middle + grad_inputs).astype(jnp.bfloat16)
    grad_attn_gain, grad_q_gain, grad_k_gain, grad_ffn_gain, grad_router = lax.psum(
        (grad_attn_gain, grad_q_gain, grad_k_gain, grad_ffn_gain, grad_router), both
    )
    return (
        block_out,
        grad_input,
        grad_attn_gain,
        grad_qkv,
        grad_q_gain,
        grad_k_gain,
        grad_out,
        grad_ffn_gain,
        grad_router,
        grad_experts,
    )


def solution(mesh):
    placed = (
        P(("rep", "shard"), None),
        P("rep"),
        P(("rep", "shard"), None),
        P(),
        P("shard", None),
        P(),
        P(),
        P("shard", None),
        P(),
        P(),
        P(("rep", "shard"), None, None, None),
        P(("rep", "shard"), None),
    )
    body = split_body if dict(mesh.shape) == {"rep": 8, "shard": 4} else plain_body
    return jax.shard_map(
        body,
        mesh=mesh,
        in_specs=placed,
        out_specs=(
            P(("rep", "shard"), None),
            P(("rep", "shard"), None),
            P(),
            P("shard", None),
            P(),
            P(),
            P("shard", None),
            P(),
            P(),
            P(("rep", "shard"), None, None, None),
        ),
        check_vma=False,
    )
```

```python
import functools

import jax
import jax.numpy as jnp
from jax import lax
from jax.experimental import pallas as pl
from jax.experimental.pallas import tpu as pltpu
from jax.sharding import PartitionSpec as P


QUERY_HEADS = 32
KEY_VALUE_HEADS = 4
HEAD_SIZE = 128


epsilon = 1e-06
rope_base = 1000000.0


def product(form, left, right):
    return jnp.einsum(form, left, right, preferred_element_type=jnp.float32)


def rms_scale(values):
    return lax.rsqrt(jnp.mean(values * values, axis=-1, keepdims=True) + epsilon)


def rms_back(values, scale, gain, upstream):
    scaled = upstream * gain
    cube = scale * scale * scale
    grad_values = scale * scaled - values * cube * jnp.mean(scaled * values, axis=-1, keepdims=True)
    grad_gain = jnp.sum((upstream * values * scale).reshape(-1, values.shape[-1]), axis=0)
    return (grad_values, grad_gain)


def rope_tables(positions):
    half = HEAD_SIZE // 2
    freq = rope_base ** (-jnp.arange(half).astype(jnp.float32) * 2.0 / HEAD_SIZE)
    angles = positions.astype(jnp.float32)[:, None] * freq[None, :]
    cosine = jnp.concatenate([jnp.cos(angles), jnp.cos(angles)], axis=-1)
    sine = jnp.concatenate([jnp.sin(angles), jnp.sin(angles)], axis=-1)
    return (cosine[:, None, :], sine[:, None, :])


def rotate(values):
    half = values.shape[-1] // 2
    return jnp.concatenate([-values[..., half:], values[..., :half]], axis=-1)


def rotate_back(values):
    half = values.shape[-1] // 2
    return jnp.concatenate([values[..., half:], -values[..., :half]], axis=-1)


def split_heads(query_key_value):
    token_rows = query_key_value.shape[0]
    q_raw = query_key_value[:, : QUERY_HEADS * HEAD_SIZE].reshape(
        token_rows, QUERY_HEADS, HEAD_SIZE
    )
    unrotated_key = query_key_value[
        :, QUERY_HEADS * HEAD_SIZE : (QUERY_HEADS + KEY_VALUE_HEADS) * HEAD_SIZE
    ].reshape(token_rows, KEY_VALUE_HEADS, HEAD_SIZE)
    projected_value = query_key_value[:, (QUERY_HEADS + KEY_VALUE_HEADS) * HEAD_SIZE :].reshape(
        token_rows, KEY_VALUE_HEADS, HEAD_SIZE
    )
    return (q_raw, unrotated_key, projected_value)


def norm_rope(raw, gain, cosine, sine):
    scale = rms_scale(raw)
    normed = raw * scale * gain
    return (scale, (normed * cosine + rotate(normed) * sine).astype(jnp.bfloat16))


def norm_rope_back(raw, scale, gain, cosine, sine, grad_rot):
    grad_normed = grad_rot * cosine + rotate_back(grad_rot * sine)
    return rms_back(raw, scale, gain, grad_normed)


def split_groups(values, groups):
    token_rows, heads, width = values.shape
    return values.reshape(token_rows, groups, heads // groups, width).transpose(1, 0, 2, 3)


def attend_forward(queries, keys, values, allowed):
    groups = keys.shape[1]
    token_rows = queries.shape[0]
    scale = queries.shape[2] ** (-0.5)

    def one_group(operands):
        q_part, k_part, v_part = operands
        scores = jnp.where(allowed[None], product("tpd,sd->pts", q_part, k_part) * scale, -1e30)
        highest = jnp.max(scores, axis=2, keepdims=True)
        lse = highest + jnp.log(jnp.sum(jnp.exp(scores - highest), axis=2, keepdims=True))
        probs = jnp.exp(scores - lse).astype(jnp.bfloat16)
        return (product("pts,sd->tpd", probs, v_part), lse[:, :, 0])

    outputs, lse = lax.map(
        one_group,
        (split_groups(queries, groups), keys.transpose(1, 0, 2), values.transpose(1, 0, 2)),
    )
    return (outputs.transpose(1, 0, 2, 3).reshape(token_rows, -1), lse)


def attend_backward(queries, keys, values, allowed, lse, attended, grad_attended):
    groups = keys.shape[1]
    token_rows, heads, width = queries.shape
    scale = width ** (-0.5)

    def one_group(operands):
        q_part, k_part, v_part, lse_part, out_part, grad_part = operands
        scores = jnp.where(allowed[None], product("tpd,sd->pts", q_part, k_part) * scale, -1e30)
        probs = jnp.exp(scores - lse_part[:, :, None])
        grad_v = product("pts,tpd->sd", probs.astype(jnp.bfloat16), grad_part)
        grad_p = product("tpd,sd->pts", grad_part, v_part)
        delta = jnp.sum(
            out_part.astype(jnp.float32) * grad_part.astype(jnp.float32), axis=2
        ).transpose(1, 0)
        grad_score = (probs * (grad_p - delta[:, :, None]) * scale).astype(jnp.bfloat16)
        return (
            product("pts,sd->tpd", grad_score, k_part),
            product("pts,tpd->sd", grad_score, q_part),
            grad_v,
        )

    shaped_out = split_groups(attended.reshape(token_rows, heads, width), groups)
    shaped_grad = split_groups(grad_attended.reshape(token_rows, heads, width), groups)
    grad_q, grad_k, grad_v = lax.map(
        one_group,
        (
            split_groups(queries, groups),
            keys.transpose(1, 0, 2),
            values.transpose(1, 0, 2),
            lse,
            shaped_out,
            shaped_grad,
        ),
    )
    return (
        grad_q.transpose(1, 0, 2, 3).reshape(token_rows, heads, width),
        grad_k.transpose(1, 0, 2),
        grad_v.transpose(1, 0, 2),
    )


def route_gates(normed, router, routes):
    logits = jnp.dot(normed, router, preferred_element_type=jnp.float32)
    weights = jax.nn.softmax(logits, axis=-1)
    chosen = (
        routes[:, :, None] == jnp.arange(router.shape[1], dtype=jnp.int32)[None, None, :]
    ).astype(jnp.float32)
    picked = jnp.sum(chosen * weights[:, None, :], axis=2)
    total = jnp.sum(picked, axis=1, keepdims=True)
    return (weights, chosen, picked, total, picked / total)


def route_gates_back(normed, router, weights, chosen, picked, total, grad_gates):
    grad_picked = grad_gates / total - jnp.sum(grad_gates * picked, axis=1, keepdims=True) / (
        total * total
    )
    grad_weights = jnp.sum(chosen * grad_picked[:, :, None], axis=1)
    grad_logits = weights * (grad_weights - jnp.sum(grad_weights * weights, axis=1, keepdims=True))
    grad_normed = jnp.dot(
        grad_logits, router.astype(jnp.float32).T, precision=lax.Precision.HIGHEST
    )
    grad_router = jnp.dot(
        normed.astype(jnp.float32).T, grad_logits, precision=lax.Precision.HIGHEST
    )
    return (grad_normed, grad_router)


def route_index(routes, experts, capacity):
    flat = routes.reshape(-1)
    onehot = (flat[:, None] == jnp.arange(experts, dtype=jnp.int32)[None, :]).astype(jnp.int32)
    before = jnp.cumsum(onehot, axis=0) - onehot
    return flat * capacity + jnp.sum(before * onehot, axis=1)


def dispatch(rows_per_route, index, experts, capacity):
    width = rows_per_route.shape[1]
    empty = jnp.zeros((experts * capacity, width), rows_per_route.dtype)
    return empty.at[index].set(rows_per_route).reshape(experts, capacity, width)


def collect(buffer, index):
    return buffer.reshape(-1, buffer.shape[-1])[index]


def expert_forward(inputs, weights):
    gate_pre = product("ecd,edf->ecf", inputs, weights[:, 0])
    up_pre = product("ecd,edf->ecf", inputs, weights[:, 1])
    hidden = (jax.nn.silu(gate_pre) * up_pre).astype(jnp.bfloat16)
    result = product("ecf,edf->ecd", hidden, weights[:, 2]).astype(jnp.bfloat16)
    return (gate_pre, up_pre, hidden, result)


def expert_backward(weights, gate_pre, up_pre, grad_result):
    grad_hidden = product("ecd,edf->ecf", grad_result, weights[:, 2])
    sig = jax.nn.sigmoid(gate_pre)
    grad_gate = (grad_hidden * up_pre * sig * (1.0 + gate_pre * (1.0 - sig))).astype(jnp.bfloat16)
    grad_up = (grad_hidden * gate_pre * sig).astype(jnp.bfloat16)
    grad_inputs = product("ecf,edf->ecd", grad_gate, weights[:, 0]) + product(
        "ecf,edf->ecd", grad_up, weights[:, 1]
    )
    return (grad_gate, grad_up, grad_inputs.astype(jnp.bfloat16))


def expert_weight_grads(inputs, hidden, grad_gate, grad_up, grad_result):
    return jnp.stack(
        [
            product("ecd,ecf->edf", inputs, grad_gate),
            product("ecd,ecf->edf", inputs, grad_up),
            product("ecd,ecf->edf", grad_result, hidden),
        ],
        axis=1,
    )


def plain_body(
    block_in,
    segments,
    routes,
    attn_gain,
    query_key_value_weight,
    q_gain,
    k_gain,
    w_out,
    ffn_gain,
    router,
    expert_weights,
    cotangent,
):
    tok = block_in.shape[0]
    width = block_in.shape[1]
    top = routes.shape[1]
    rep_count = lax.axis_size("rep")
    shard_count = lax.axis_size("shard")
    experts = expert_weights.shape[0] * rep_count * shard_count
    capacity = tok * top * 2 // experts
    shard_pos = lax.axis_index("shard")
    qkv_whole, out_whole = (
        lax.all_gather(query_key_value_weight, "shard", axis=0, tiled=True),
        lax.all_gather(w_out, "shard", axis=0, tiled=True),
    )
    inputs = block_in.astype(jnp.float32)
    scale_one = rms_scale(inputs)
    normed_one = (inputs * scale_one * attn_gain).astype(jnp.bfloat16)
    query_key_value = jnp.dot(normed_one, qkv_whole, preferred_element_type=jnp.float32)
    q_raw, unrotated_key, projected_value = split_heads(query_key_value)
    positions = shard_pos * tok + jnp.arange(tok, dtype=jnp.int32)
    cosine, sine = rope_tables(positions)
    q_scale, q_rot = norm_rope(q_raw, q_gain, cosine, sine)
    k_scale, k_rot = norm_rope(unrotated_key, k_gain, cosine, sine)
    keys_all, values_all = (
        lax.all_gather(k_rot, "shard", axis=0, tiled=True),
        lax.all_gather(projected_value.astype(jnp.bfloat16), "shard", axis=0, tiled=True),
    )
    query_seg = lax.dynamic_slice_in_dim(segments, shard_pos * tok, tok)
    key_pos = jnp.arange(segments.shape[0], dtype=jnp.int32)
    allowed = (query_seg[:, None] == segments[None, :]) & (key_pos[None, :] <= positions[:, None])
    attended_f, lse = attend_forward(q_rot, keys_all, values_all, allowed)
    attended = attended_f.astype(jnp.bfloat16)
    middle = inputs + jnp.dot(attended, out_whole, preferred_element_type=jnp.float32)
    scale_two = rms_scale(middle)
    normed_two = (middle * scale_two * ffn_gain).astype(jnp.bfloat16)
    weights, chosen, picked, total, gates = route_gates(normed_two, router, routes)
    index = route_index(routes, experts, capacity)
    upstream = cotangent.astype(jnp.float32)
    grad_rows = (
        (gates[:, :, None] * upstream[:, None, :]).astype(jnp.bfloat16).reshape(tok * top, width)
    )
    paired = jnp.concatenate([jnp.repeat(normed_two, top, axis=0), grad_rows], axis=1)
    buffer = dispatch(paired, index, experts, capacity)
    received = lax.all_to_all(buffer, ("rep", "shard"), split_axis=0, concat_axis=1, tiled=True)
    token_rows = received[:, :, :width]
    grads = received[:, :, width:]
    gate_pre, up_pre, hidden, result = expert_forward(token_rows, expert_weights)
    grad_gate, grad_up, grad_inner = expert_backward(expert_weights, gate_pre, up_pre, grads)
    grad_experts = expert_weight_grads(token_rows, hidden, grad_gate, grad_up, grads)
    outgoing = jnp.concatenate([result, grad_inner], axis=2)
    returned = lax.all_to_all(outgoing, ("rep", "shard"), split_axis=1, concat_axis=0, tiled=True)
    fetched = collect(returned, index).reshape(tok, top, 2 * width)
    expert_rows = fetched[:, :, :width].astype(jnp.float32)
    grad_from_experts = jnp.sum(fetched[:, :, width:].astype(jnp.float32), axis=1)
    block_out = (middle + jnp.sum(gates[:, :, None] * expert_rows, axis=1)).astype(jnp.bfloat16)
    grad_gates = jnp.sum(expert_rows * upstream[:, None, :], axis=2)
    grad_from_router, grad_router = route_gates_back(
        normed_two, router, weights, chosen, picked, total, grad_gates
    )
    grad_norm_two, grad_ffn_gain = rms_back(
        middle, scale_two, ffn_gain, grad_from_experts + grad_from_router
    )
    grad_middle = upstream + grad_norm_two
    grad_middle_b = grad_middle.astype(jnp.bfloat16)
    columns = attended
    grad_out = lax.psum_scatter(
        lax.dot_general(
            columns, grad_middle_b, (((0,), (0,)), ((), ())), preferred_element_type=jnp.float32
        ).astype(jnp.bfloat16),
        "shard",
        scatter_dimension=0,
        tiled=True,
    ).astype(jnp.float32)
    grad_attended = jnp.dot(grad_middle_b, out_whole.T, preferred_element_type=jnp.float32).astype(
        jnp.bfloat16
    )
    grad_q_rot, grad_k_all, grad_v_all = attend_backward(
        q_rot, keys_all, values_all, allowed, lse, attended, grad_attended
    )
    grad_k_rot, grad_v = (
        lax.psum_scatter(
            grad_k_all.astype(jnp.bfloat16), "shard", scatter_dimension=0, tiled=True
        ).astype(jnp.float32),
        lax.psum_scatter(
            grad_v_all.astype(jnp.bfloat16), "shard", scatter_dimension=0, tiled=True
        ).astype(jnp.float32),
    )
    grad_q_raw, grad_q_gain = norm_rope_back(q_raw, q_scale, q_gain, cosine, sine, grad_q_rot)
    grad_k_raw, grad_k_gain = norm_rope_back(
        unrotated_key, k_scale, k_gain, cosine, sine, grad_k_rot
    )
    grad_qkv_b = jnp.concatenate(
        [grad_q_raw.reshape(tok, -1), grad_k_raw.reshape(tok, -1), grad_v.reshape(tok, -1)], axis=1
    ).astype(jnp.bfloat16)
    columns = normed_one
    grad_qkv = lax.psum_scatter(
        lax.dot_general(
            columns, grad_qkv_b, (((0,), (0,)), ((), ())), preferred_element_type=jnp.float32
        ).astype(jnp.bfloat16),
        "shard",
        scatter_dimension=0,
        tiled=True,
    ).astype(jnp.float32)
    grad_norm_one = jnp.dot(grad_qkv_b, qkv_whole.T, preferred_element_type=jnp.float32)
    grad_inputs, grad_attn_gain = rms_back(inputs, scale_one, attn_gain, grad_norm_one)
    grad_input = (grad_middle + grad_inputs).astype(jnp.bfloat16)
    grad_attn_gain, grad_q_gain, grad_k_gain, grad_ffn_gain, grad_router = lax.psum(
        (grad_attn_gain, grad_q_gain, grad_k_gain, grad_ffn_gain, grad_router), ("rep", "shard")
    )
    grad_qkv, grad_out = (
        lax.psum(grad_qkv.astype(jnp.bfloat16), "rep").astype(jnp.float32),
        lax.psum(grad_out.astype(jnp.bfloat16), "rep").astype(jnp.float32),
    )
    return (
        block_out,
        grad_input,
        grad_attn_gain,
        grad_qkv,
        grad_q_gain,
        grad_k_gain,
        grad_out,
        grad_ffn_gain,
        grad_router,
        grad_experts,
    )


MESH_ID = pl.DeviceIdType.MESH
PLANES = 4


def place():
    rep, shard = lax.axis_index("rep"), lax.axis_index("shard")
    return rep // 2, rep % 2, shard // 2, shard % 2


def device(z, core, y, x):
    return (z * 2 + core, y * 2 + x)


def block_of(z, core, y, x):
    return (z * 2 + core) * 4 + y * 2 + x


def greet(targets):
    barrier = pltpu.get_barrier_semaphore()
    for condition, target in targets:
        if condition is None:
            pl.semaphore_signal(barrier, inc=1, device_id=target, device_id_type=MESH_ID)
        else:

            @pl.when(condition)
            def _():
                pl.semaphore_signal(barrier, inc=1, device_id=target, device_id_type=MESH_ID)

    peers = 0
    for condition, _ in targets:
        peers = peers + (1 if condition is None else condition.astype(jnp.int32))
    pl.semaphore_wait(barrier, peers)


def experts_kernel(
    x_ref,
    table_ref,
    upstream_ref,
    w_ref,
    x_all,
    table_all,
    out_ref,
    grad_ref,
    gg_ref,
    rows_out,
    hidden_out,
    gs,
    rows_hold,
    hidden_hold,
    x_hold,
    g_hold,
    t_hold,
    out_hold,
    grad_hold,
    send_sem,
    recv_sem,
    own_sem,
    load_sem,
    store_sem,
):
    ins, outs = (x_ref, table_ref), (x_all, table_all)
    rows = (x_ref.shape[0], table_ref.shape[0])
    count = len(ins)
    tok = rows[0]
    experts = rows[1] // 2
    z, core, y, x = place()
    partner = device(z, 1 - core, y, x)
    x_next, y_next = device(z, core, y, 1 - x), device(z, core, 1 - y, x)
    up, down = device(z + 1, core, y, x), device(z - 1, core, y, x)
    can_up, can_down = z < PLANES - 1, z > 0
    greet(
        [
            (None, partner),
            (None, x_next),
            (None, y_next),
            (can_up, up),
            (can_down, down),
        ]
    )
    tables = ((0, 1, 2, 3), (1, 0, 2, 3), (2, 3, 1, 0), (3, 2, 1, 0))
    order = [
        sum((z == level).astype(jnp.int32) * tables[level][n] for level in range(PLANES))
        for n in range(PLANES)
    ]
    pending, used = [], [0]

    def region(array, block, part):
        size = rows[array]
        if part is None:
            return pl.ds(pl.multiple_of(block * size, size), size)
        return pl.ds(pl.multiple_of(block * size + part * (size // 2), size // 2), size // 2)

    def copy_of(array, block, part, target, index, own=False):
        where = region(array, block, part)
        source = ins[array] if own else outs[array].at[where]
        return remote(
            source,
            outs[array].at[where],
            send_sem.at[array, index],
            recv_sem.at[array, block * 2 + (part or 0)],
            target,
        )

    def plan(block, part, target, condition=None, own=False):
        index = used[0]
        used[0] += 1

        def start():
            for array in range(count):
                copy_of(array, block, part, target, index, own).start()

        def finish():
            for array in range(count):
                copy_of(array, block, part, target, index, own).wait_send()

        pending.append((condition, finish))
        return lambda: start() if condition is None else pl.when(condition)(start)

    def arrived(block, part):
        for array in range(count):
            copy_of(array, block, part, partner, 0).wait_recv()

    own = block_of(z, core, y, x)
    for target, condition in (
        (up, can_up),
        (down, can_down),
        (x_next, None),
        (y_next, None),
        (partner, None),
    ):
        plan(own, None, target, condition, own=True)()
    locals_ = [
        pltpu.make_async_copy(ins[n], outs[n].at[region(n, own, None)], own_sem.at[n])
        for n in range(count)
    ]
    for copy in locals_:
        copy.start()

    def along(n):
        plane = order[n]
        block = block_of(plane, core, y, x)
        moves = [
            plan(block, None, up, jnp.logical_and(plane < z, can_up)),
            plan(block, None, down, jnp.logical_and(plane > z, can_down)),
            plan(block, None, x_next),
            plan(block, None, y_next),
            plan(block, None, partner),
        ]

        def run():
            arrived(block, None)
            for move in moves:
                move()

        return run

    def across(n):
        plane = order[n]
        from_x, from_y = block_of(plane, core, y, 1 - x), block_of(plane, core, 1 - y, x)
        moves = [
            plan(from_x, 1, y_next),
            plan(from_x, None, partner),
            plan(from_y, 0, x_next),
            plan(from_y, None, partner),
        ]

        def run():
            arrived(from_x, None)
            moves[0]()
            moves[1]()
            arrived(from_y, None)
            moves[2]()
            moves[3]()

        return run

    def diagonal(n):
        block = block_of(order[n], core, 1 - y, 1 - x)
        moves = [plan(block, part, partner) for part in range(2)]

        def run():
            for part in range(2):
                arrived(block, part)
                moves[part]()

        return run

    def paired(n):
        plane = order[n]

        def run():
            for where_y, where_x in ((y, x), (y, 1 - x), (1 - y, x)):
                arrived(block_of(plane, 1 - core, where_y, where_x), None)
            for part in range(2):
                arrived(block_of(plane, 1 - core, 1 - y, 1 - x), part)

        return run

    def settled():
        for copy in locals_:
            copy.wait()

    inside = jnp.logical_and(can_up, can_down)
    steps_along = [along(n) for n in range(1, PLANES)]

    def hop(n, condition):
        return lambda: pl.when(condition)(steps_along[n - 1])

    outside = jnp.logical_not(inside)
    work = (
        (across(0), steps_along[0], hop(2, inside), diagonal(0), settled),
        (across(1), hop(2, outside), hop(3, inside), paired(0)),
        (hop(3, outside), diagonal(1)),
        (across(2), paired(1)),
        (across(3), diagonal(2)),
        (diagonal(3), paired(2)),
        (),
        (paired(3),),
    )
    group = 4 * tok
    steps = len(work)
    cap = gs.shape[0] // 4
    me = block_of(z, core, y, x)

    def group_of(i):
        if isinstance(i, int):
            plane = order[i // 2]
        else:
            plane = sum((i // 2 == n).astype(jnp.int32) * order[n] for n in range(PLANES))
        return plane * 2 + (core + i % 2) % 2

    def group_rows(ref, i):
        return ref.at[pl.ds(pl.multiple_of(group_of(i) * group, group), group)]

    def load_g(i):
        return pltpu.make_async_copy(
            group_rows(upstream_ref, i), g_hold.at[i % 2], load_sem.at[i % 2]
        )

    def load_x(i):
        return pltpu.make_async_copy(group_rows(x_all, i), x_hold, load_sem.at[2])

    def load_t(i):
        size = 4 * rows[1]
        return pltpu.make_async_copy(
            table_all.at[pl.ds(pl.multiple_of(group_of(i) * size, size), size)],
            t_hold,
            load_sem.at[3],
        )

    def store(i):
        held = pl.ds(pl.multiple_of(i * 4 * cap, 4 * cap), 4 * cap)
        return [
            pltpu.make_async_copy(hold.at[i % 2], target, store_sem.at[n, i % 2])
            for n, (hold, target) in enumerate(
                (
                    (out_hold, group_rows(out_ref, i)),
                    (grad_hold, group_rows(grad_ref, i)),
                    (rows_hold, rows_out.at[:, held]),
                    (hidden_hold, hidden_out.at[:, held]),
                )
            )
        ]

    def dot(left, right, dims):
        return lax.dot_general(
            left, right, ((dims[:1], dims[1:]), ((), ())), preferred_element_type=jnp.float32
        )

    load_g(0).start()

    @pl.loop(0, steps)
    def _(i):
        for n in range(steps):
            if work[n]:

                @pl.when(i == n)
                def _():
                    for run in work[n]:
                        run()

        load_x(i).start()
        load_t(i).start()

        @pl.when(i + 1 < steps)
        def _():
            load_g(i + 1).start()

        @pl.when(i >= 2)
        def _():
            for copy in store(i - 2):
                copy.wait()

        load_t(i).wait()
        load_x(i).wait()
        load_g(i).wait()
        slot = i % 2
        chosen, gate_cols = [], []
        for pair in range(2):
            first = [(pair * 2 + j) * 2 * experts + me for j in range(2)]
            gate_row = jnp.concatenate([t_hold[pl.ds(at, 1), :] for at in first], axis=1)
            slot_row = jnp.concatenate(
                [
                    t_hold[pl.ds(at + experts, 1), :] + float(cap * j)
                    for j, at in enumerate(first)
                ],
                axis=1,
            )
            ids = lax.broadcasted_iota(jnp.int32, (2 * cap, 2 * tok), 0).astype(jnp.float32)
            mask = jnp.where(ids == slot_row, 1.0, 0.0)
            pick = mask.astype(jnp.bfloat16)
            held = pl.ds(pair * 2 * cap, 2 * cap)
            tokens = pl.ds(pair * 2 * tok, 2 * tok)
            gate = jnp.sum(mask * gate_row, axis=1, keepdims=True)
            rows_hold[slot, 0, held] = dot(pick, x_hold[tokens], (1, 0)).astype(jnp.bfloat16)
            upstream = dot(pick, g_hold[slot, tokens], (1, 0))
            gs[held] = upstream.astype(jnp.bfloat16)
            rows_hold[slot, 1, held] = (upstream * gate).astype(jnp.bfloat16)
            chosen.append(pick)
            gate_cols.append(gate)
        rows_x = rows_hold[slot, 0]
        rows_g = rows_hold[slot, 1]
        gate_pre = dot(rows_x, w_ref[0], (1, 0))
        up_pre = dot(rows_x, w_ref[1], (1, 0))
        sig = jax.nn.sigmoid(gate_pre)
        silu = gate_pre * sig
        hidden = (silu * up_pre).astype(jnp.bfloat16)
        grad_hidden = dot(rows_g, w_ref[2], (1, 0))
        grad_gate = (grad_hidden * up_pre * sig * (1.0 + gate_pre * (1.0 - sig))).astype(
            jnp.bfloat16
        )
        grad_up = (grad_hidden * silu).astype(jnp.bfloat16)
        result = dot(hidden, w_ref[2], (1, 1)).astype(jnp.bfloat16)
        grad_in = (dot(grad_gate, w_ref[0], (1, 1)) + dot(grad_up, w_ref[1], (1, 1))).astype(
            jnp.bfloat16
        )
        hidden_hold[slot, 0] = grad_gate
        hidden_hold[slot, 1] = grad_up
        hidden_hold[slot, 2] = hidden
        result_f = result.astype(jnp.float32)
        share = jnp.sum(gs[...].astype(jnp.float32) * result_f, axis=1, keepdims=True)
        for pair in range(2):
            tokens = pl.ds(pair * 2 * tok, 2 * tok)
            low, high = pair * 2 * cap, (pair + 1) * 2 * cap
            pick = chosen[pair]
            scaled = (result_f[low:high] * gate_cols[pair]).astype(jnp.bfloat16)
            out_hold[slot, tokens] = dot(pick, scaled, (0, 0)).astype(jnp.bfloat16)
            grad_hold[slot, tokens] = dot(pick, grad_in[low:high], (0, 0)).astype(jnp.bfloat16)
            row = jnp.sum(pick.astype(jnp.float32) * share[low:high], axis=0, keepdims=True)
            for j in range(2):
                gg_ref[pl.ds(group_of(i) * 4 + pair * 2 + j, 1), :] = row[
                    :, j * tok : (j + 1) * tok
                ]
        for copy in store(i):
            copy.start()

    for i in (steps - 2, steps - 1):
        for copy in store(i):
            copy.wait()
    for condition, finish in pending:
        if condition is None:
            finish()
        else:
            pl.when(condition)(finish)


def run_experts(tokens, table, upstream, weights, cap, collective_id):
    tok, width = tokens.shape
    _, three, _, ff = weights.shape
    devices = 32
    total = tok * devices
    held = 4 * cap
    group = 4 * tok
    return pl.pallas_call(
        experts_kernel,
        out_shape=[
            jax.ShapeDtypeStruct((total, width), tokens.dtype),
            jax.ShapeDtypeStruct((table.shape[0] * devices, tok), table.dtype),
            jax.ShapeDtypeStruct((total, width), jnp.bfloat16),
            jax.ShapeDtypeStruct((total, width), jnp.bfloat16),
            jax.ShapeDtypeStruct((devices, tok), jnp.float32),
            jax.ShapeDtypeStruct((2, 8 * held, width), jnp.bfloat16),
            jax.ShapeDtypeStruct((3, 8 * held, ff), jnp.bfloat16),
        ],
        in_specs=[
            pl.BlockSpec(memory_space=pltpu.VMEM),
            pl.BlockSpec(memory_space=pltpu.VMEM),
            pl.BlockSpec(memory_space=pltpu.HBM),
            pl.BlockSpec(memory_space=pltpu.VMEM),
        ],
        out_specs=[pl.BlockSpec(memory_space=pltpu.HBM)] * 4
        + [pl.BlockSpec(memory_space=pltpu.VMEM)]
        + [pl.BlockSpec(memory_space=pltpu.HBM)] * 2,
        scratch_shapes=[
            pltpu.VMEM((held, width), jnp.bfloat16),
            pltpu.VMEM((2, 2, held, width), jnp.bfloat16),
            pltpu.VMEM((2, 3, held, ff), jnp.bfloat16),
            pltpu.VMEM((group, width), jnp.bfloat16),
            pltpu.VMEM((2, group, width), jnp.bfloat16),
            pltpu.VMEM((4 * table.shape[0], tok), jnp.float32),
            pltpu.VMEM((2, group, width), jnp.bfloat16),
            pltpu.VMEM((2, group, width), jnp.bfloat16),
            pltpu.SemaphoreType.DMA((2, 44)),
            pltpu.SemaphoreType.DMA((2, 64)),
            pltpu.SemaphoreType.DMA((2,)),
            pltpu.SemaphoreType.DMA((4,)),
            pltpu.SemaphoreType.DMA((4, 2)),
        ],
        compiler_params=pltpu.CompilerParams(
            collective_id=collective_id, has_side_effects=True, vmem_limit_bytes=63 << 20
        ),
        name="run_experts",
    )(tokens, table, upstream, weights.reshape(three, width, ff))


def add_rows(target, sources, rows=128, step=16):
    @pl.loop(0, rows // step)
    def _(i):
        where = pl.ds(pl.multiple_of(i * step, step), step)
        total = target[where].astype(jnp.float32)
        for source in sources:
            total += source[where].astype(jnp.float32)
        target[where] = total.astype(target.dtype)


def rolled(values):
    return pltpu.roll(values, HEAD_SIZE // 2, 1)


def inverse_rms(values):
    return lax.rsqrt(jnp.mean(values * values, axis=1, keepdims=True) + epsilon)


def mm(left, right, dims):
    return lax.dot_general(
        left, right, ((dims[:1], dims[1:]), ((), ())), preferred_element_type=jnp.float32
    )


def fill_bias(bias, seg_col, seg_row):
    seq = bias.shape[0]
    key = lax.broadcasted_iota(jnp.int32, (seq, seq), 0)
    query = lax.broadcasted_iota(jnp.int32, (seq, seq), 1)
    same = seg_col[...] == seg_row[...]
    bias[...] = jnp.where(jnp.logical_and(same, key <= query), 0.0, -1e30)


def attend_kernel(
    x_ref,
    weight_ref,
    w_out_ref,
    gain_ref,
    q_gain_ref,
    k_gain_ref,
    cos_ref,
    sin_ref,
    seg_col,
    seg_row,
    normed_ref,
    raw_ref,
    q_ref,
    k_ref,
    v_ref,
    attended_ref,
    lse_ref,
    part_ref,
    bias,
):
    seq = x_ref.shape[0]
    size = HEAD_SIZE
    heads = q_ref.shape[1] // size
    scale = size ** (-0.5)

    @pl.loop(0, seq // 64)
    def _(n):
        rows = pl.ds(pl.multiple_of(n * 64, 64), 64)
        x = x_ref[rows].astype(jnp.float32)
        normed_ref[rows] = (x * inverse_rms(x) * gain_ref[...]).astype(jnp.bfloat16)

    fill_bias(bias, seg_col, seg_row)

    @pl.loop(0, raw_ref.shape[1] // 256)
    def _(n):
        columns = pl.ds(pl.multiple_of(n * 256, 256), 256)
        raw_ref[:, columns] = mm(normed_ref[...], weight_ref[:, columns], (1, 0))

    def turned(raw, gain_row):
        normed = raw * inverse_rms(raw) * gain_row
        return (normed * cos_ref[...] + rolled(normed) * sin_ref[...]).astype(jnp.bfloat16)

    k_ref[...] = turned(raw_ref[:, heads * size : (heads + 1) * size], k_gain_ref[...])
    v_ref[...] = raw_ref[:, (heads + 1) * size :].astype(jnp.bfloat16)
    half = seq // 2

    @pl.loop(0, heads)
    def _(h):
        columns = pl.ds(pl.multiple_of(h * size, size), size)
        q_ref[:, columns] = turned(raw_ref[:, columns], q_gain_ref[...])
        for first, keys in ((0, half), (half, seq)):
            queries = pl.ds(first, half)
            score = mm(k_ref[:keys], q_ref[queries, columns], (1, 1)) * scale
            score = score + bias[:keys, first : first + half]
            highest = jnp.max(score, axis=0, keepdims=True)
            power = jnp.exp(score - highest)
            total = jnp.sum(power, axis=0, keepdims=True)
            lse_ref[pl.ds(h, 1), queries] = highest + jnp.log(total)
            probs = (power * (1.0 / total)).astype(jnp.bfloat16)
            attended_ref[queries, columns] = mm(probs, v_ref[:keys], (0, 0)).astype(jnp.bfloat16)

    @pl.loop(0, part_ref.shape[1] // 512)
    def _(n):
        columns = pl.ds(pl.multiple_of(n * 512, 512), 512)
        part_ref[:, columns] = mm(attended_ref[...], w_out_ref[:, columns], (1, 0)).astype(
            jnp.bfloat16
        )


def attend(x, weight, w_out, gain, q_gain, k_gain, cosine, sine, segments):
    seq, width = x.shape
    columns = weight.shape[1]
    heads = w_out.shape[0] // HEAD_SIZE
    bf, f4 = jnp.bfloat16, jnp.float32
    out = jax.ShapeDtypeStruct
    return pl.pallas_call(
        attend_kernel,
        out_shape=[
            out((seq, width), bf),
            out((seq, columns), f4),
            out((seq, heads * HEAD_SIZE), bf),
            out((seq, HEAD_SIZE), bf),
            out((seq, HEAD_SIZE), bf),
            out((seq, heads * HEAD_SIZE), bf),
            out((heads, seq), f4),
            out((seq, width), bf),
        ],
        in_specs=[pl.BlockSpec(memory_space=pltpu.VMEM)] * 10,
        out_specs=[pl.BlockSpec(memory_space=pltpu.VMEM)] * 8,
        scratch_shapes=[pltpu.VMEM((seq, seq), f4)],
        compiler_params=pltpu.CompilerParams(vmem_limit_bytes=56 << 20),
        name="attend",
    )(
        x,
        weight,
        w_out,
        gain[None],
        q_gain[None],
        k_gain[None],
        cosine,
        sine,
        segments[:, None],
        segments[None],
    )


def backward_steps(refs):
    q_ref, k_ref, v_ref, raw_ref, upstream, lse_ref, delta_ref = refs[:7]
    q_gain_ref, k_gain_ref, cos_ref, sin_ref, seg_col, seg_row = refs[7:13]
    grad_ref, gains_ref, bias, grad_k, grad_v = refs[13:]
    seq, size = k_ref.shape
    heads = q_ref.shape[1] // size
    scale = size ** (-0.5)
    half = seq // 2

    def prepare():
        fill_bias(bias, seg_col, seg_row)
        grad_k[...] = jnp.zeros_like(grad_k)
        grad_v[...] = jnp.zeros_like(grad_v)
        gains_ref[...] = jnp.zeros_like(gains_ref)

    def turn_back(grad, queries, columns, gain, line):
        turned = grad * cos_ref[queries] + rolled(grad * sin_ref[queries])
        raw = raw_ref[queries, columns]
        inverse = inverse_rms(raw)
        scaled = turned * gain
        mean = jnp.mean(scaled * raw, axis=1, keepdims=True)
        grad_raw = inverse * scaled - raw * (inverse * inverse * inverse) * mean
        grad_ref[queries, columns] = grad_raw.astype(jnp.bfloat16)
        gains_ref[line : line + 1] += jnp.sum(turned * raw * inverse, axis=0, keepdims=True)

    def head(h):
        columns = pl.ds(h * size, size)
        for first, keys in ((0, half), (half, seq)):
            queries = pl.ds(first, half)
            q, above = q_ref[queries, columns], upstream[queries, columns]
            score = mm(k_ref[:keys], q, (1, 1)) * scale + bias[:keys, first : first + half]
            probs = jnp.exp(score - lse_ref[h : h + 1, first : first + half])
            grad_v[:keys] += mm(probs.astype(jnp.bfloat16), above, (1, 0))
            grad_p = mm(v_ref[:keys], above, (1, 1))
            delta = delta_ref[h : h + 1, first : first + half]
            grad_score = (probs * (grad_p - delta) * scale).astype(jnp.bfloat16)
            grad_k[:keys] += mm(grad_score, q, (1, 0))
            grad_q = mm(grad_score, k_ref[:keys], (0, 0))
            turn_back(grad_q, queries, columns, q_gain_ref[...], 0)

    def keys_and_values():
        for first in (0, half):
            queries = pl.ds(first, half)
            turn_back(grad_k[queries], queries, pl.ds(heads * size, size), k_gain_ref[...], 1)
        grad_ref[:, (heads + 1) * size :] = grad_v[...].astype(jnp.bfloat16)

    return [prepare] + [functools.partial(head, h) for h in range(heads)] + [keys_and_values]


class Sends:
    def __init__(self, send_sem, partner):
        self.send_sem, self.partner, self.used, self.pending = send_sem, partner, 0, []

    def make(self, source, landing, sem, target, *conditions):
        copy = remote(source, landing, self.send_sem.at[self.used], sem, target)
        self.used += 1
        self.pending.append((conditions, copy))
        return copy

    def send(self, source, landing, sem, target):
        self.make(source, landing, sem, target).start()

    def arrived(self, landing, sem):
        remote(landing, landing, self.send_sem.at[0], sem, self.partner).wait_recv()

    def finish(self):
        for conditions, copy in self.pending:
            if not conditions:
                copy.wait_send()
            elif len(conditions) == 1:
                pl.when(conditions[0])(copy.wait_send)
            else:
                pl.when(jnp.logical_and(*conditions))(copy.wait_send)


def add_into(target, sources, rows):
    @pl.loop(0, rows // 16)
    def _(n):
        where = pl.ds(pl.multiple_of(n * 16, 16), 16)
        total = sources[0][where].astype(jnp.float32)
        for source in sources[1:]:
            total += source[where].astype(jnp.float32)
        target[where] = total.astype(target.dtype)


def ladder(sends, count, before, piece, from_up, from_down, final, size, sems):
    climb_send, spread_send, close_send, climb_sem, spread_sem, close_sem = sems
    z, core, y, x = place()
    partner = sends.partner
    up, down = device(z + 1, core, y, x), device(z - 1, core, y, x)
    can_up, can_down = z < PLANES - 1, z > 0

    def climb(n, rising):
        landing = from_down(n) if rising else from_up(n)
        side = 1 if rising else 0
        return remote(
            piece(n), landing, climb_send.at[n], climb_sem.at[n, side], up if rising else down
        )

    def gained(n, rising):
        landing = from_down(n) if rising else from_up(n)
        sends.arrived(landing, climb_sem.at[n, 1 if rising else 0])
        return landing

    def spread(n, rising):
        block = final(n, core)
        target = up if rising else down
        return remote(block, block, spread_send.at[n, 1 if rising else 0], spread_sem.at[n], target)

    def hand_over(n):
        block = final(n, core)
        return remote(block, block, close_send.at[n], close_sem.at[n], partner)

    def ends(n, root):
        before(n)
        pl.when(z == 0)(climb(n, True).start)
        pl.when(z == PLANES - 1)(climb(n, False).start)

    def between(n, root):
        for rising, level in ((True, 1), (False, 2)):

            @pl.when(jnp.logical_and(z == level, root == 3 - level))
            def _():
                add_rows(piece(n), (gained(n, rising),), size)
                climb(n, rising).start()

    def settle(n, root):
        @pl.when(z == root)
        def _():
            add_into(final(n, core), (piece(n), gained(n, True), gained(n, False)), size)
            spread(n, True).start()
            spread(n, False).start()
            hand_over(n).start()

    def receive(n, root, distance):
        for rising, there, more in (
            (True, z == root + distance, can_up),
            (False, z == root - distance, can_down),
        ):

            @pl.when(there)
            def _():
                sends.arrived(final(n, core), spread_sem.at[n])
                pl.when(more)(spread(n, rising).start)
                hand_over(n).start()

    stages = (
        ends,
        between,
        settle,
        functools.partial(receive, distance=1),
        functools.partial(receive, distance=2),
    )

    def step(m):
        for stage, run in enumerate(stages):
            n = m - stage * SLACK

            @pl.when(jnp.logical_and(n >= 0, n < count))
            def _():
                run(n, 1 + n % 2)

    def close():
        @pl.loop(0, count)
        def _(n):
            root = 1 + n % 2
            pl.when(z != root)(climb(n, True).wait_send)
            pl.when(jnp.logical_and(z >= root, can_up))(spread(n, True).wait_send)
            pl.when(jnp.logical_and(z <= root, can_down))(spread(n, False).wait_send)
            hand_over(n).wait_send()

    def closed(n):
        sends.arrived(final(n, 1 - core), close_sem.at[n])

    return step, closed, close


SLACK = 2
LADDER_MORE = 4 * SLACK


def ladder_scratch(count):
    return [
        pltpu.SemaphoreType.DMA((count,)),
        pltpu.SemaphoreType.DMA((count, 2)),
        pltpu.SemaphoreType.DMA((count,)),
        pltpu.SemaphoreType.DMA((count, 2)),
        pltpu.SemaphoreType.DMA((count,)),
        pltpu.SemaphoreType.DMA((count,)),
    ]


LADDER = 32
PER = LADDER // 4


def reduce_kernel(with_weight, *refs):
    refs = list(refs)
    part_ref = refs.pop(0)
    weight_ref = refs.pop(0) if with_weight else None
    back = [refs.pop(0) for _ in range(13)] if with_weight else []
    rows_ref, hidden_ref = (None, None) if with_weight else (refs.pop(0), refs.pop(0))
    out_ref = refs.pop(0)
    weight_out = refs.pop(0) if with_weight else None
    grad_w = None if with_weight else refs.pop(0)
    back += [refs.pop(0) for _ in range(2)] if with_weight else []
    kept, paired, x_half, x_full, y_half, y_full, from_up, from_down = refs[:8]
    send_sem, pair_sem, x_sem, y_sem, z_sem, load_sem = refs[8:14]
    rows = out_ref.shape[0]
    half = rows // 2
    z, core, y, x = place()
    partner = device(z, 1 - core, y, x)
    x_next, y_next = device(z, core, y, 1 - x), device(z, core, 1 - y, x)
    up, down = device(z + 1, core, y, x), device(z - 1, core, y, x)
    greet(
        [
            (None, partner),
            (None, x_next),
            (None, y_next),
            (z < PLANES - 1, up),
            (z > 0, down),
        ]
    )
    sends = Sends(send_sem, partner)
    tables = ((3, 2, 1, 0), (3, 0, 2, 1), (0, 3, 1, 2), (0, 1, 2, 3))
    order = [
        sum((z == level).astype(jnp.int32) * tables[level][n] for level in range(PLANES))
        for n in range(PLANES)
    ]
    spots = ((1 - y, 1 - x), (y, 1 - x), (1 - y, x), (y, x))

    def slot(plane, spot):
        return plane * 4 + spots[spot][0] * 2 + spots[spot][1]

    def block(plane, which, spot):
        size = pl.multiple_of(block_of(plane, which, *spots[spot]) * rows, rows)
        return part_ref.at[pl.ds(size, rows)]

    def load(plane, spot):
        return pltpu.make_async_copy(
            block(plane, core, spot), kept.at[slot(plane, spot)], load_sem.at[spot * 4 + plane]
        )

    for spot in range(4):
        for plane in order:
            where = slot(plane, spot)
            sends.send(block(plane, 1 - core, spot), paired.at[where], pair_sem.at[where], partner)
            load(plane, spot).start()
    if with_weight:
        out_pair, out_part, out_up, out_down, out_done = refs[14:19]
        out_pair_sem, out_sem = refs[19:21]
        out_half = weight_ref.shape[0] // 2
        out_block = out_half // LADDER
        big = out_half // 4

        def out_rows(n, which, count=1):
            start = pl.multiple_of(which * out_half + n * out_block, out_block)
            return weight_ref.at[pl.ds(start, out_block * count)]

        for n in range(4):
            sends.send(out_rows(n * PER, 1 - core, PER), out_pair.at[n], out_pair_sem.at[n], partner)

        def before(n):
            @pl.when(n % PER == 0)
            def _():
                where = n // PER
                sends.arrived(out_pair.at[where], out_pair_sem.at[where])
                add_into(out_part.at[where], (out_rows(n, core, PER), out_pair.at[where]), big)

        def done_rows(n, which):
            start = pl.multiple_of(which * out_half + n * out_block, out_block)
            return out_done.at[pl.ds(start, out_block)]

        ladder_step, closed, close = ladder(
            sends,
            LADDER,
            before,
            lambda n: out_part.at[
                n // PER, pl.ds(pl.multiple_of((n % PER) * out_block, out_block), out_block)
            ],
            lambda n: out_up.at[n],
            lambda n: out_down.at[n],
            done_rows,
            out_block,
            refs[21:27],
        )
        fill = backward_steps(back + refs[27:])

    else:
        rows_hold, hidden_hold, sums, part_sem, sum_sem = refs[14:]
        held = rows_hold.shape[2]

        def fetch(i):
            span = pl.ds(i * held, held)
            return (
                pltpu.make_async_copy(
                    rows_ref.at[:, span], rows_hold.at[i % 2], part_sem.at[0, i % 2]
                ),
                pltpu.make_async_copy(
                    hidden_ref.at[:, span], hidden_hold.at[i % 2], part_sem.at[1, i % 2]
                ),
            )

        parts = rows_ref.shape[1] // held
        for copy in fetch(0):
            copy.start()

        def add_product(i):
            if i + 1 < parts:
                for copy in fetch(i + 1):
                    copy.start()
            for copy in fetch(i):
                copy.wait()
            for matrix, source in ((0, 0), (1, 0), (2, 1)):

                @pl.loop(0, sums.shape[1] // 512)
                def _(n):
                    span = pl.ds(pl.multiple_of(n * 512, 512), 512)
                    product = mm(
                        rows_hold[i % 2, source, :, span], hidden_hold[i % 2, matrix], (0, 0)
                    )
                    if i:
                        sums[matrix, span] += product
                    else:
                        sums[matrix, span] = product

        write_sums = pltpu.make_async_copy(sums, grad_w.at[0], sum_sem)

    def joined(plane, spot, more=()):
        where = slot(plane, spot)
        load(plane, spot).wait()
        sends.arrived(paired.at[where], pair_sem.at[where])
        add_rows(kept.at[where], (paired.at[where],) + tuple(more), rows)

    def across(plane):
        joined(plane, 0)
        source = kept.at[slot(plane, 0)]
        sends.send(source.at[pl.ds(0, half)], x_half.at[plane], x_sem.at[plane], x_next)
        sends.send(source.at[pl.ds(half, half)], y_half.at[plane], y_sem.at[plane], y_next)

    def beside(plane):
        joined(plane, 1)
        sends.arrived(y_half.at[plane], y_sem.at[plane])
        add_rows(kept.at[slot(plane, 1)].at[pl.ds(half, half)], (y_half.at[plane],), half)
        sends.send(kept.at[slot(plane, 1)], x_full.at[plane], x_sem.at[4 + plane], x_next)
        joined(plane, 2)
        sends.arrived(x_half.at[plane], x_sem.at[plane])
        add_rows(kept.at[slot(plane, 2)].at[pl.ds(0, half)], (x_half.at[plane],), half)
        sends.send(kept.at[slot(plane, 2)], y_full.at[plane], y_sem.at[4 + plane], y_next)

    def along(plane):
        sends.arrived(x_full.at[plane], x_sem.at[4 + plane])
        sends.arrived(y_full.at[plane], y_sem.at[4 + plane])
        joined(plane, 3, (x_full.at[plane], y_full.at[plane]))

    moves = {}

    def pass_on(n, first):
        plane = order[n]
        total = kept.at[slot(plane, 3)]
        if first:
            fall = sends.make(total, from_up.at[plane], z_sem.at[0, plane], down, z > plane)
            rise = sends.make(total, from_down.at[plane], z_sem.at[1, plane], up, z < plane)
            moves[n] = (fall, rise)
        fall, rise = moves[n]
        for copy, way, end, landing, sem in (
            (fall, z > plane, z == PLANES - 1, from_up.at[plane], z_sem.at[0, plane]),
            (rise, z < plane, z == 0, from_down.at[plane], z_sem.at[1, plane]),
        ):
            if first:
                pl.when(jnp.logical_and(way, end))(copy.start)
            else:

                @pl.when(jnp.logical_and(way, jnp.logical_not(end)))
                def _():
                    sends.arrived(landing, sem)
                    add_rows(total, (landing,), rows)
                    copy.start()

    total_steps = LADDER + LADDER_MORE
    done_steps = 0
    if with_weight:
        fill[0]()
    for late, run in enumerate((across, beside)):
        for n, plane in enumerate(order):
            run(plane)
            if not with_weight:
                add_product(late * PLANES + n)
            if with_weight:
                if run is across:
                    fill[1 + n]()
                more = min(-(-total_steps // (2 * PLANES)), total_steps - done_steps)

                @pl.loop(done_steps, done_steps + more)
                def _(m):
                    ladder_step(m)

                done_steps += more
    if not with_weight:
        write_sums.start()
    for n in range(PLANES):
        along(order[n])
        if n < PLANES - 1:
            pass_on(n, True)
        if n:
            pass_on(n - 1, False)
        if with_weight:
            fill[1 + PLANES + n]()
    if with_weight:
        fill[-1]()
    mine = kept.at[slot(z, 3)]

    @pl.when(z < PLANES - 1)
    def _():
        sends.arrived(from_up.at[z], z_sem.at[0, z])
        add_rows(mine, (from_up.at[z],), rows)

    @pl.when(z > 0)
    def _():
        sends.arrived(from_down.at[z], z_sem.at[1, z])
        add_rows(mine, (from_down.at[z],), rows)

    out_ref[...] = mine[...]
    if with_weight:

        @pl.loop(0, LADDER)
        def _(n):
            closed(n)

        write = pltpu.make_async_copy(out_done, weight_out, out_sem)
        write.start()
        close()
        write.wait()
    else:
        write_sums.wait()
    sends.finish()


def reduce_all(part, collective_id, weight=None, back=(), expert=()):
    total, width = part.shape
    rows = total // 32
    half = rows // 2
    dtype = part.dtype
    out_shape = [jax.ShapeDtypeStruct((rows, width), dtype)]
    in_specs = [pl.BlockSpec(memory_space=pltpu.HBM)]
    out_specs = [pl.BlockSpec(memory_space=pltpu.VMEM)]
    scratch = [
        pltpu.VMEM((16, rows, width), dtype),
        pltpu.VMEM((16, rows, width), dtype),
        pltpu.VMEM((4, half, width), dtype),
        pltpu.VMEM((4, rows, width), dtype),
        pltpu.VMEM((4, half, width), dtype),
        pltpu.VMEM((4, rows, width), dtype),
        pltpu.VMEM((4, rows, width), dtype),
        pltpu.VMEM((4, rows, width), dtype),
        pltpu.SemaphoreType.DMA((52,)),
        pltpu.SemaphoreType.DMA((16,)),
        pltpu.SemaphoreType.DMA((8,)),
        pltpu.SemaphoreType.DMA((8,)),
        pltpu.SemaphoreType.DMA((2, 4)),
        pltpu.SemaphoreType.DMA((16,)),
    ]
    operands = [part]
    if weight is not None:
        operands.append(weight)
        block = weight.shape[0] // 8
        seq = back[0].shape[0]
        operands += back
        out_shape += [
            jax.ShapeDtypeStruct(weight.shape, dtype),
            jax.ShapeDtypeStruct(back[3].shape, dtype),
            jax.ShapeDtypeStruct((8, HEAD_SIZE), jnp.float32),
        ]
        in_specs += [pl.BlockSpec(memory_space=pltpu.VMEM)] * (1 + len(back))
        out_specs += [
            pl.BlockSpec(memory_space=pltpu.HBM),
            pl.BlockSpec(memory_space=pltpu.VMEM),
            pl.BlockSpec(memory_space=pltpu.VMEM),
        ]
        scratch += [
            pltpu.VMEM((4, block, width), dtype),
            pltpu.VMEM((4, block, width), dtype),
            pltpu.VMEM((LADDER, weight.shape[0] // 2 // LADDER, width), dtype),
            pltpu.VMEM((LADDER, weight.shape[0] // 2 // LADDER, width), dtype),
            pltpu.VMEM(weight.shape, dtype),
            pltpu.SemaphoreType.DMA((4,)),
            pltpu.SemaphoreType.DMA,
        ] + ladder_scratch(LADDER)
        scratch += [
            pltpu.VMEM((seq, seq), jnp.float32),
            pltpu.VMEM((seq, HEAD_SIZE), jnp.float32),
            pltpu.VMEM((seq, HEAD_SIZE), jnp.float32),
        ]
    else:
        rows_held, hidden_held = expert
        held, ff = rows_held.shape[1] // 8, hidden_held.shape[2]
        operands += expert
        in_specs += [pl.BlockSpec(memory_space=pltpu.HBM)] * 2
        out_shape.append(jax.ShapeDtypeStruct((1, 3, width, ff), jnp.float32))
        out_specs.append(pl.BlockSpec(memory_space=pltpu.HBM))
        scratch += [
            pltpu.VMEM((2, 2, held, width), dtype),
            pltpu.VMEM((2, 3, held, ff), dtype),
            pltpu.VMEM((3, width, ff), jnp.float32),
            pltpu.SemaphoreType.DMA((2, 2)),
            pltpu.SemaphoreType.DMA,
        ]
    return pl.pallas_call(
        functools.partial(reduce_kernel, weight is not None),
        out_shape=out_shape,
        in_specs=in_specs,
        out_specs=out_specs,
        scratch_shapes=scratch,
        compiler_params=pltpu.CompilerParams(
            collective_id=collective_id, has_side_effects=True, vmem_limit_bytes=63 << 20
        ),
        name="reduce_all",
    )(*operands)


def others():
    z, core, y, x = place()
    return [
        (device(z, core, yy, xx), yy * 2 + xx)
        for yy, xx in ((y, 1 - x), (1 - y, x), (1 - y, 1 - x))
    ]


def remote(source, landing, send_sem, recv_sem, target):
    return pltpu.make_async_remote_copy(
        src_ref=source,
        dst_ref=landing,
        send_sem=send_sem,
        recv_sem=recv_sem,
        device_id=target,
        device_id_type=MESH_ID,
    )


def start_kernel(
    x_ref, w_ref, x_all, w_own, hold, send_sem, x_sem, w_sem, pair_sem, own_sem
):
    tok = x_ref.shape[0]
    depth = w_ref.shape[0]
    half = depth // 2
    z, core, y, x = place()
    me = y * 2 + x
    partner = device(z, 1 - core, y, x)
    near = others()
    greet([(None, target) for target, _ in near] + [(None, partner)])
    parts = QUERY_HEADS // 4 * HEAD_SIZE
    single = HEAD_SIZE
    widths = (
        (0, parts, 0),
        (QUERY_HEADS * HEAD_SIZE, single, parts),
        ((QUERY_HEADS + KEY_VALUE_HEADS) * HEAD_SIZE, single, parts + single),
    )

    def columns(piece, who):
        base, width, _ = widths[piece]
        return pl.ds(pl.multiple_of(base + who * width, 128), width)

    def landing(piece, who, part, ref=w_own):
        _, width, offset = widths[piece]
        rows = pl.ds(pl.multiple_of(who * depth + part * half, half), half)
        return ref.at[rows, pl.ds(offset, width)]

    sends = []
    for slot, (target, who) in enumerate(near):
        for piece in range(3):
            copy = remote(
                w_ref.at[pl.ds(pl.multiple_of(core * half, half), half), columns(piece, who)],
                landing(piece, me, core),
                send_sem.at[slot * 4 + piece],
                w_sem.at[slot * 3 + piece],
                target,
            )
            copy.start()
            sends.append(copy)
        copy = remote(
            x_ref,
            x_all.at[pl.ds(pl.multiple_of(me * tok, tok), tok)],
            send_sem.at[slot * 4 + 3],
            x_sem.at[slot],
            target,
        )
        copy.start()
        sends.append(copy)
    mine = pltpu.make_async_copy(
        x_ref, x_all.at[pl.ds(pl.multiple_of(me * tok, tok), tok)], own_sem.at[0]
    )
    mine.start()
    loads = []
    for piece in range(3):
        _, width, offset = widths[piece]
        loads.append(
            pltpu.make_async_copy(
                w_ref.at[:, columns(piece, me)], hold.at[:, pl.ds(offset, width)], own_sem.at[1 + piece]
            )
        )
        loads[-1].start()
    for copy in loads:
        copy.wait()
    keep = pltpu.make_async_copy(
        hold, w_own.at[pl.ds(pl.multiple_of(me * depth, depth), depth)], own_sem.at[4]
    )
    keep.start()
    for slot, (target, who) in enumerate(near):
        for piece in range(3):
            where = landing(piece, who, core)
            remote(where, where, send_sem.at[0], w_sem.at[slot * 3 + piece], partner).wait_recv()
        rows = w_own.at[pl.ds(pl.multiple_of(who * depth + core * half, half), half)]
        copy = remote(rows, rows, send_sem.at[12 + slot], pair_sem.at[slot], partner)
        copy.start()
        sends.append(copy)
    for slot, (target, who) in enumerate(near):
        rows = w_own.at[pl.ds(pl.multiple_of(who * depth + (1 - core) * half, half), half)]
        remote(rows, rows, send_sem.at[0], pair_sem.at[slot], partner).wait_recv()
        rows = x_all.at[pl.ds(pl.multiple_of(who * tok, tok), tok)]
        remote(rows, rows, send_sem.at[0], x_sem.at[slot], partner).wait_recv()
    mine.wait()
    keep.wait()
    for copy in sends:
        copy.wait_send()


def start_exchange(block_in, weight, collective_id):
    tok, width = block_in.shape
    depth, columns = weight.shape
    return pl.pallas_call(
        start_kernel,
        out_shape=[
            jax.ShapeDtypeStruct((tok * 4, width), block_in.dtype),
            jax.ShapeDtypeStruct((depth * 4, columns // 4), weight.dtype),
        ],
        in_specs=[
            pl.BlockSpec(memory_space=pltpu.VMEM),
            pl.BlockSpec(memory_space=pltpu.HBM),
        ],
        out_specs=[pl.BlockSpec(memory_space=pltpu.HBM)] * 2,
        scratch_shapes=[
            pltpu.VMEM((depth, columns // 4), weight.dtype),
            pltpu.SemaphoreType.DMA((16,)),
            pltpu.SemaphoreType.DMA((3,)),
            pltpu.SemaphoreType.DMA((9,)),
            pltpu.SemaphoreType.DMA((3,)),
            pltpu.SemaphoreType.DMA((5,)),
        ],
        compiler_params=pltpu.CompilerParams(
            collective_id=collective_id, has_side_effects=True, vmem_limit_bytes=40 << 20
        ),
        name="start_exchange",
    )(block_in, weight)


def spread_kernel(x_ref, x_all, send_sem, x_sem, own_sem):
    tok = x_ref.shape[0]
    z, core, y, x = place()
    me = y * 2 + x
    near = others()
    greet([(None, target) for target, _ in near[:2]])
    sends = Sends(send_sem, near[0][0])

    def rows(who, part=None):
        if part is None:
            return x_all.at[pl.ds(pl.multiple_of(who * tok, tok), tok)]
        start = who * tok + part * (tok // 2)
        return x_all.at[pl.ds(pl.multiple_of(start, tok // 2), tok // 2)]

    for slot in range(2):
        for part in (1 - slot, slot):
            sends.send(
                x_ref.at[pl.ds(part * (tok // 2), tok // 2)],
                rows(me, part),
                x_sem.at[slot, part],
                near[slot][0],
            )
    own_x = pltpu.make_async_copy(x_ref, rows(me), own_sem)
    own_x.start()
    for slot in range(2):
        who, part = near[slot][1], 1 - slot
        sends.arrived(rows(who, part), x_sem.at[slot, part])
        sends.send(rows(who, part), rows(who, part), x_sem.at[2, part], near[1 - slot][0])
    for slot in range(2):
        sends.arrived(rows(near[slot][1], slot), x_sem.at[slot, slot])
    for part in range(2):
        sends.arrived(rows(near[2][1], part), x_sem.at[2, part])
    own_x.wait()
    sends.finish()


def spread_sequence(rows, collective_id):
    tok, width = rows.shape
    return pl.pallas_call(
        spread_kernel,
        out_shape=jax.ShapeDtypeStruct((tok * 4, width), rows.dtype),
        in_specs=[pl.BlockSpec(memory_space=pltpu.VMEM)],
        out_specs=pl.BlockSpec(memory_space=pltpu.HBM),
        scratch_shapes=[
            pltpu.SemaphoreType.DMA((6,)),
            pltpu.SemaphoreType.DMA((3, 2)),
            pltpu.SemaphoreType.DMA,
        ],
        compiler_params=pltpu.CompilerParams(
            collective_id=collective_id, has_side_effects=True, vmem_limit_bytes=40 << 20
        ),
        name="spread_sequence",
    )(rows)


def fold_kernel(part_ref, out_ref, across, beside, summed, send_sem, recv_sem):
    tok = out_ref.shape[0]
    half = tok // 2
    z, core, y, x = place()
    me = y * 2 + x
    near = others()
    greet([(None, target) for target, _ in near[:2]])
    sends = Sends(send_sem, near[0][0])

    def rows(who, part):
        start = who * tok + part * half
        return part_ref.at[pl.ds(pl.multiple_of(start, half), half)]

    def landing(slot, part):
        return beside.at[slot, pl.ds(part * half, half)]

    for slot in range(2):
        sends.send(rows(near[2][1], slot), across.at[slot], recv_sem.at[0, slot], near[slot][0])
    for slot in range(2):
        sends.send(
            rows(near[slot][1], slot), landing(slot, slot), recv_sem.at[1, slot], near[slot][0]
        )
    for slot in range(2):
        part = 1 - slot
        sends.arrived(across.at[part], recv_sem.at[0, part])
        add_into(summed.at[slot], (rows(near[slot][1], part), across.at[part]), half)
        sends.send(summed.at[slot], landing(slot, part), recv_sem.at[2, slot], near[slot][0])
    for slot in range(2):
        sends.arrived(landing(slot, slot), recv_sem.at[1, slot])
        sends.arrived(landing(slot, 1 - slot), recv_sem.at[2, slot])
    own = part_ref.at[pl.ds(pl.multiple_of(me * tok, tok), tok)]
    add_into(out_ref, (own, beside.at[0], beside.at[1]), tok)
    sends.finish()


def fold_sequence(part, collective_id):
    total, width = part.shape
    tok = total // 4
    return pl.pallas_call(
        fold_kernel,
        out_shape=jax.ShapeDtypeStruct((tok, width), jnp.float32),
        in_specs=[pl.BlockSpec(memory_space=pltpu.VMEM)],
        out_specs=pl.BlockSpec(memory_space=pltpu.VMEM),
        scratch_shapes=[
            pltpu.VMEM((2, tok // 2, width), part.dtype),
            pltpu.VMEM((2, tok, width), part.dtype),
            pltpu.VMEM((2, tok // 2, width), part.dtype),
            pltpu.SemaphoreType.DMA((6,)),
            pltpu.SemaphoreType.DMA((3, 2)),
        ],
        compiler_params=pltpu.CompilerParams(
            collective_id=collective_id, has_side_effects=True, vmem_limit_bytes=40 << 20
        ),
        name="fold_sequence",
    )(part)


def weight_kernel(
    grad_ref,
    fold_ref,
    out_ref,
    fold_out,
    pair,
    part,
    landed,
    from_up,
    from_down,
    done,
    folds,
    send_sem,
    pair_sem,
    cross_sem,
    fold_sem,
    write_sem,
    *ladder_sems,
):
    depth = done.shape[1]
    half = depth // 2
    block = half // PER
    tok = fold_out.shape[0]
    z, core, y, x = place()
    me = y * 2 + x
    partner = device(z, 1 - core, y, x)
    up, down = device(z + 1, core, y, x), device(z - 1, core, y, x)
    near = [(device(z, core, y, x), me)] + others()
    greet(
        [(None, partner)]
        + [(None, target) for target, _ in near[1:]]
        + [(z < PLANES - 1, up), (z > 0, down)]
    )
    sends = Sends(send_sem, partner)

    def own_rows(n, which):
        start = pl.multiple_of(near[n][1] * depth + which * half, half)
        return grad_ref.at[pl.ds(start, half)]

    for n in range(4):
        sends.send(own_rows(n, 1 - core), pair.at[n], pair_sem.at[n], partner)
    for n in range(4):
        sends.arrived(pair.at[n], pair_sem.at[n])
        target = part.at[n - 1] if n else landed.at[0]
        add_into(target, (own_rows(n, core), pair.at[n]), half)
        if n:
            sends.send(target, landed.at[n], cross_sem.at[n - 1], near[n][0])
    for n in (1, 2, 3):
        target, who = near[n]
        rows = fold_ref.at[pl.ds(pl.multiple_of(who * tok, tok), tok)]
        sends.send(rows, folds.at[n - 1], fold_sem.at[n - 1], target)

    def before(n):
        @pl.when(jnp.logical_and(n % PER == 0, n > 0))
        def _():
            sends.arrived(landed.at[n // PER], cross_sem.at[n // PER - 1])

    def done_rows(n, which):
        source = n // PER
        who = ((y + source // 2) % 2) * 2 + (x + source % 2) % 2
        start = pl.multiple_of(which * half + (n % PER) * block, block)
        return done.at[who, pl.ds(start, block)]

    ladder_step, closed, close = ladder(
        sends,
        LADDER,
        before,
        lambda n: landed.at[n // PER, pl.ds(pl.multiple_of((n % PER) * block, block), block)],
        lambda n: from_up.at[n],
        lambda n: from_down.at[n],
        done_rows,
        block,
        ladder_sems,
    )

    @pl.loop(0, LADDER + LADDER_MORE)
    def _(m):
        ladder_step(m)

    for n in range(3):
        sends.arrived(folds.at[n], fold_sem.at[n])
    add_into(
        fold_out,
        [fold_ref.at[pl.ds(pl.multiple_of(me * tok, tok), tok)]] + [folds.at[n] for n in range(3)],
        tok,
    )
    single = HEAD_SIZE
    heads = QUERY_HEADS // 4 * HEAD_SIZE
    writes = []

    @pl.loop(0, LADDER)
    def _(n):
        closed(n)

    for n in range(4):
        who = near[n][1]
        for c, (base, width, offset) in enumerate(
            (
                (0, heads, 0),
                (QUERY_HEADS * HEAD_SIZE, single, heads),
                ((QUERY_HEADS + KEY_VALUE_HEADS) * HEAD_SIZE, single, heads + single),
            )
        ):
            copy = pltpu.make_async_copy(
                done.at[who, :, pl.ds(offset, width)],
                out_ref.at[:, pl.ds(pl.multiple_of(base + who * width, 128), width)],
                write_sem.at[n * 3 + c],
            )
            copy.start()
            writes.append(copy)
    close()
    for copy in writes:
        copy.wait()
    sends.finish()


def weight_reduce(grad, fold, collective_id):
    rows, columns = grad.shape
    depth = rows // 4
    half = depth // 2
    tok, width = fold.shape[0] // 4, fold.shape[1]
    dtype = grad.dtype
    return pl.pallas_call(
        weight_kernel,
        out_shape=[
            jax.ShapeDtypeStruct((depth, columns * 4), dtype),
            jax.ShapeDtypeStruct((tok, width), jnp.float32),
        ],
        in_specs=[pl.BlockSpec(memory_space=pltpu.VMEM)] * 2,
        out_specs=[pl.BlockSpec(memory_space=pltpu.HBM), pl.BlockSpec(memory_space=pltpu.VMEM)],
        scratch_shapes=[
            pltpu.VMEM((4, half, columns), dtype),
            pltpu.VMEM((3, half, columns), dtype),
            pltpu.VMEM((4, half, columns), dtype),
            pltpu.VMEM((LADDER, half // PER, columns), dtype),
            pltpu.VMEM((LADDER, half // PER, columns), dtype),
            pltpu.VMEM((4, depth, columns), dtype),
            pltpu.VMEM((3, tok, width), dtype),
            pltpu.SemaphoreType.DMA((10,)),
            pltpu.SemaphoreType.DMA((4,)),
            pltpu.SemaphoreType.DMA((3,)),
            pltpu.SemaphoreType.DMA((3,)),
            pltpu.SemaphoreType.DMA((12,)),
        ]
        + ladder_scratch(LADDER),
        compiler_params=pltpu.CompilerParams(
            collective_id=collective_id, has_side_effects=True, vmem_limit_bytes=56 << 20
        ),
        name="weight_reduce",
    )(grad, fold)


def project_back_kernel(
    grad_ref,
    weight_ref,
    normed_ref,
    x_ref,
    experts_ref,
    part_ref,
    grad_weight_ref,
    gain_ref,
    experts_out,
    inverse,
    ring,
    load_sem,
    store_sem,
):
    stripes = x_ref.shape[1] // 256
    chunk = ring.shape[1]
    slots = ring.shape[0]
    each = experts_ref.shape[2] // chunk
    chunks = 3 * each
    per = chunks // stripes

    def rows(ref, c):
        return ref.at[0, c // each, pl.ds(pl.multiple_of((c % each) * chunk, chunk), chunk)]

    def load(c):
        return pltpu.make_async_copy(
            rows(experts_ref, c), ring.at[c % slots], load_sem.at[c % slots]
        )

    def store(c):
        return pltpu.make_async_copy(
            ring.at[c % slots], rows(experts_out, c), store_sem.at[c % slots]
        )

    for c in range(slots):
        load(c).start()

    @pl.loop(0, x_ref.shape[0] // 64)
    def _(n):
        span = pl.ds(pl.multiple_of(n * 64, 64), 64)
        inverse[span] = inverse_rms(x_ref[span].astype(jnp.float32))

    @pl.loop(0, stripes)
    def _(i):
        for k in range(per):
            load(i * per + k).wait()
            store(i * per + k).start()
        span = pl.ds(pl.multiple_of(i * 256, 256), 256)
        part = mm(grad_ref[...], weight_ref[span], (1, 1))
        part_ref[:, span] = part.astype(jnp.bfloat16)
        scaled = part * x_ref[:, span].astype(jnp.float32) * inverse[...]
        gain_ref[:, span] = jnp.sum(scaled, axis=0, keepdims=True)
        grad_weight_ref[span] = mm(normed_ref[:, span], grad_ref[...], (0, 0)).astype(jnp.bfloat16)
        for k in range(per):
            store(i * per + k).wait()

            @pl.when(i * per + k + slots < chunks)
            def _():
                load(i * per + k + slots).start()


def project_back(grad, weight, normed, x, experts):
    seq, width = x.shape
    bf, f4 = jnp.bfloat16, jnp.float32
    return pl.pallas_call(
        project_back_kernel,
        out_shape=[
            jax.ShapeDtypeStruct((seq, width), bf),
            jax.ShapeDtypeStruct(weight.shape, bf),
            jax.ShapeDtypeStruct((1, width), f4),
            jax.ShapeDtypeStruct(experts.shape, f4),
        ],
        in_specs=[pl.BlockSpec(memory_space=pltpu.VMEM)] * 4
        + [pl.BlockSpec(memory_space=pltpu.HBM)],
        out_specs=[pl.BlockSpec(memory_space=pltpu.VMEM)] * 3
        + [pl.BlockSpec(memory_space=pltpu.HBM)],
        scratch_shapes=[
            pltpu.VMEM((seq, 1), f4),
            pltpu.VMEM((6, 256, experts.shape[3]), f4),
            pltpu.SemaphoreType.DMA((6,)),
            pltpu.SemaphoreType.DMA((6,)),
        ],
        compiler_params=pltpu.CompilerParams(vmem_limit_bytes=48 << 20),
        name="project_back",
    )(grad, weight, normed, x, experts)


def split_body(
    block_in,
    segments,
    routes,
    attn_gain,
    query_key_value_weight,
    q_gain,
    k_gain,
    w_out,
    ffn_gain,
    router,
    expert_weights,
    cotangent,
):
    tok, width = block_in.shape
    seq = segments.shape[0]
    experts = router.shape[1]
    capacity = tok * routes.shape[1] * 2 // experts
    heads = QUERY_HEADS // 4
    both = ("rep", "shard")
    upstream_all = lax.all_gather(cotangent, both, axis=0, tiled=True)
    x_all, weight = start_exchange(block_in, query_key_value_weight, 0)

    mask = jnp.any(
        routes[:, :, None] == jnp.arange(experts, dtype=jnp.int32)[None, None, :], axis=1
    )
    mask_f = mask.astype(jnp.float32)
    earlier = (jnp.arange(tok)[:, None] > jnp.arange(tok)[None, :]).astype(jnp.bfloat16)
    slot = jnp.dot(earlier, mask.astype(jnp.bfloat16), preferred_element_type=jnp.float32)
    slot_table = jnp.where(mask, slot, -4096.0).T

    cosine, sine = rope_tables(jnp.arange(seq, dtype=jnp.int32))
    cosine = cosine[:, 0]
    sine = sine[:, 0] * jnp.where(jnp.arange(HEAD_SIZE) < HEAD_SIZE // 2, -1.0, 1.0)
    normed_one, raw, q_rot, k_rot, values, attended, lse, partial = attend(
        x_all, weight, w_out, attn_gain, q_gain, k_gain, cosine, sine, segments
    )
    inputs = block_in.astype(jnp.float32)
    middle = inputs + fold_sequence(partial, 1)
    scale_two = rms_scale(middle)
    normed_two = (middle * scale_two * ffn_gain).astype(jnp.bfloat16)
    logits = jnp.dot(normed_two, router, preferred_element_type=jnp.float32)
    weights = jax.nn.softmax(logits, axis=-1)
    picked = weights * mask_f
    total = jnp.sum(picked, axis=1, keepdims=True)
    gates = picked / total
    table = jnp.concatenate([gates.T, slot_table], axis=0)
    tokens_all, _, out_part, grad_part, gate_part, rows_held, hidden_held = run_experts(
        normed_two, table, upstream_all, expert_weights, capacity, 2
    )
    grad_gates = lax.all_to_all(gate_part, both, split_axis=0, concat_axis=0, tiled=True).T
    grad_from_experts, grad_experts = reduce_all(grad_part, 3, expert=[rows_held, hidden_held])
    grad_from_experts = grad_from_experts.astype(jnp.float32)

    upstream = cotangent.astype(jnp.float32)
    grad_picked = grad_gates / total - jnp.sum(grad_gates * picked, axis=1, keepdims=True) / (
        total * total
    )
    grad_weights = grad_picked * mask_f
    grad_logits = weights * (grad_weights - jnp.sum(grad_weights * weights, axis=1, keepdims=True))
    grad_from_router = jnp.dot(
        grad_logits, router.astype(jnp.float32).T, precision=lax.Precision.HIGHEST
    )
    grad_norm_two, grad_ffn_gain = rms_back(
        middle, scale_two, ffn_gain, grad_from_experts + grad_from_router
    )
    grad_middle = upstream + grad_norm_two
    grad_middle_all = spread_sequence(grad_middle.astype(jnp.bfloat16), 5)
    grad_out = lax.dot_general(
        attended, grad_middle_all, (((0,), (0,)), ((), ())), preferred_element_type=jnp.float32
    ).astype(jnp.bfloat16)
    grad_attended = jnp.dot(
        grad_middle_all, w_out.T, preferred_element_type=jnp.float32
    ).astype(jnp.bfloat16)
    delta = attended.astype(jnp.float32) * grad_attended.astype(jnp.float32)
    delta = jnp.sum(delta.reshape(seq, heads, HEAD_SIZE), axis=2).T
    expert_sum, grad_out, grad_qkv_b, grad_gains = reduce_all(
        out_part,
        4,
        grad_out,
        [
            q_rot,
            k_rot,
            values,
            raw,
            grad_attended,
            lse,
            delta,
            q_gain[None],
            k_gain[None],
            cosine,
            sine,
            segments[:, None],
            segments[None],
        ],
    )
    block_out = (middle + expert_sum.astype(jnp.float32)).astype(jnp.bfloat16)
    grad_out = grad_out.astype(jnp.float32)
    grad_q_gain, grad_k_gain = grad_gains[0], grad_gains[1]
    norm_part, grad_weight, grad_attn_gain, grad_experts = project_back(
        grad_qkv_b, weight, normed_one, x_all, grad_experts
    )
    grad_attn_gain = grad_attn_gain[0]
    gains = jnp.concatenate([grad_attn_gain, grad_ffn_gain, grad_q_gain, grad_k_gain])
    lines = gains.shape[0] // tok
    spare = -(lines + experts) % 16
    small = jnp.concatenate(
        [grad_logits.T, gains.reshape(lines, tok), jnp.zeros((spare, tok), jnp.float32)], axis=0
    )
    small_all = lax.all_gather(small, both)
    grad_qkv, grad_norm_one = weight_reduce(grad_weight, norm_part, 7)
    grad_qkv = grad_qkv.astype(jnp.float32)
    grad_inputs, _ = rms_back(inputs, rms_scale(inputs), attn_gain, grad_norm_one)
    grad_input = (grad_middle + grad_inputs).astype(jnp.bfloat16)
    gains = jnp.sum(small_all[:, experts : experts + lines], axis=0).reshape(-1)
    grad_attn_gain, grad_ffn_gain, grad_q_gain, grad_k_gain = jnp.split(
        gains, (width, 2 * width, 2 * width + HEAD_SIZE)
    )
    logits_all = small_all[:, :experts].transpose(1, 0, 2).reshape(experts, -1)
    high = lax.reduce_precision(logits_all, 8, 7)
    middle_part = lax.reduce_precision(logits_all - high, 8, 7)
    low = logits_all - high - middle_part
    pieces = jnp.concatenate([high, middle_part, low], axis=0).astype(jnp.bfloat16)
    pieces = jnp.dot(pieces, tokens_all, preferred_element_type=jnp.float32)
    grad_router = jnp.sum(pieces.reshape(3, experts, width), axis=0).T
    return (
        block_out,
        grad_input,
        grad_attn_gain,
        grad_qkv,
        grad_q_gain,
        grad_k_gain,
        grad_out,
        grad_ffn_gain,
        grad_router,
        grad_experts,
    )


def solution(mesh):
    placed = (
        P(("rep", "shard"), None),
        P("rep"),
        P(("rep", "shard"), None),
        P(),
        P("shard", None),
        P(),
        P(),
        P("shard", None),
        P(),
        P(),
        P(("rep", "shard"), None, None, None),
        P(("rep", "shard"), None),
    )
    body = split_body if dict(mesh.shape) == {"rep": 8, "shard": 4} else plain_body
    return jax.shard_map(
        body,
        mesh=mesh,
        in_specs=placed,
        out_specs=(
            P(("rep", "shard"), None),
            P(("rep", "shard"), None),
            P(),
            P("shard", None),
            P(),
            P(),
            P("shard", None),
            P(),
            P(),
            P(("rep", "shard"), None, None, None),
        ),
        check_vma=False,
    )
```

```python
import functools

import jax
import jax.numpy as jnp
from jax import lax
from jax.experimental import pallas as pl
from jax.experimental.pallas import tpu as pltpu
from jax.sharding import PartitionSpec as P


QUERY_HEADS = 32
KEY_VALUE_HEADS = 4
HEAD_SIZE = 128


epsilon = 1e-06
rope_base = 1000000.0


def product(form, left, right):
    return jnp.einsum(form, left, right, preferred_element_type=jnp.float32)


def rms_scale(values):
    return lax.rsqrt(jnp.mean(values * values, axis=-1, keepdims=True) + epsilon)


def rms_back(values, scale, gain, upstream):
    scaled = upstream * gain
    cube = scale * scale * scale
    grad_values = scale * scaled - values * cube * jnp.mean(scaled * values, axis=-1, keepdims=True)
    grad_gain = jnp.sum((upstream * values * scale).reshape(-1, values.shape[-1]), axis=0)
    return (grad_values, grad_gain)


def rope_tables(positions):
    half = HEAD_SIZE // 2
    freq = rope_base ** (-jnp.arange(half).astype(jnp.float32) * 2.0 / HEAD_SIZE)
    angles = positions.astype(jnp.float32)[:, None] * freq[None, :]
    cosine = jnp.concatenate([jnp.cos(angles), jnp.cos(angles)], axis=-1)
    sine = jnp.concatenate([jnp.sin(angles), jnp.sin(angles)], axis=-1)
    return (cosine[:, None, :], sine[:, None, :])


def rotate(values):
    half = values.shape[-1] // 2
    return jnp.concatenate([-values[..., half:], values[..., :half]], axis=-1)


def rotate_back(values):
    half = values.shape[-1] // 2
    return jnp.concatenate([values[..., half:], -values[..., :half]], axis=-1)


def split_heads(query_key_value):
    token_rows = query_key_value.shape[0]
    q_raw = query_key_value[:, : QUERY_HEADS * HEAD_SIZE].reshape(
        token_rows, QUERY_HEADS, HEAD_SIZE
    )
    unrotated_key = query_key_value[
        :, QUERY_HEADS * HEAD_SIZE : (QUERY_HEADS + KEY_VALUE_HEADS) * HEAD_SIZE
    ].reshape(token_rows, KEY_VALUE_HEADS, HEAD_SIZE)
    projected_value = query_key_value[:, (QUERY_HEADS + KEY_VALUE_HEADS) * HEAD_SIZE :].reshape(
        token_rows, KEY_VALUE_HEADS, HEAD_SIZE
    )
    return (q_raw, unrotated_key, projected_value)


def norm_rope(raw, gain, cosine, sine):
    scale = rms_scale(raw)
    normed = raw * scale * gain
    return (scale, (normed * cosine + rotate(normed) * sine).astype(jnp.bfloat16))


def norm_rope_back(raw, scale, gain, cosine, sine, grad_rot):
    grad_normed = grad_rot * cosine + rotate_back(grad_rot * sine)
    return rms_back(raw, scale, gain, grad_normed)


def split_groups(values, groups):
    token_rows, heads, width = values.shape
    return values.reshape(token_rows, groups, heads // groups, width).transpose(1, 0, 2, 3)


def attend_forward(queries, keys, values, allowed):
    groups = keys.shape[1]
    token_rows = queries.shape[0]
    scale = queries.shape[2] ** (-0.5)

    def one_group(operands):
        q_part, k_part, v_part = operands
        scores = jnp.where(allowed[None], product("tpd,sd->pts", q_part, k_part) * scale, -1e30)
        highest = jnp.max(scores, axis=2, keepdims=True)
        lse = highest + jnp.log(jnp.sum(jnp.exp(scores - highest), axis=2, keepdims=True))
        probs = jnp.exp(scores - lse).astype(jnp.bfloat16)
        return (product("pts,sd->tpd", probs, v_part), lse[:, :, 0])

    outputs, lse = lax.map(
        one_group,
        (split_groups(queries, groups), keys.transpose(1, 0, 2), values.transpose(1, 0, 2)),
    )
    return (outputs.transpose(1, 0, 2, 3).reshape(token_rows, -1), lse)


def attend_backward(queries, keys, values, allowed, lse, attended, grad_attended):
    groups = keys.shape[1]
    token_rows, heads, width = queries.shape
    scale = width ** (-0.5)

    def one_group(operands):
        q_part, k_part, v_part, lse_part, out_part, grad_part = operands
        scores = jnp.where(allowed[None], product("tpd,sd->pts", q_part, k_part) * scale, -1e30)
        probs = jnp.exp(scores - lse_part[:, :, None])
        grad_v = product("pts,tpd->sd", probs.astype(jnp.bfloat16), grad_part)
        grad_p = product("tpd,sd->pts", grad_part, v_part)
        delta = jnp.sum(
            out_part.astype(jnp.float32) * grad_part.astype(jnp.float32), axis=2
        ).transpose(1, 0)
        grad_score = (probs * (grad_p - delta[:, :, None]) * scale).astype(jnp.bfloat16)
        return (
            product("pts,sd->tpd", grad_score, k_part),
            product("pts,tpd->sd", grad_score, q_part),
            grad_v,
        )

    shaped_out = split_groups(attended.reshape(token_rows, heads, width), groups)
    shaped_grad = split_groups(grad_attended.reshape(token_rows, heads, width), groups)
    grad_q, grad_k, grad_v = lax.map(
        one_group,
        (
            split_groups(queries, groups),
            keys.transpose(1, 0, 2),
            values.transpose(1, 0, 2),
            lse,
            shaped_out,
            shaped_grad,
        ),
    )
    return (
        grad_q.transpose(1, 0, 2, 3).reshape(token_rows, heads, width),
        grad_k.transpose(1, 0, 2),
        grad_v.transpose(1, 0, 2),
    )


def route_gates(normed, router, routes):
    logits = jnp.dot(normed, router, preferred_element_type=jnp.float32)
    weights = jax.nn.softmax(logits, axis=-1)
    chosen = (
        routes[:, :, None] == jnp.arange(router.shape[1], dtype=jnp.int32)[None, None, :]
    ).astype(jnp.float32)
    picked = jnp.sum(chosen * weights[:, None, :], axis=2)
    total = jnp.sum(picked, axis=1, keepdims=True)
    return (weights, chosen, picked, total, picked / total)


def route_gates_back(normed, router, weights, chosen, picked, total, grad_gates):
    grad_picked = grad_gates / total - jnp.sum(grad_gates * picked, axis=1, keepdims=True) / (
        total * total
    )
    grad_weights = jnp.sum(chosen * grad_picked[:, :, None], axis=1)
    grad_logits = weights * (grad_weights - jnp.sum(grad_weights * weights, axis=1, keepdims=True))
    grad_normed = jnp.dot(
        grad_logits, router.astype(jnp.float32).T, precision=lax.Precision.HIGHEST
    )
    grad_router = jnp.dot(
        normed.astype(jnp.float32).T, grad_logits, precision=lax.Precision.HIGHEST
    )
    return (grad_normed, grad_router)


def route_index(routes, experts, capacity):
    flat = routes.reshape(-1)
    onehot = (flat[:, None] == jnp.arange(experts, dtype=jnp.int32)[None, :]).astype(jnp.int32)
    before = jnp.cumsum(onehot, axis=0) - onehot
    return flat * capacity + jnp.sum(before * onehot, axis=1)


def dispatch(rows_per_route, index, experts, capacity):
    width = rows_per_route.shape[1]
    empty = jnp.zeros((experts * capacity, width), rows_per_route.dtype)
    return empty.at[index].set(rows_per_route).reshape(experts, capacity, width)


def collect(buffer, index):
    return buffer.reshape(-1, buffer.shape[-1])[index]


def expert_forward(inputs, weights):
    gate_pre = product("ecd,edf->ecf", inputs, weights[:, 0])
    up_pre = product("ecd,edf->ecf", inputs, weights[:, 1])
    hidden = (jax.nn.silu(gate_pre) * up_pre).astype(jnp.bfloat16)
    result = product("ecf,edf->ecd", hidden, weights[:, 2]).astype(jnp.bfloat16)
    return (gate_pre, up_pre, hidden, result)


def expert_backward(weights, gate_pre, up_pre, grad_result):
    grad_hidden = product("ecd,edf->ecf", grad_result, weights[:, 2])
    sig = jax.nn.sigmoid(gate_pre)
    grad_gate = (grad_hidden * up_pre * sig * (1.0 + gate_pre * (1.0 - sig))).astype(jnp.bfloat16)
    grad_up = (grad_hidden * gate_pre * sig).astype(jnp.bfloat16)
    grad_inputs = product("ecf,edf->ecd", grad_gate, weights[:, 0]) + product(
        "ecf,edf->ecd", grad_up, weights[:, 1]
    )
    return (grad_gate, grad_up, grad_inputs.astype(jnp.bfloat16))


def expert_weight_grads(inputs, hidden, grad_gate, grad_up, grad_result):
    return jnp.stack(
        [
            product("ecd,ecf->edf", inputs, grad_gate),
            product("ecd,ecf->edf", inputs, grad_up),
            product("ecd,ecf->edf", grad_result, hidden),
        ],
        axis=1,
    )


def plain_body(
    block_in,
    segments,
    routes,
    attn_gain,
    query_key_value_weight,
    q_gain,
    k_gain,
    w_out,
    ffn_gain,
    router,
    expert_weights,
    cotangent,
):
    tok = block_in.shape[0]
    width = block_in.shape[1]
    top = routes.shape[1]
    rep_count = lax.axis_size("rep")
    shard_count = lax.axis_size("shard")
    experts = expert_weights.shape[0] * rep_count * shard_count
    capacity = tok * top * 2 // experts
    shard_pos = lax.axis_index("shard")
    qkv_whole, out_whole = (
        lax.all_gather(query_key_value_weight, "shard", axis=0, tiled=True),
        lax.all_gather(w_out, "shard", axis=0, tiled=True),
    )
    inputs = block_in.astype(jnp.float32)
    scale_one = rms_scale(inputs)
    normed_one = (inputs * scale_one * attn_gain).astype(jnp.bfloat16)
    query_key_value = jnp.dot(normed_one, qkv_whole, preferred_element_type=jnp.float32)
    q_raw, unrotated_key, projected_value = split_heads(query_key_value)
    positions = shard_pos * tok + jnp.arange(tok, dtype=jnp.int32)
    cosine, sine = rope_tables(positions)
    q_scale, q_rot = norm_rope(q_raw, q_gain, cosine, sine)
    k_scale, k_rot = norm_rope(unrotated_key, k_gain, cosine, sine)
    keys_all, values_all = (
        lax.all_gather(k_rot, "shard", axis=0, tiled=True),
        lax.all_gather(projected_value.astype(jnp.bfloat16), "shard", axis=0, tiled=True),
    )
    query_seg = lax.dynamic_slice_in_dim(segments, shard_pos * tok, tok)
    key_pos = jnp.arange(segments.shape[0], dtype=jnp.int32)
    allowed = (query_seg[:, None] == segments[None, :]) & (key_pos[None, :] <= positions[:, None])
    attended_f, lse = attend_forward(q_rot, keys_all, values_all, allowed)
    attended = attended_f.astype(jnp.bfloat16)
    middle = inputs + jnp.dot(attended, out_whole, preferred_element_type=jnp.float32)
    scale_two = rms_scale(middle)
    normed_two = (middle * scale_two * ffn_gain).astype(jnp.bfloat16)
    weights, chosen, picked, total, gates = route_gates(normed_two, router, routes)
    index = route_index(routes, experts, capacity)
    upstream = cotangent.astype(jnp.float32)
    grad_rows = (
        (gates[:, :, None] * upstream[:, None, :]).astype(jnp.bfloat16).reshape(tok * top, width)
    )
    paired = jnp.concatenate([jnp.repeat(normed_two, top, axis=0), grad_rows], axis=1)
    buffer = dispatch(paired, index, experts, capacity)
    received = lax.all_to_all(buffer, ("rep", "shard"), split_axis=0, concat_axis=1, tiled=True)
    token_rows = received[:, :, :width]
    grads = received[:, :, width:]
    gate_pre, up_pre, hidden, result = expert_forward(token_rows, expert_weights)
    grad_gate, grad_up, grad_inner = expert_backward(expert_weights, gate_pre, up_pre, grads)
    grad_experts = expert_weight_grads(token_rows, hidden, grad_gate, grad_up, grads)
    outgoing = jnp.concatenate([result, grad_inner], axis=2)
    returned = lax.all_to_all(outgoing, ("rep", "shard"), split_axis=1, concat_axis=0, tiled=True)
    fetched = collect(returned, index).reshape(tok, top, 2 * width)
    expert_rows = fetched[:, :, :width].astype(jnp.float32)
    grad_from_experts = jnp.sum(fetched[:, :, width:].astype(jnp.float32), axis=1)
    block_out = (middle + jnp.sum(gates[:, :, None] * expert_rows, axis=1)).astype(jnp.bfloat16)
    grad_gates = jnp.sum(expert_rows * upstream[:, None, :], axis=2)
    grad_from_router, grad_router = route_gates_back(
        normed_two, router, weights, chosen, picked, total, grad_gates
    )
    grad_norm_two, grad_ffn_gain = rms_back(
        middle, scale_two, ffn_gain, grad_from_experts + grad_from_router
    )
    grad_middle = upstream + grad_norm_two
    grad_middle_b = grad_middle.astype(jnp.bfloat16)
    columns = attended
    grad_out = lax.psum_scatter(
        lax.dot_general(
            columns, grad_middle_b, (((0,), (0,)), ((), ())), preferred_element_type=jnp.float32
        ).astype(jnp.bfloat16),
        "shard",
        scatter_dimension=0,
        tiled=True,
    ).astype(jnp.float32)
    grad_attended = jnp.dot(grad_middle_b, out_whole.T, preferred_element_type=jnp.float32).astype(
        jnp.bfloat16
    )
    grad_q_rot, grad_k_all, grad_v_all = attend_backward(
        q_rot, keys_all, values_all, allowed, lse, attended, grad_attended
    )
    grad_k_rot, grad_v = (
        lax.psum_scatter(
            grad_k_all.astype(jnp.bfloat16), "shard", scatter_dimension=0, tiled=True
        ).astype(jnp.float32),
        lax.psum_scatter(
            grad_v_all.astype(jnp.bfloat16), "shard", scatter_dimension=0, tiled=True
        ).astype(jnp.float32),
    )
    grad_q_raw, grad_q_gain = norm_rope_back(q_raw, q_scale, q_gain, cosine, sine, grad_q_rot)
    grad_k_raw, grad_k_gain = norm_rope_back(
        unrotated_key, k_scale, k_gain, cosine, sine, grad_k_rot
    )
    grad_qkv_b = jnp.concatenate(
        [grad_q_raw.reshape(tok, -1), grad_k_raw.reshape(tok, -1), grad_v.reshape(tok, -1)], axis=1
    ).astype(jnp.bfloat16)
    columns = normed_one
    grad_qkv = lax.psum_scatter(
        lax.dot_general(
            columns, grad_qkv_b, (((0,), (0,)), ((), ())), preferred_element_type=jnp.float32
        ).astype(jnp.bfloat16),
        "shard",
        scatter_dimension=0,
        tiled=True,
    ).astype(jnp.float32)
    grad_norm_one = jnp.dot(grad_qkv_b, qkv_whole.T, preferred_element_type=jnp.float32)
    grad_inputs, grad_attn_gain = rms_back(inputs, scale_one, attn_gain, grad_norm_one)
    grad_input = (grad_middle + grad_inputs).astype(jnp.bfloat16)
    grad_attn_gain, grad_q_gain, grad_k_gain, grad_ffn_gain, grad_router = lax.psum(
        (grad_attn_gain, grad_q_gain, grad_k_gain, grad_ffn_gain, grad_router), ("rep", "shard")
    )
    grad_qkv, grad_out = (
        lax.psum(grad_qkv.astype(jnp.bfloat16), "rep").astype(jnp.float32),
        lax.psum(grad_out.astype(jnp.bfloat16), "rep").astype(jnp.float32),
    )
    return (
        block_out,
        grad_input,
        grad_attn_gain,
        grad_qkv,
        grad_q_gain,
        grad_k_gain,
        grad_out,
        grad_ffn_gain,
        grad_router,
        grad_experts,
    )


MESH_ID = pl.DeviceIdType.MESH
PLANES = 4


def place():
    rep, shard = lax.axis_index("rep"), lax.axis_index("shard")
    return rep // 2, rep % 2, shard // 2, shard % 2


def device(z, core, y, x):
    return (z * 2 + core, y * 2 + x)


def block_of(z, core, y, x):
    return (z * 2 + core) * 4 + y * 2 + x


def greet(targets):
    barrier = pltpu.get_barrier_semaphore()
    for condition, target in targets:
        if condition is None:
            pl.semaphore_signal(barrier, inc=1, device_id=target, device_id_type=MESH_ID)
        else:

            @pl.when(condition)
            def _():
                pl.semaphore_signal(barrier, inc=1, device_id=target, device_id_type=MESH_ID)

    peers = 0
    for condition, _ in targets:
        peers = peers + (1 if condition is None else condition.astype(jnp.int32))
    pl.semaphore_wait(barrier, peers)


def experts_kernel(
    x_ref,
    table_ref,
    upstream_ref,
    w_ref,
    x_all,
    table_all,
    out_ref,
    grad_ref,
    gg_ref,
    rows_out,
    hidden_out,
    gs,
    rows_hold,
    hidden_hold,
    x_hold,
    g_hold,
    t_hold,
    out_hold,
    grad_hold,
    send_sem,
    recv_sem,
    own_sem,
    load_sem,
    store_sem,
):
    ins, outs = (x_ref, table_ref), (x_all, table_all)
    rows = (x_ref.shape[0], table_ref.shape[0])
    count = len(ins)
    tok = rows[0]
    experts = rows[1] // 2
    z, core, y, x = place()
    partner = device(z, 1 - core, y, x)
    x_next, y_next = device(z, core, y, 1 - x), device(z, core, 1 - y, x)
    up, down = device(z + 1, core, y, x), device(z - 1, core, y, x)
    can_up, can_down = z < PLANES - 1, z > 0
    greet(
        [
            (None, partner),
            (None, x_next),
            (None, y_next),
            (can_up, up),
            (can_down, down),
        ]
    )
    tables = ((0, 1, 2, 3), (1, 0, 2, 3), (2, 3, 1, 0), (3, 2, 1, 0))
    order = [
        sum((z == level).astype(jnp.int32) * tables[level][n] for level in range(PLANES))
        for n in range(PLANES)
    ]
    pending, used = [], [0]

    def region(array, block, part):
        size = rows[array]
        if part is None:
            return pl.ds(pl.multiple_of(block * size, size), size)
        return pl.ds(pl.multiple_of(block * size + part * (size // 2), size // 2), size // 2)

    def copy_of(array, block, part, target, index, own=False):
        where = region(array, block, part)
        source = ins[array] if own else outs[array].at[where]
        return remote(
            source,
            outs[array].at[where],
            send_sem.at[array, index],
            recv_sem.at[array, block * 2 + (part or 0)],
            target,
        )

    def plan(block, part, target, condition=None, own=False):
        index = used[0]
        used[0] += 1

        def start():
            for array in range(count):
                copy_of(array, block, part, target, index, own).start()

        def finish():
            for array in range(count):
                copy_of(array, block, part, target, index, own).wait_send()

        pending.append((condition, finish))
        return lambda: start() if condition is None else pl.when(condition)(start)

    def arrived(block, part):
        for array in range(count):
            copy_of(array, block, part, partner, 0).wait_recv()

    own = block_of(z, core, y, x)
    for target, condition in (
        (up, can_up),
        (down, can_down),
        (x_next, None),
        (y_next, None),
        (partner, None),
    ):
        plan(own, None, target, condition, own=True)()
    locals_ = [
        pltpu.make_async_copy(ins[n], outs[n].at[region(n, own, None)], own_sem.at[n])
        for n in range(count)
    ]
    for copy in locals_:
        copy.start()

    def along(n):
        plane = order[n]
        block = block_of(plane, core, y, x)
        moves = [
            plan(block, None, up, jnp.logical_and(plane < z, can_up)),
            plan(block, None, down, jnp.logical_and(plane > z, can_down)),
            plan(block, None, x_next),
            plan(block, None, y_next),
            plan(block, None, partner),
        ]

        def run():
            arrived(block, None)
            for move in moves:
                move()

        return run

    def across(n):
        plane = order[n]
        from_x, from_y = block_of(plane, core, y, 1 - x), block_of(plane, core, 1 - y, x)
        moves = [
            plan(from_x, 1, y_next),
            plan(from_x, None, partner),
            plan(from_y, 0, x_next),
            plan(from_y, None, partner),
        ]

        def run():
            arrived(from_x, None)
            moves[0]()
            moves[1]()
            arrived(from_y, None)
            moves[2]()
            moves[3]()

        return run

    def diagonal(n):
        block = block_of(order[n], core, 1 - y, 1 - x)
        moves = [plan(block, part, partner) for part in range(2)]

        def run():
            for part in range(2):
                arrived(block, part)
                moves[part]()

        return run

    def paired(n):
        plane = order[n]

        def run():
            for where_y, where_x in ((y, x), (y, 1 - x), (1 - y, x)):
                arrived(block_of(plane, 1 - core, where_y, where_x), None)
            for part in range(2):
                arrived(block_of(plane, 1 - core, 1 - y, 1 - x), part)

        return run

    def settled():
        for copy in locals_:
            copy.wait()

    inside = jnp.logical_and(can_up, can_down)
    steps_along = [along(n) for n in range(1, PLANES)]

    def hop(n, condition):
        return lambda: pl.when(condition)(steps_along[n - 1])

    outside = jnp.logical_not(inside)
    work = (
        (across(0), steps_along[0], hop(2, inside), diagonal(0), settled),
        (across(1), hop(2, outside), hop(3, inside), paired(0)),
        (hop(3, outside), diagonal(1)),
        (across(2), paired(1)),
        (across(3), diagonal(2)),
        (diagonal(3), paired(2)),
        (),
        (paired(3),),
    )
    group = 4 * tok
    steps = len(work)
    cap = gs.shape[0] // 4
    me = block_of(z, core, y, x)

    def group_of(i):
        if isinstance(i, int):
            plane = order[i // 2]
        else:
            plane = sum((i // 2 == n).astype(jnp.int32) * order[n] for n in range(PLANES))
        return plane * 2 + (core + i % 2) % 2

    def group_rows(ref, i):
        return ref.at[pl.ds(pl.multiple_of(group_of(i) * group, group), group)]

    def load_g(i):
        return pltpu.make_async_copy(
            group_rows(upstream_ref, i), g_hold.at[i % 2], load_sem.at[i % 2]
        )

    def load_x(i):
        return pltpu.make_async_copy(group_rows(x_all, i), x_hold, load_sem.at[2])

    def load_t(i):
        size = 4 * rows[1]
        return pltpu.make_async_copy(
            table_all.at[pl.ds(pl.multiple_of(group_of(i) * size, size), size)],
            t_hold,
            load_sem.at[3],
        )

    def store(i):
        held = pl.ds(pl.multiple_of(i * 4 * cap, 4 * cap), 4 * cap)
        return [
            pltpu.make_async_copy(hold.at[i % 2], target, store_sem.at[n, i % 2])
            for n, (hold, target) in enumerate(
                (
                    (out_hold, group_rows(out_ref, i)),
                    (grad_hold, group_rows(grad_ref, i)),
                    (rows_hold, rows_out.at[:, held]),
                    (hidden_hold, hidden_out.at[:, held]),
                )
            )
        ]

    def dot(left, right, dims):
        return lax.dot_general(
            left, right, ((dims[:1], dims[1:]), ((), ())), preferred_element_type=jnp.float32
        )

    load_g(0).start()

    @pl.loop(0, steps)
    def _(i):
        for n in range(steps):
            if work[n]:

                @pl.when(i == n)
                def _():
                    for run in work[n]:
                        run()

        load_x(i).start()
        load_t(i).start()

        @pl.when(i + 1 < steps)
        def _():
            load_g(i + 1).start()

        @pl.when(i >= 2)
        def _():
            for copy in store(i - 2):
                copy.wait()

        load_t(i).wait()
        load_x(i).wait()
        load_g(i).wait()
        slot = i % 2
        chosen, gate_cols = [], []
        for pair in range(2):
            first = [(pair * 2 + j) * 2 * experts + me for j in range(2)]
            gate_row = jnp.concatenate([t_hold[pl.ds(at, 1), :] for at in first], axis=1)
            slot_row = jnp.concatenate(
                [
                    t_hold[pl.ds(at + experts, 1), :] + float(cap * j)
                    for j, at in enumerate(first)
                ],
                axis=1,
            )
            ids = lax.broadcasted_iota(jnp.int32, (2 * cap, 2 * tok), 0).astype(jnp.float32)
            mask = jnp.where(ids == slot_row, 1.0, 0.0)
            pick = mask.astype(jnp.bfloat16)
            held = pl.ds(pair * 2 * cap, 2 * cap)
            tokens = pl.ds(pair * 2 * tok, 2 * tok)
            gate = jnp.sum(mask * gate_row, axis=1, keepdims=True)
            rows_hold[slot, 0, held] = dot(pick, x_hold[tokens], (1, 0)).astype(jnp.bfloat16)
            upstream = dot(pick, g_hold[slot, tokens], (1, 0))
            gs[held] = upstream.astype(jnp.bfloat16)
            rows_hold[slot, 1, held] = (upstream * gate).astype(jnp.bfloat16)
            chosen.append(pick)
            gate_cols.append(gate)
        rows_x = rows_hold[slot, 0]
        rows_g = rows_hold[slot, 1]
        gate_pre = dot(rows_x, w_ref[0], (1, 0))
        up_pre = dot(rows_x, w_ref[1], (1, 0))
        sig = jax.nn.sigmoid(gate_pre)
        silu = gate_pre * sig
        hidden = (silu * up_pre).astype(jnp.bfloat16)
        grad_hidden = dot(rows_g, w_ref[2], (1, 0))
        grad_gate = (grad_hidden * up_pre * sig * (1.0 + gate_pre * (1.0 - sig))).astype(
            jnp.bfloat16
        )
        grad_up = (grad_hidden * silu).astype(jnp.bfloat16)
        result = dot(hidden, w_ref[2], (1, 1)).astype(jnp.bfloat16)
        grad_in = (dot(grad_gate, w_ref[0], (1, 1)) + dot(grad_up, w_ref[1], (1, 1))).astype(
            jnp.bfloat16
        )
        hidden_hold[slot, 0] = grad_gate
        hidden_hold[slot, 1] = grad_up
        hidden_hold[slot, 2] = hidden
        result_f = result.astype(jnp.float32)
        share = jnp.sum(gs[...].astype(jnp.float32) * result_f, axis=1, keepdims=True)
        for pair in range(2):
            tokens = pl.ds(pair * 2 * tok, 2 * tok)
            low, high = pair * 2 * cap, (pair + 1) * 2 * cap
            pick = chosen[pair]
            scaled = (result_f[low:high] * gate_cols[pair]).astype(jnp.bfloat16)
            out_hold[slot, tokens] = dot(pick, scaled, (0, 0)).astype(jnp.bfloat16)
            grad_hold[slot, tokens] = dot(pick, grad_in[low:high], (0, 0)).astype(jnp.bfloat16)
            row = jnp.sum(pick.astype(jnp.float32) * share[low:high], axis=0, keepdims=True)
            for j in range(2):
                gg_ref[pl.ds(group_of(i) * 4 + pair * 2 + j, 1), :] = row[
                    :, j * tok : (j + 1) * tok
                ]
        for copy in store(i):
            copy.start()

    for i in (steps - 2, steps - 1):
        for copy in store(i):
            copy.wait()
    for condition, finish in pending:
        if condition is None:
            finish()
        else:
            pl.when(condition)(finish)


def run_experts(tokens, table, upstream, weights, cap, collective_id):
    tok, width = tokens.shape
    _, three, _, ff = weights.shape
    devices = 32
    total = tok * devices
    held = 4 * cap
    group = 4 * tok
    return pl.pallas_call(
        experts_kernel,
        out_shape=[
            jax.ShapeDtypeStruct((total, width), tokens.dtype),
            jax.ShapeDtypeStruct((table.shape[0] * devices, tok), table.dtype),
            jax.ShapeDtypeStruct((total, width), jnp.bfloat16),
            jax.ShapeDtypeStruct((total, width), jnp.bfloat16),
            jax.ShapeDtypeStruct((devices, tok), jnp.float32),
            jax.ShapeDtypeStruct((2, 8 * held, width), jnp.bfloat16),
            jax.ShapeDtypeStruct((3, 8 * held, ff), jnp.bfloat16),
        ],
        in_specs=[
            pl.BlockSpec(memory_space=pltpu.VMEM),
            pl.BlockSpec(memory_space=pltpu.VMEM),
            pl.BlockSpec(memory_space=pltpu.HBM),
            pl.BlockSpec(memory_space=pltpu.VMEM),
        ],
        out_specs=[pl.BlockSpec(memory_space=pltpu.HBM)] * 4
        + [pl.BlockSpec(memory_space=pltpu.VMEM)]
        + [pl.BlockSpec(memory_space=pltpu.HBM)] * 2,
        scratch_shapes=[
            pltpu.VMEM((held, width), jnp.bfloat16),
            pltpu.VMEM((2, 2, held, width), jnp.bfloat16),
            pltpu.VMEM((2, 3, held, ff), jnp.bfloat16),
            pltpu.VMEM((group, width), jnp.bfloat16),
            pltpu.VMEM((2, group, width), jnp.bfloat16),
            pltpu.VMEM((4 * table.shape[0], tok), jnp.float32),
            pltpu.VMEM((2, group, width), jnp.bfloat16),
            pltpu.VMEM((2, group, width), jnp.bfloat16),
            pltpu.SemaphoreType.DMA((2, 44)),
            pltpu.SemaphoreType.DMA((2, 64)),
            pltpu.SemaphoreType.DMA((2,)),
            pltpu.SemaphoreType.DMA((4,)),
            pltpu.SemaphoreType.DMA((4, 2)),
        ],
        compiler_params=pltpu.CompilerParams(
            collective_id=collective_id, has_side_effects=True, vmem_limit_bytes=63 << 20
        ),
        name="run_experts",
    )(tokens, table, upstream, weights.reshape(three, width, ff))


def add_rows(target, sources, rows=128, step=16):
    @pl.loop(0, rows // step)
    def _(i):
        where = pl.ds(pl.multiple_of(i * step, step), step)
        total = target[where].astype(jnp.float32)
        for source in sources:
            total += source[where].astype(jnp.float32)
        target[where] = total.astype(target.dtype)


def rolled(values):
    return pltpu.roll(values, HEAD_SIZE // 2, 1)


def inverse_rms(values):
    return lax.rsqrt(jnp.mean(values * values, axis=1, keepdims=True) + epsilon)


def mm(left, right, dims):
    return lax.dot_general(
        left, right, ((dims[:1], dims[1:]), ((), ())), preferred_element_type=jnp.float32
    )


def fill_bias(bias, seg_col, seg_row):
    seq = bias.shape[0]
    key = lax.broadcasted_iota(jnp.int32, (seq, seq), 0)
    query = lax.broadcasted_iota(jnp.int32, (seq, seq), 1)
    same = seg_col[...] == seg_row[...]
    bias[...] = jnp.where(jnp.logical_and(same, key <= query), 0.0, -1e30)


def attend_kernel(
    x_ref,
    weight_ref,
    w_out_ref,
    gain_ref,
    q_gain_ref,
    k_gain_ref,
    cos_ref,
    sin_ref,
    seg_col,
    seg_row,
    normed_ref,
    raw_ref,
    q_ref,
    k_ref,
    v_ref,
    attended_ref,
    lse_ref,
    part_ref,
    bias,
):
    seq = x_ref.shape[0]
    size = HEAD_SIZE
    heads = q_ref.shape[1] // size
    scale = size ** (-0.5)

    @pl.loop(0, seq // 64)
    def _(n):
        rows = pl.ds(pl.multiple_of(n * 64, 64), 64)
        x = x_ref[rows].astype(jnp.float32)
        normed_ref[rows] = (x * inverse_rms(x) * gain_ref[...]).astype(jnp.bfloat16)

    fill_bias(bias, seg_col, seg_row)

    @pl.loop(0, raw_ref.shape[1] // 256)
    def _(n):
        columns = pl.ds(pl.multiple_of(n * 256, 256), 256)
        raw_ref[:, columns] = mm(normed_ref[...], weight_ref[:, columns], (1, 0))

    def turned(raw, gain_row):
        normed = raw * inverse_rms(raw) * gain_row
        return (normed * cos_ref[...] + rolled(normed) * sin_ref[...]).astype(jnp.bfloat16)

    k_ref[...] = turned(raw_ref[:, heads * size : (heads + 1) * size], k_gain_ref[...])
    v_ref[...] = raw_ref[:, (heads + 1) * size :].astype(jnp.bfloat16)
    half = seq // 2

    @pl.loop(0, heads)
    def _(h):
        columns = pl.ds(pl.multiple_of(h * size, size), size)
        q_ref[:, columns] = turned(raw_ref[:, columns], q_gain_ref[...])
        for first, keys in ((0, half), (half, seq)):
            queries = pl.ds(first, half)
            score = mm(k_ref[:keys], q_ref[queries, columns], (1, 1)) * scale
            score = score + bias[:keys, first : first + half]
            highest = jnp.max(score, axis=0, keepdims=True)
            power = jnp.exp(score - highest)
            total = jnp.sum(power, axis=0, keepdims=True)
            lse_ref[pl.ds(h, 1), queries] = highest + jnp.log(total)
            probs = (power * (1.0 / total)).astype(jnp.bfloat16)
            attended_ref[queries, columns] = mm(probs, v_ref[:keys], (0, 0)).astype(jnp.bfloat16)

    @pl.loop(0, part_ref.shape[1] // 512)
    def _(n):
        columns = pl.ds(pl.multiple_of(n * 512, 512), 512)
        part_ref[:, columns] = mm(attended_ref[...], w_out_ref[:, columns], (1, 0)).astype(
            jnp.bfloat16
        )


def attend(x, weight, w_out, gain, q_gain, k_gain, cosine, sine, segments):
    seq, width = x.shape
    columns = weight.shape[1]
    heads = w_out.shape[0] // HEAD_SIZE
    bf, f4 = jnp.bfloat16, jnp.float32
    out = jax.ShapeDtypeStruct
    return pl.pallas_call(
        attend_kernel,
        out_shape=[
            out((seq, width), bf),
            out((seq, columns), f4),
            out((seq, heads * HEAD_SIZE), bf),
            out((seq, HEAD_SIZE), bf),
            out((seq, HEAD_SIZE), bf),
            out((seq, heads * HEAD_SIZE), bf),
            out((heads, seq), f4),
            out((seq, width), bf),
        ],
        in_specs=[pl.BlockSpec(memory_space=pltpu.VMEM)] * 10,
        out_specs=[pl.BlockSpec(memory_space=pltpu.VMEM)] * 8,
        scratch_shapes=[pltpu.VMEM((seq, seq), f4)],
        compiler_params=pltpu.CompilerParams(vmem_limit_bytes=56 << 20),
        name="attend",
    )(
        x,
        weight,
        w_out,
        gain[None],
        q_gain[None],
        k_gain[None],
        cosine,
        sine,
        segments[:, None],
        segments[None],
    )


def backward_steps(refs):
    q_ref, k_ref, v_ref, raw_ref, upstream, lse_ref = refs[:6]
    q_gain_ref, k_gain_ref, cos_ref, sin_ref, seg_col, seg_row = refs[6:12]
    grad_ref, gains_ref, bias, grad_k, grad_v = refs[12:]
    seq, size = k_ref.shape
    heads = q_ref.shape[1] // size
    scale = size ** (-0.5)
    half = seq // 2

    def prepare():
        fill_bias(bias, seg_col, seg_row)
        grad_k[...] = jnp.zeros_like(grad_k)
        grad_v[...] = jnp.zeros_like(grad_v)
        gains_ref[...] = jnp.zeros_like(gains_ref)

    def turn_back(grad, queries, columns, gain, line):
        turned = grad * cos_ref[queries] + rolled(grad * sin_ref[queries])
        raw = raw_ref[queries, columns]
        inverse = inverse_rms(raw)
        scaled = turned * gain
        mean = jnp.mean(scaled * raw, axis=1, keepdims=True)
        grad_raw = inverse * scaled - raw * (inverse * inverse * inverse) * mean
        grad_ref[queries, columns] = grad_raw.astype(jnp.bfloat16)
        gains_ref[line : line + 1] += jnp.sum(turned * raw * inverse, axis=0, keepdims=True)

    def head(h):
        columns = pl.ds(pl.multiple_of(h * size, size), size)
        for first, keys in ((0, half), (half, seq)):
            queries = pl.ds(first, half)
            q, above = q_ref[queries, columns], upstream[queries, columns]
            score = mm(k_ref[:keys], q, (1, 1)) * scale + bias[:keys, first : first + half]
            probs = jnp.exp(score - lse_ref[pl.ds(h, 1), queries])
            grad_v[:keys] += mm(probs.astype(jnp.bfloat16), above, (1, 0))
            grad_p = mm(v_ref[:keys], above, (1, 1))
            delta = jnp.sum(probs * grad_p, axis=0, keepdims=True)
            grad_score = (probs * (grad_p - delta) * scale).astype(jnp.bfloat16)
            grad_k[:keys] += mm(grad_score, q, (1, 0))
            grad_q = mm(grad_score, k_ref[:keys], (0, 0))
            turn_back(grad_q, queries, columns, q_gain_ref[...], 0)

    def keys_and_values():
        for first in (0, half):
            queries = pl.ds(first, half)
            turn_back(grad_k[queries], queries, pl.ds(heads * size, size), k_gain_ref[...], 1)
        grad_ref[:, (heads + 1) * size :] = grad_v[...].astype(jnp.bfloat16)

    return prepare, head, keys_and_values


class Sends:
    def __init__(self, send_sem, partner):
        self.send_sem, self.partner, self.used, self.pending = send_sem, partner, 0, []

    def make(self, source, landing, sem, target, *conditions):
        copy = remote(source, landing, self.send_sem.at[self.used], sem, target)
        self.used += 1
        self.pending.append((conditions, copy))
        return copy

    def send(self, source, landing, sem, target):
        self.make(source, landing, sem, target).start()

    def arrived(self, landing, sem):
        remote(landing, landing, self.send_sem.at[0], sem, self.partner).wait_recv()

    def finish(self):
        for conditions, copy in self.pending:
            if not conditions:
                copy.wait_send()
            elif len(conditions) == 1:
                pl.when(conditions[0])(copy.wait_send)
            else:
                pl.when(jnp.logical_and(*conditions))(copy.wait_send)


def add_into(target, sources, rows):
    @pl.loop(0, rows // 16)
    def _(n):
        where = pl.ds(pl.multiple_of(n * 16, 16), 16)
        total = sources[0][where].astype(jnp.float32)
        for source in sources[1:]:
            total += source[where].astype(jnp.float32)
        target[where] = total.astype(target.dtype)


def ladder(sends, count, before, piece, from_up, from_down, final, size, sems):
    climb_send, spread_send, close_send, climb_sem, spread_sem, close_sem = sems
    z, core, y, x = place()
    partner = sends.partner
    up, down = device(z + 1, core, y, x), device(z - 1, core, y, x)
    can_up, can_down = z < PLANES - 1, z > 0

    def climb(n, rising):
        landing = from_down(n) if rising else from_up(n)
        side = 1 if rising else 0
        return remote(
            piece(n), landing, climb_send.at[n], climb_sem.at[n, side], up if rising else down
        )

    def gained(n, rising):
        landing = from_down(n) if rising else from_up(n)
        sends.arrived(landing, climb_sem.at[n, 1 if rising else 0])
        return landing

    def spread(n, rising):
        block = final(n, core)
        target = up if rising else down
        return remote(block, block, spread_send.at[n, 1 if rising else 0], spread_sem.at[n], target)

    def hand_over(n):
        block = final(n, core)
        return remote(block, block, close_send.at[n], close_sem.at[n], partner)

    def ends(n, root):
        before(n)
        pl.when(z == 0)(climb(n, True).start)
        pl.when(z == PLANES - 1)(climb(n, False).start)

    def between(n, root):
        for rising, level in ((True, 1), (False, 2)):

            @pl.when(jnp.logical_and(z == level, root == 3 - level))
            def _():
                add_rows(piece(n), (gained(n, rising),), size)
                climb(n, rising).start()

    def settle(n, root):
        @pl.when(z == root)
        def _():
            add_into(final(n, core), (piece(n), gained(n, True), gained(n, False)), size)
            spread(n, True).start()
            spread(n, False).start()
            hand_over(n).start()

    def receive(n, root, distance):
        for rising, there, more in (
            (True, z == root + distance, can_up),
            (False, z == root - distance, can_down),
        ):

            @pl.when(there)
            def _():
                sends.arrived(final(n, core), spread_sem.at[n])
                pl.when(more)(spread(n, rising).start)
                hand_over(n).start()

    stages = (
        ends,
        between,
        settle,
        functools.partial(receive, distance=1),
        functools.partial(receive, distance=2),
    )

    def step(m):
        for stage, run in enumerate(stages):
            n = m - stage * SLACK

            @pl.when(jnp.logical_and(n >= 0, n < count))
            def _():
                run(n, 1 + n % 2)

    def close():
        @pl.loop(0, count)
        def _(n):
            root = 1 + n % 2
            pl.when(z != root)(climb(n, True).wait_send)
            pl.when(jnp.logical_and(z >= root, can_up))(spread(n, True).wait_send)
            pl.when(jnp.logical_and(z <= root, can_down))(spread(n, False).wait_send)
            hand_over(n).wait_send()

    def closed(n):
        sends.arrived(final(n, 1 - core), close_sem.at[n])

    return step, closed, close


SLACK = 2
LADDER_MORE = 4 * SLACK


def ladder_scratch(count):
    return [
        pltpu.SemaphoreType.DMA((count,)),
        pltpu.SemaphoreType.DMA((count, 2)),
        pltpu.SemaphoreType.DMA((count,)),
        pltpu.SemaphoreType.DMA((count, 2)),
        pltpu.SemaphoreType.DMA((count,)),
        pltpu.SemaphoreType.DMA((count,)),
    ]


LADDER = 32
PER = LADDER // 4


def reduce_kernel(with_weight, *refs):
    refs = list(refs)
    part_ref = refs.pop(0)
    weight_ref = refs.pop(0) if with_weight else None
    back = [refs.pop(0) for _ in range(12)] if with_weight else []
    rows_ref, hidden_ref = (None, None) if with_weight else (refs.pop(0), refs.pop(0))
    out_ref = refs.pop(0)
    weight_out = refs.pop(0) if with_weight else None
    grad_w = None if with_weight else refs.pop(0)
    back += [refs.pop(0) for _ in range(2)] if with_weight else []
    kept, paired, x_half, x_full, y_half, y_full, from_up, from_down = refs[:8]
    send_sem, pair_sem, x_sem, y_sem, z_sem, load_sem, step_sem = refs[8:15]
    refs = refs[:8] + refs[9:]
    rows = out_ref.shape[0]
    half = rows // 2
    z, core, y, x = place()
    partner = device(z, 1 - core, y, x)
    x_next, y_next = device(z, core, y, 1 - x), device(z, core, 1 - y, x)
    up, down = device(z + 1, core, y, x), device(z - 1, core, y, x)
    greet(
        [
            (None, partner),
            (None, x_next),
            (None, y_next),
            (z < PLANES - 1, up),
            (z > 0, down),
        ]
    )
    sends = Sends(send_sem, partner)
    tables = ((3, 2, 1, 0), (3, 0, 2, 1), (0, 3, 1, 2), (0, 1, 2, 3))
    order = [
        sum((z == level).astype(jnp.int32) * tables[level][n] for level in range(PLANES))
        for n in range(PLANES)
    ]

    def plane_at(n):
        return sum((n == k).astype(jnp.int32) * order[k] for k in range(PLANES))

    spots = ((1 - y, 1 - x), (y, 1 - x), (1 - y, x), (y, x))

    def slot(plane, spot):
        return plane * 4 + spots[spot][0] * 2 + spots[spot][1]

    def block(plane, which, spot):
        size = pl.multiple_of(block_of(plane, which, *spots[spot]) * rows, rows)
        return part_ref.at[pl.ds(size, rows)]

    def load(plane, spot):
        return pltpu.make_async_copy(
            block(plane, core, spot), kept.at[slot(plane, spot)], load_sem.at[spot * 4 + plane]
        )

    for spot in range(4):
        for plane in order:
            where = slot(plane, spot)
            sends.send(block(plane, 1 - core, spot), paired.at[where], pair_sem.at[where], partner)
            load(plane, spot).start()
    if with_weight:
        out_pair, out_part, out_up, out_down, out_done = refs[14:19]
        out_pair_sem, out_sem = refs[19:21]
        out_half = weight_ref.shape[0] // 2
        out_block = out_half // LADDER
        big = out_half // 4

        def out_rows(n, which, count=1):
            start = pl.multiple_of(which * out_half + n * out_block, out_block)
            return weight_ref.at[pl.ds(start, out_block * count)]

        for n in range(4):
            sends.send(out_rows(n * PER, 1 - core, PER), out_pair.at[n], out_pair_sem.at[n], partner)

        def before(n):
            @pl.when(n % PER == 0)
            def _():
                where = n // PER
                sends.arrived(out_pair.at[where], out_pair_sem.at[where])
                add_into(out_part.at[where], (out_rows(n, core, PER), out_pair.at[where]), big)

        def done_rows(n, which):
            start = pl.multiple_of(which * out_half + n * out_block, out_block)
            return out_done.at[pl.ds(start, out_block)]

        ladder_step, closed, close = ladder(
            sends,
            LADDER,
            before,
            lambda n: out_part.at[
                n // PER, pl.ds(pl.multiple_of((n % PER) * out_block, out_block), out_block)
            ],
            lambda n: out_up.at[n],
            lambda n: out_down.at[n],
            done_rows,
            out_block,
            refs[21:27],
        )
        fill = backward_steps(back + refs[27:])

    else:
        rows_hold, hidden_hold, sums, part_sem, sum_sem = refs[14:]
        held = rows_hold.shape[2]

        def fetch(i):
            span = pl.ds(pl.multiple_of(i * held, held), held)
            return (
                pltpu.make_async_copy(
                    rows_ref.at[:, span], rows_hold.at[i % 2], part_sem.at[0, i % 2]
                ),
                pltpu.make_async_copy(
                    hidden_ref.at[:, span], hidden_hold.at[i % 2], part_sem.at[1, i % 2]
                ),
            )

        parts = rows_ref.shape[1] // held
        for copy in fetch(0):
            copy.start()

        sums[...] = jnp.zeros_like(sums)

        def add_product(i):
            @pl.when(i + 1 < parts)
            def _():
                for copy in fetch(i + 1):
                    copy.start()

            for copy in fetch(i):
                copy.wait()
            stripes = sums.shape[1] // 512

            @pl.loop(0, 3 * stripes)
            def _(n):
                matrix = n // stripes
                span = pl.ds(pl.multiple_of((n % stripes) * 512, 512), 512)
                sums[matrix, span] += mm(
                    rows_hold[i % 2, matrix // 2, :, span], hidden_hold[i % 2, matrix], (0, 0)
                )

        write_sums = pltpu.make_async_copy(sums, grad_w.at[0], sum_sem)

    def joined(plane, spot, more=()):
        where = slot(plane, spot)
        load(plane, spot).wait()
        sends.arrived(paired.at[where], pair_sem.at[where])
        add_rows(kept.at[where], (paired.at[where],) + tuple(more), rows)

    def across_copies(plane):
        source = kept.at[slot(plane, 0)]
        return (
            remote(
                source.at[pl.ds(0, half)],
                x_half.at[plane],
                step_sem.at[0, plane],
                x_sem.at[plane],
                x_next,
            ),
            remote(
                source.at[pl.ds(half, half)],
                y_half.at[plane],
                step_sem.at[1, plane],
                y_sem.at[plane],
                y_next,
            ),
        )

    def beside_copies(plane):
        return (
            remote(
                kept.at[slot(plane, 1)],
                x_full.at[plane],
                step_sem.at[2, plane],
                x_sem.at[4 + plane],
                x_next,
            ),
            remote(
                kept.at[slot(plane, 2)],
                y_full.at[plane],
                step_sem.at[3, plane],
                y_sem.at[4 + plane],
                y_next,
            ),
        )

    def across(plane):
        joined(plane, 0)
        for copy in across_copies(plane):
            copy.start()

    def beside(plane):
        along_x, along_y = beside_copies(plane)
        joined(plane, 1)
        sends.arrived(y_half.at[plane], y_sem.at[plane])
        add_rows(kept.at[slot(plane, 1)].at[pl.ds(half, half)], (y_half.at[plane],), half)
        along_x.start()
        joined(plane, 2)
        sends.arrived(x_half.at[plane], x_sem.at[plane])
        add_rows(kept.at[slot(plane, 2)].at[pl.ds(0, half)], (x_half.at[plane],), half)
        along_y.start()

    def along(plane):
        sends.arrived(x_full.at[plane], x_sem.at[4 + plane])
        sends.arrived(y_full.at[plane], y_sem.at[4 + plane])
        joined(plane, 3, (x_full.at[plane], y_full.at[plane]))

    def onward(plane):
        total = kept.at[slot(plane, 3)]
        return (
            remote(total, from_up.at[plane], step_sem.at[4, plane], z_sem.at[0, plane], down),
            remote(total, from_down.at[plane], step_sem.at[4, plane], z_sem.at[1, plane], up),
        )

    def pass_on(plane, first):
        total = kept.at[slot(plane, 3)]
        fall, rise = onward(plane)
        for copy, way, end, landing, sem in (
            (fall, z > plane, z == PLANES - 1, from_up.at[plane], z_sem.at[0, plane]),
            (rise, z < plane, z == 0, from_down.at[plane], z_sem.at[1, plane]),
        ):
            if first:
                pl.when(jnp.logical_and(way, end))(copy.start)
            else:

                @pl.when(jnp.logical_and(way, jnp.logical_not(end)))
                def _():
                    sends.arrived(landing, sem)
                    add_rows(total, (landing,), rows)
                    copy.start()

    if with_weight:
        fill[0]()
        share = (LADDER + LADDER_MORE) // (2 * PLANES)
    for late, run in enumerate((across, beside)):

        @pl.loop(0, PLANES)
        def _(n):
            run(plane_at(n))
            if with_weight:
                if not late:
                    fill[1](n)
                first = (late * PLANES + n) * share

                @pl.loop(0, share)
                def _(m):
                    ladder_step(first + m)
            else:
                add_product(late * PLANES + n)

    if not with_weight:
        write_sums.start()

    @pl.loop(0, PLANES)
    def _(n):
        plane = plane_at(n)
        along(plane)

        @pl.when(n < PLANES - 1)
        def _():
            pass_on(plane, True)

        @pl.when(n > 0)
        def _():
            pass_on(plane_at(n - 1), False)

        if with_weight:
            fill[1](PLANES + n)

    if with_weight:
        fill[-1]()
    mine = kept.at[slot(z, 3)]

    @pl.when(z < PLANES - 1)
    def _():
        sends.arrived(from_up.at[z], z_sem.at[0, z])
        add_rows(mine, (from_up.at[z],), rows)

    @pl.when(z > 0)
    def _():
        sends.arrived(from_down.at[z], z_sem.at[1, z])
        add_rows(mine, (from_down.at[z],), rows)

    out_ref[...] = mine[...]
    if with_weight:

        @pl.loop(0, LADDER)
        def _(n):
            closed(n)

        write = pltpu.make_async_copy(out_done, weight_out, out_sem)
        write.start()
        close()
        write.wait()
    else:
        write_sums.wait()

    @pl.loop(0, PLANES)
    def _(plane):
        for copy in across_copies(plane) + beside_copies(plane):
            copy.wait_send()
        pl.when(plane != z)(onward(plane)[0].wait_send)

    sends.finish()


def reduce_all(part, collective_id, weight=None, back=(), expert=()):
    total, width = part.shape
    rows = total // 32
    half = rows // 2
    dtype = part.dtype
    out_shape = [jax.ShapeDtypeStruct((rows, width), dtype)]
    in_specs = [pl.BlockSpec(memory_space=pltpu.HBM)]
    out_specs = [pl.BlockSpec(memory_space=pltpu.VMEM)]
    scratch = [
        pltpu.VMEM((16, rows, width), dtype),
        pltpu.VMEM((16, rows, width), dtype),
        pltpu.VMEM((4, half, width), dtype),
        pltpu.VMEM((4, rows, width), dtype),
        pltpu.VMEM((4, half, width), dtype),
        pltpu.VMEM((4, rows, width), dtype),
        pltpu.VMEM((4, rows, width), dtype),
        pltpu.VMEM((4, rows, width), dtype),
        pltpu.SemaphoreType.DMA((20,)),
        pltpu.SemaphoreType.DMA((16,)),
        pltpu.SemaphoreType.DMA((8,)),
        pltpu.SemaphoreType.DMA((8,)),
        pltpu.SemaphoreType.DMA((2, 4)),
        pltpu.SemaphoreType.DMA((16,)),
        pltpu.SemaphoreType.DMA((5, 4)),
    ]
    operands = [part]
    if weight is not None:
        operands.append(weight)
        block = weight.shape[0] // 8
        seq = back[0].shape[0]
        operands += back
        out_shape += [
            jax.ShapeDtypeStruct(weight.shape, dtype),
            jax.ShapeDtypeStruct(back[3].shape, dtype),
            jax.ShapeDtypeStruct((8, HEAD_SIZE), jnp.float32),
        ]
        in_specs += [pl.BlockSpec(memory_space=pltpu.VMEM)] * (1 + len(back))
        out_specs += [
            pl.BlockSpec(memory_space=pltpu.HBM),
            pl.BlockSpec(memory_space=pltpu.VMEM),
            pl.BlockSpec(memory_space=pltpu.VMEM),
        ]
        scratch += [
            pltpu.VMEM((4, block, width), dtype),
            pltpu.VMEM((4, block, width), dtype),
            pltpu.VMEM((LADDER, weight.shape[0] // 2 // LADDER, width), dtype),
            pltpu.VMEM((LADDER, weight.shape[0] // 2 // LADDER, width), dtype),
            pltpu.VMEM(weight.shape, dtype),
            pltpu.SemaphoreType.DMA((4,)),
            pltpu.SemaphoreType.DMA,
        ] + ladder_scratch(LADDER)
        scratch += [
            pltpu.VMEM((seq, seq), jnp.float32),
            pltpu.VMEM((seq, HEAD_SIZE), jnp.float32),
            pltpu.VMEM((seq, HEAD_SIZE), jnp.float32),
        ]
    else:
        rows_held, hidden_held = expert
        held, ff = rows_held.shape[1] // 8, hidden_held.shape[2]
        operands += expert
        in_specs += [pl.BlockSpec(memory_space=pltpu.HBM)] * 2
        out_shape.append(jax.ShapeDtypeStruct((1, 3, width, ff), jnp.float32))
        out_specs.append(pl.BlockSpec(memory_space=pltpu.HBM))
        scratch += [
            pltpu.VMEM((2, 2, held, width), dtype),
            pltpu.VMEM((2, 3, held, ff), dtype),
            pltpu.VMEM((3, width, ff), jnp.float32),
            pltpu.SemaphoreType.DMA((2, 2)),
            pltpu.SemaphoreType.DMA,
        ]
    return pl.pallas_call(
        functools.partial(reduce_kernel, weight is not None),
        out_shape=out_shape,
        in_specs=in_specs,
        out_specs=out_specs,
        scratch_shapes=scratch,
        compiler_params=pltpu.CompilerParams(
            collective_id=collective_id, has_side_effects=True, vmem_limit_bytes=63 << 20
        ),
        name="reduce_all",
    )(*operands)


def others():
    z, core, y, x = place()
    return [
        (device(z, core, yy, xx), yy * 2 + xx)
        for yy, xx in ((y, 1 - x), (1 - y, x), (1 - y, 1 - x))
    ]


def remote(source, landing, send_sem, recv_sem, target):
    return pltpu.make_async_remote_copy(
        src_ref=source,
        dst_ref=landing,
        send_sem=send_sem,
        recv_sem=recv_sem,
        device_id=target,
        device_id_type=MESH_ID,
    )


def start_kernel(
    x_ref, w_ref, x_all, w_own, hold, send_sem, x_sem, w_sem, pair_sem, own_sem
):
    tok = x_ref.shape[0]
    depth = w_ref.shape[0]
    half = depth // 2
    z, core, y, x = place()
    me = y * 2 + x
    partner = device(z, 1 - core, y, x)
    near = others()
    greet([(None, target) for target, _ in near] + [(None, partner)])
    parts = QUERY_HEADS // 4 * HEAD_SIZE
    single = HEAD_SIZE
    widths = (
        (0, parts, 0),
        (QUERY_HEADS * HEAD_SIZE, single, parts),
        ((QUERY_HEADS + KEY_VALUE_HEADS) * HEAD_SIZE, single, parts + single),
    )

    def columns(piece, who):
        base, width, _ = widths[piece]
        return pl.ds(pl.multiple_of(base + who * width, 128), width)

    def landing(piece, who, part, ref=w_own):
        _, width, offset = widths[piece]
        rows = pl.ds(pl.multiple_of(who * depth + part * half, half), half)
        return ref.at[rows, pl.ds(offset, width)]

    sends = []
    for slot, (target, who) in enumerate(near):
        for piece in range(3):
            copy = remote(
                w_ref.at[pl.ds(pl.multiple_of(core * half, half), half), columns(piece, who)],
                landing(piece, me, core),
                send_sem.at[slot * 4 + piece],
                w_sem.at[slot * 3 + piece],
                target,
            )
            copy.start()
            sends.append(copy)
        copy = remote(
            x_ref,
            x_all.at[pl.ds(pl.multiple_of(me * tok, tok), tok)],
            send_sem.at[slot * 4 + 3],
            x_sem.at[slot],
            target,
        )
        copy.start()
        sends.append(copy)
    mine = pltpu.make_async_copy(
        x_ref, x_all.at[pl.ds(pl.multiple_of(me * tok, tok), tok)], own_sem.at[0]
    )
    mine.start()
    loads = []
    for piece in range(3):
        _, width, offset = widths[piece]
        loads.append(
            pltpu.make_async_copy(
                w_ref.at[:, columns(piece, me)], hold.at[:, pl.ds(offset, width)], own_sem.at[1 + piece]
            )
        )
        loads[-1].start()
    for copy in loads:
        copy.wait()
    keep = pltpu.make_async_copy(
        hold, w_own.at[pl.ds(pl.multiple_of(me * depth, depth), depth)], own_sem.at[4]
    )
    keep.start()
    for slot, (target, who) in enumerate(near):
        for piece in range(3):
            where = landing(piece, who, core)
            remote(where, where, send_sem.at[0], w_sem.at[slot * 3 + piece], partner).wait_recv()
        rows = w_own.at[pl.ds(pl.multiple_of(who * depth + core * half, half), half)]
        copy = remote(rows, rows, send_sem.at[12 + slot], pair_sem.at[slot], partner)
        copy.start()
        sends.append(copy)
    for slot, (target, who) in enumerate(near):
        rows = w_own.at[pl.ds(pl.multiple_of(who * depth + (1 - core) * half, half), half)]
        remote(rows, rows, send_sem.at[0], pair_sem.at[slot], partner).wait_recv()
        rows = x_all.at[pl.ds(pl.multiple_of(who * tok, tok), tok)]
        remote(rows, rows, send_sem.at[0], x_sem.at[slot], partner).wait_recv()
    mine.wait()
    keep.wait()
    for copy in sends:
        copy.wait_send()


def start_exchange(block_in, weight, collective_id):
    tok, width = block_in.shape
    depth, columns = weight.shape
    return pl.pallas_call(
        start_kernel,
        out_shape=[
            jax.ShapeDtypeStruct((tok * 4, width), block_in.dtype),
            jax.ShapeDtypeStruct((depth * 4, columns // 4), weight.dtype),
        ],
        in_specs=[
            pl.BlockSpec(memory_space=pltpu.VMEM),
            pl.BlockSpec(memory_space=pltpu.HBM),
        ],
        out_specs=[pl.BlockSpec(memory_space=pltpu.HBM)] * 2,
        scratch_shapes=[
            pltpu.VMEM((depth, columns // 4), weight.dtype),
            pltpu.SemaphoreType.DMA((16,)),
            pltpu.SemaphoreType.DMA((3,)),
            pltpu.SemaphoreType.DMA((9,)),
            pltpu.SemaphoreType.DMA((3,)),
            pltpu.SemaphoreType.DMA((5,)),
        ],
        compiler_params=pltpu.CompilerParams(
            collective_id=collective_id, has_side_effects=True, vmem_limit_bytes=40 << 20
        ),
        name="start_exchange",
    )(block_in, weight)


def spread_kernel(x_ref, x_all, send_sem, x_sem, own_sem):
    tok = x_ref.shape[0]
    z, core, y, x = place()
    me = y * 2 + x
    near = others()
    greet([(None, target) for target, _ in near[:2]])
    sends = Sends(send_sem, near[0][0])

    def rows(who, part=None):
        if part is None:
            return x_all.at[pl.ds(pl.multiple_of(who * tok, tok), tok)]
        start = who * tok + part * (tok // 2)
        return x_all.at[pl.ds(pl.multiple_of(start, tok // 2), tok // 2)]

    for slot in range(2):
        for part in (1 - slot, slot):
            sends.send(
                x_ref.at[pl.ds(part * (tok // 2), tok // 2)],
                rows(me, part),
                x_sem.at[slot, part],
                near[slot][0],
            )
    own_x = pltpu.make_async_copy(x_ref, rows(me), own_sem)
    own_x.start()
    for slot in range(2):
        who, part = near[slot][1], 1 - slot
        sends.arrived(rows(who, part), x_sem.at[slot, part])
        sends.send(rows(who, part), rows(who, part), x_sem.at[2, part], near[1 - slot][0])
    for slot in range(2):
        sends.arrived(rows(near[slot][1], slot), x_sem.at[slot, slot])
    for part in range(2):
        sends.arrived(rows(near[2][1], part), x_sem.at[2, part])
    own_x.wait()
    sends.finish()


def spread_sequence(rows, collective_id):
    tok, width = rows.shape
    return pl.pallas_call(
        spread_kernel,
        out_shape=jax.ShapeDtypeStruct((tok * 4, width), rows.dtype),
        in_specs=[pl.BlockSpec(memory_space=pltpu.VMEM)],
        out_specs=pl.BlockSpec(memory_space=pltpu.HBM),
        scratch_shapes=[
            pltpu.SemaphoreType.DMA((6,)),
            pltpu.SemaphoreType.DMA((3, 2)),
            pltpu.SemaphoreType.DMA,
        ],
        compiler_params=pltpu.CompilerParams(
            collective_id=collective_id, has_side_effects=True, vmem_limit_bytes=40 << 20
        ),
        name="spread_sequence",
    )(rows)


def fold_kernel(part_ref, out_ref, across, beside, summed, send_sem, recv_sem):
    tok = out_ref.shape[0]
    half = tok // 2
    z, core, y, x = place()
    me = y * 2 + x
    near = others()
    greet([(None, target) for target, _ in near[:2]])
    sends = Sends(send_sem, near[0][0])

    def rows(who, part):
        start = who * tok + part * half
        return part_ref.at[pl.ds(pl.multiple_of(start, half), half)]

    def landing(slot, part):
        return beside.at[slot, pl.ds(part * half, half)]

    for slot in range(2):
        sends.send(rows(near[2][1], slot), across.at[slot], recv_sem.at[0, slot], near[slot][0])
    for slot in range(2):
        sends.send(
            rows(near[slot][1], slot), landing(slot, slot), recv_sem.at[1, slot], near[slot][0]
        )
    for slot in range(2):
        part = 1 - slot
        sends.arrived(across.at[part], recv_sem.at[0, part])
        add_into(summed.at[slot], (rows(near[slot][1], part), across.at[part]), half)
        sends.send(summed.at[slot], landing(slot, part), recv_sem.at[2, slot], near[slot][0])
    for slot in range(2):
        sends.arrived(landing(slot, slot), recv_sem.at[1, slot])
        sends.arrived(landing(slot, 1 - slot), recv_sem.at[2, slot])
    own = part_ref.at[pl.ds(pl.multiple_of(me * tok, tok), tok)]
    add_into(out_ref, (own, beside.at[0], beside.at[1]), tok)
    sends.finish()


def fold_sequence(part, collective_id):
    total, width = part.shape
    tok = total // 4
    return pl.pallas_call(
        fold_kernel,
        out_shape=jax.ShapeDtypeStruct((tok, width), jnp.float32),
        in_specs=[pl.BlockSpec(memory_space=pltpu.VMEM)],
        out_specs=pl.BlockSpec(memory_space=pltpu.VMEM),
        scratch_shapes=[
            pltpu.VMEM((2, tok // 2, width), part.dtype),
            pltpu.VMEM((2, tok, width), part.dtype),
            pltpu.VMEM((2, tok // 2, width), part.dtype),
            pltpu.SemaphoreType.DMA((6,)),
            pltpu.SemaphoreType.DMA((3, 2)),
        ],
        compiler_params=pltpu.CompilerParams(
            collective_id=collective_id, has_side_effects=True, vmem_limit_bytes=40 << 20
        ),
        name="fold_sequence",
    )(part)


def weight_kernel(
    grad_ref,
    fold_ref,
    out_ref,
    fold_out,
    pair,
    part,
    landed,
    from_up,
    from_down,
    done,
    folds,
    send_sem,
    pair_sem,
    cross_sem,
    fold_sem,
    write_sem,
    *ladder_sems,
):
    depth = done.shape[1]
    half = depth // 2
    block = half // PER
    tok = fold_out.shape[0]
    z, core, y, x = place()
    me = y * 2 + x
    partner = device(z, 1 - core, y, x)
    up, down = device(z + 1, core, y, x), device(z - 1, core, y, x)
    near = [(device(z, core, y, x), me)] + others()
    greet(
        [(None, partner)]
        + [(None, target) for target, _ in near[1:]]
        + [(z < PLANES - 1, up), (z > 0, down)]
    )
    sends = Sends(send_sem, partner)

    def own_rows(n, which):
        start = pl.multiple_of(near[n][1] * depth + which * half, half)
        return grad_ref.at[pl.ds(start, half)]

    for n in range(4):
        sends.send(own_rows(n, 1 - core), pair.at[n], pair_sem.at[n], partner)
    for n in range(4):
        sends.arrived(pair.at[n], pair_sem.at[n])
        target = part.at[n - 1] if n else landed.at[0]
        add_into(target, (own_rows(n, core), pair.at[n]), half)
        if n:
            sends.send(target, landed.at[n], cross_sem.at[n - 1], near[n][0])
    for n in (1, 2, 3):
        target, who = near[n]
        rows = fold_ref.at[pl.ds(pl.multiple_of(who * tok, tok), tok)]
        sends.send(rows, folds.at[n - 1], fold_sem.at[n - 1], target)

    def before(n):
        @pl.when(jnp.logical_and(n % PER == 0, n > 0))
        def _():
            sends.arrived(landed.at[n // PER], cross_sem.at[n // PER - 1])

    def done_rows(n, which):
        source = n // PER
        who = ((y + source // 2) % 2) * 2 + (x + source % 2) % 2
        start = pl.multiple_of(which * half + (n % PER) * block, block)
        return done.at[who, pl.ds(start, block)]

    ladder_step, closed, close = ladder(
        sends,
        LADDER,
        before,
        lambda n: landed.at[n // PER, pl.ds(pl.multiple_of((n % PER) * block, block), block)],
        lambda n: from_up.at[n],
        lambda n: from_down.at[n],
        done_rows,
        block,
        ladder_sems,
    )

    @pl.loop(0, LADDER + LADDER_MORE)
    def _(m):
        ladder_step(m)

    for n in range(3):
        sends.arrived(folds.at[n], fold_sem.at[n])
    add_into(
        fold_out,
        [fold_ref.at[pl.ds(pl.multiple_of(me * tok, tok), tok)]] + [folds.at[n] for n in range(3)],
        tok,
    )
    single = HEAD_SIZE
    heads = QUERY_HEADS // 4 * HEAD_SIZE
    writes = []

    @pl.loop(0, LADDER)
    def _(n):
        closed(n)

    for n in range(4):
        who = near[n][1]
        for c, (base, width, offset) in enumerate(
            (
                (0, heads, 0),
                (QUERY_HEADS * HEAD_SIZE, single, heads),
                ((QUERY_HEADS + KEY_VALUE_HEADS) * HEAD_SIZE, single, heads + single),
            )
        ):
            copy = pltpu.make_async_copy(
                done.at[who, :, pl.ds(offset, width)],
                out_ref.at[:, pl.ds(pl.multiple_of(base + who * width, 128), width)],
                write_sem.at[n * 3 + c],
            )
            copy.start()
            writes.append(copy)
    close()
    for copy in writes:
        copy.wait()
    sends.finish()


def weight_reduce(grad, fold, collective_id):
    rows, columns = grad.shape
    depth = rows // 4
    half = depth // 2
    tok, width = fold.shape[0] // 4, fold.shape[1]
    dtype = grad.dtype
    return pl.pallas_call(
        weight_kernel,
        out_shape=[
            jax.ShapeDtypeStruct((depth, columns * 4), dtype),
            jax.ShapeDtypeStruct((tok, width), jnp.float32),
        ],
        in_specs=[pl.BlockSpec(memory_space=pltpu.VMEM)] * 2,
        out_specs=[pl.BlockSpec(memory_space=pltpu.HBM), pl.BlockSpec(memory_space=pltpu.VMEM)],
        scratch_shapes=[
            pltpu.VMEM((4, half, columns), dtype),
            pltpu.VMEM((3, half, columns), dtype),
            pltpu.VMEM((4, half, columns), dtype),
            pltpu.VMEM((LADDER, half // PER, columns), dtype),
            pltpu.VMEM((LADDER, half // PER, columns), dtype),
            pltpu.VMEM((4, depth, columns), dtype),
            pltpu.VMEM((3, tok, width), dtype),
            pltpu.SemaphoreType.DMA((10,)),
            pltpu.SemaphoreType.DMA((4,)),
            pltpu.SemaphoreType.DMA((3,)),
            pltpu.SemaphoreType.DMA((3,)),
            pltpu.SemaphoreType.DMA((12,)),
        ]
        + ladder_scratch(LADDER),
        compiler_params=pltpu.CompilerParams(
            collective_id=collective_id, has_side_effects=True, vmem_limit_bytes=56 << 20
        ),
        name="weight_reduce",
    )(grad, fold)


def project_back_kernel(
    grad_ref,
    weight_ref,
    normed_ref,
    x_ref,
    experts_ref,
    part_ref,
    grad_weight_ref,
    gain_ref,
    experts_out,
    inverse,
    ring,
    load_sem,
    store_sem,
):
    stripes = x_ref.shape[1] // 256
    chunk = ring.shape[1]
    slots = ring.shape[0]
    each = experts_ref.shape[2] // chunk
    chunks = 3 * each
    per = chunks // stripes

    def rows(ref, c):
        return ref.at[0, c // each, pl.ds(pl.multiple_of((c % each) * chunk, chunk), chunk)]

    def load(c):
        return pltpu.make_async_copy(
            rows(experts_ref, c), ring.at[c % slots], load_sem.at[c % slots]
        )

    def store(c):
        return pltpu.make_async_copy(
            ring.at[c % slots], rows(experts_out, c), store_sem.at[c % slots]
        )

    for c in range(slots):
        load(c).start()

    @pl.loop(0, x_ref.shape[0] // 64)
    def _(n):
        span = pl.ds(pl.multiple_of(n * 64, 64), 64)
        inverse[span] = inverse_rms(x_ref[span].astype(jnp.float32))

    @pl.loop(0, stripes)
    def _(i):
        for k in range(per):
            load(i * per + k).wait()
            store(i * per + k).start()
        span = pl.ds(pl.multiple_of(i * 256, 256), 256)
        part = mm(grad_ref[...], weight_ref[span], (1, 1))
        part_ref[:, span] = part.astype(jnp.bfloat16)
        scaled = part * x_ref[:, span].astype(jnp.float32) * inverse[...]
        gain_ref[:, span] = jnp.sum(scaled, axis=0, keepdims=True)
        grad_weight_ref[span] = mm(normed_ref[:, span], grad_ref[...], (0, 0)).astype(jnp.bfloat16)
        for k in range(per):
            store(i * per + k).wait()

            @pl.when(i * per + k + slots < chunks)
            def _():
                load(i * per + k + slots).start()


def project_back(grad, weight, normed, x, experts):
    seq, width = x.shape
    bf, f4 = jnp.bfloat16, jnp.float32
    return pl.pallas_call(
        project_back_kernel,
        out_shape=[
            jax.ShapeDtypeStruct((seq, width), bf),
            jax.ShapeDtypeStruct(weight.shape, bf),
            jax.ShapeDtypeStruct((1, width), f4),
            jax.ShapeDtypeStruct(experts.shape, f4),
        ],
        in_specs=[pl.BlockSpec(memory_space=pltpu.VMEM)] * 4
        + [pl.BlockSpec(memory_space=pltpu.HBM)],
        out_specs=[pl.BlockSpec(memory_space=pltpu.VMEM)] * 3
        + [pl.BlockSpec(memory_space=pltpu.HBM)],
        scratch_shapes=[
            pltpu.VMEM((seq, 1), f4),
            pltpu.VMEM((6, 256, experts.shape[3]), f4),
            pltpu.SemaphoreType.DMA((6,)),
            pltpu.SemaphoreType.DMA((6,)),
        ],
        compiler_params=pltpu.CompilerParams(vmem_limit_bytes=48 << 20),
        name="project_back",
    )(grad, weight, normed, x, experts)


def split_body(
    block_in,
    segments,
    routes,
    attn_gain,
    query_key_value_weight,
    q_gain,
    k_gain,
    w_out,
    ffn_gain,
    router,
    expert_weights,
    cotangent,
):
    tok, width = block_in.shape
    seq = segments.shape[0]
    experts = router.shape[1]
    capacity = tok * routes.shape[1] * 2 // experts
    heads = QUERY_HEADS // 4
    both = ("rep", "shard")
    upstream_all = lax.all_gather(cotangent, both, axis=0, tiled=True)
    x_all, weight = start_exchange(block_in, query_key_value_weight, 0)

    mask = jnp.any(
        routes[:, :, None] == jnp.arange(experts, dtype=jnp.int32)[None, None, :], axis=1
    )
    mask_f = mask.astype(jnp.float32)
    earlier = (jnp.arange(tok)[:, None] > jnp.arange(tok)[None, :]).astype(jnp.bfloat16)
    slot = jnp.dot(earlier, mask.astype(jnp.bfloat16), preferred_element_type=jnp.float32)
    slot_table = jnp.where(mask, slot, -4096.0).T

    cosine, sine = rope_tables(jnp.arange(seq, dtype=jnp.int32))
    cosine = cosine[:, 0]
    sine = sine[:, 0] * jnp.where(jnp.arange(HEAD_SIZE) < HEAD_SIZE // 2, -1.0, 1.0)
    normed_one, raw, q_rot, k_rot, values, attended, lse, partial = attend(
        x_all, weight, w_out, attn_gain, q_gain, k_gain, cosine, sine, segments
    )
    inputs = block_in.astype(jnp.float32)
    middle = inputs + fold_sequence(partial, 1)
    scale_two = rms_scale(middle)
    normed_two = (middle * scale_two * ffn_gain).astype(jnp.bfloat16)
    logits = jnp.dot(normed_two, router, preferred_element_type=jnp.float32)
    weights = jax.nn.softmax(logits, axis=-1)
    picked = weights * mask_f
    total = jnp.sum(picked, axis=1, keepdims=True)
    gates = picked / total
    table = jnp.concatenate([gates.T, slot_table], axis=0)
    tokens_all, _, out_part, grad_part, gate_part, rows_held, hidden_held = run_experts(
        normed_two, table, upstream_all, expert_weights, capacity, 2
    )
    grad_gates = lax.all_to_all(gate_part, both, split_axis=0, concat_axis=0, tiled=True).T
    grad_from_experts, grad_experts = reduce_all(grad_part, 3, expert=[rows_held, hidden_held])
    grad_from_experts = grad_from_experts.astype(jnp.float32)

    upstream = cotangent.astype(jnp.float32)
    grad_picked = grad_gates / total - jnp.sum(grad_gates * picked, axis=1, keepdims=True) / (
        total * total
    )
    grad_weights = grad_picked * mask_f
    grad_logits = weights * (grad_weights - jnp.sum(grad_weights * weights, axis=1, keepdims=True))
    grad_from_router = jnp.dot(
        grad_logits, router.astype(jnp.float32).T, precision=lax.Precision.HIGHEST
    )
    grad_norm_two, grad_ffn_gain = rms_back(
        middle, scale_two, ffn_gain, grad_from_experts + grad_from_router
    )
    grad_middle = upstream + grad_norm_two
    grad_middle_all = spread_sequence(grad_middle.astype(jnp.bfloat16), 5)
    grad_out = lax.dot_general(
        attended, grad_middle_all, (((0,), (0,)), ((), ())), preferred_element_type=jnp.float32
    ).astype(jnp.bfloat16)
    grad_attended = jnp.dot(
        grad_middle_all, w_out.T, preferred_element_type=jnp.float32
    ).astype(jnp.bfloat16)
    expert_sum, grad_out, grad_qkv_b, grad_gains = reduce_all(
        out_part,
        4,
        grad_out,
        [
            q_rot,
            k_rot,
            values,
            raw,
            grad_attended,
            lse,
            q_gain[None],
            k_gain[None],
            cosine,
            sine,
            segments[:, None],
            segments[None],
        ],
    )
    block_out = (middle + expert_sum.astype(jnp.float32)).astype(jnp.bfloat16)
    grad_out = grad_out.astype(jnp.float32)
    grad_q_gain, grad_k_gain = grad_gains[0], grad_gains[1]
    norm_part, grad_weight, grad_attn_gain, grad_experts = project_back(
        grad_qkv_b, weight, normed_one, x_all, grad_experts
    )
    grad_attn_gain = grad_attn_gain[0]
    gains = jnp.concatenate([grad_attn_gain, grad_ffn_gain, grad_q_gain, grad_k_gain])
    lines = gains.shape[0] // tok
    spare = -(lines + experts) % 16
    small = jnp.concatenate(
        [grad_logits.T, gains.reshape(lines, tok), jnp.zeros((spare, tok), jnp.float32)], axis=0
    )
    small_all = lax.all_gather(small, both)
    grad_qkv, grad_norm_one = weight_reduce(grad_weight, norm_part, 7)
    grad_qkv = grad_qkv.astype(jnp.float32)
    grad_inputs, _ = rms_back(inputs, rms_scale(inputs), attn_gain, grad_norm_one)
    grad_input = (grad_middle + grad_inputs).astype(jnp.bfloat16)
    gains = jnp.sum(small_all[:, experts : experts + lines], axis=0).reshape(-1)
    grad_attn_gain, grad_ffn_gain, grad_q_gain, grad_k_gain = jnp.split(
        gains, (width, 2 * width, 2 * width + HEAD_SIZE)
    )
    logits_all = small_all[:, :experts].transpose(1, 0, 2).reshape(experts, -1)
    high = lax.reduce_precision(logits_all, 8, 7)
    middle_part = lax.reduce_precision(logits_all - high, 8, 7)
    low = logits_all - high - middle_part
    pieces = jnp.concatenate([high, middle_part, low], axis=0).astype(jnp.bfloat16)
    pieces = jnp.dot(pieces, tokens_all, preferred_element_type=jnp.float32)
    grad_router = jnp.sum(pieces.reshape(3, experts, width), axis=0).T
    return (
        block_out,
        grad_input,
        grad_attn_gain,
        grad_qkv,
        grad_q_gain,
        grad_k_gain,
        grad_out,
        grad_ffn_gain,
        grad_router,
        grad_experts,
    )


def solution(mesh):
    placed = (
        P(("rep", "shard"), None),
        P("rep"),
        P(("rep", "shard"), None),
        P(),
        P("shard", None),
        P(),
        P(),
        P("shard", None),
        P(),
        P(),
        P(("rep", "shard"), None, None, None),
        P(("rep", "shard"), None),
    )
    body = split_body if dict(mesh.shape) == {"rep": 8, "shard": 4} else plain_body
    return jax.shard_map(
        body,
        mesh=mesh,
        in_specs=placed,
        out_specs=(
            P(("rep", "shard"), None),
            P(("rep", "shard"), None),
            P(),
            P("shard", None),
            P(),
            P(),
            P("shard", None),
            P(),
            P(),
            P(("rep", "shard"), None, None, None),
        ),
        check_vma=False,
    )
```

```python
import functools

import jax
import jax.numpy as jnp
from jax import lax
from jax.experimental import pallas as pl
from jax.experimental.pallas import tpu as pltpu
from jax.sharding import PartitionSpec as P


QUERY_HEADS = 32
KEY_VALUE_HEADS = 4
HEAD_SIZE = 128


epsilon = 1e-06
rope_base = 1000000.0


def product(form, left, right):
    return jnp.einsum(form, left, right, preferred_element_type=jnp.float32)


def rms_scale(values):
    return lax.rsqrt(jnp.mean(values * values, axis=-1, keepdims=True) + epsilon)


def rms_back(values, scale, gain, upstream):
    scaled = upstream * gain
    cube = scale * scale * scale
    grad_values = scale * scaled - values * cube * jnp.mean(scaled * values, axis=-1, keepdims=True)
    grad_gain = jnp.sum((upstream * values * scale).reshape(-1, values.shape[-1]), axis=0)
    return (grad_values, grad_gain)


def rope_tables(positions):
    half = HEAD_SIZE // 2
    freq = rope_base ** (-jnp.arange(half).astype(jnp.float32) * 2.0 / HEAD_SIZE)
    angles = positions.astype(jnp.float32)[:, None] * freq[None, :]
    cosine = jnp.concatenate([jnp.cos(angles), jnp.cos(angles)], axis=-1)
    sine = jnp.concatenate([jnp.sin(angles), jnp.sin(angles)], axis=-1)
    return (cosine[:, None, :], sine[:, None, :])


def rotate(values):
    half = values.shape[-1] // 2
    return jnp.concatenate([-values[..., half:], values[..., :half]], axis=-1)


def rotate_back(values):
    half = values.shape[-1] // 2
    return jnp.concatenate([values[..., half:], -values[..., :half]], axis=-1)


def split_heads(query_key_value):
    token_rows = query_key_value.shape[0]
    q_raw = query_key_value[:, : QUERY_HEADS * HEAD_SIZE].reshape(
        token_rows, QUERY_HEADS, HEAD_SIZE
    )
    unrotated_key = query_key_value[
        :, QUERY_HEADS * HEAD_SIZE : (QUERY_HEADS + KEY_VALUE_HEADS) * HEAD_SIZE
    ].reshape(token_rows, KEY_VALUE_HEADS, HEAD_SIZE)
    projected_value = query_key_value[:, (QUERY_HEADS + KEY_VALUE_HEADS) * HEAD_SIZE :].reshape(
        token_rows, KEY_VALUE_HEADS, HEAD_SIZE
    )
    return (q_raw, unrotated_key, projected_value)


def norm_rope(raw, gain, cosine, sine):
    scale = rms_scale(raw)
    normed = raw * scale * gain
    return (scale, (normed * cosine + rotate(normed) * sine).astype(jnp.bfloat16))


def norm_rope_back(raw, scale, gain, cosine, sine, grad_rot):
    grad_normed = grad_rot * cosine + rotate_back(grad_rot * sine)
    return rms_back(raw, scale, gain, grad_normed)


def split_groups(values, groups):
    token_rows, heads, width = values.shape
    return values.reshape(token_rows, groups, heads // groups, width).transpose(1, 0, 2, 3)


def attend_forward(queries, keys, values, allowed):
    groups = keys.shape[1]
    token_rows = queries.shape[0]
    scale = queries.shape[2] ** (-0.5)

    def one_group(operands):
        q_part, k_part, v_part = operands
        scores = jnp.where(allowed[None], product("tpd,sd->pts", q_part, k_part) * scale, -1e30)
        highest = jnp.max(scores, axis=2, keepdims=True)
        lse = highest + jnp.log(jnp.sum(jnp.exp(scores - highest), axis=2, keepdims=True))
        probs = jnp.exp(scores - lse).astype(jnp.bfloat16)
        return (product("pts,sd->tpd", probs, v_part), lse[:, :, 0])

    outputs, lse = lax.map(
        one_group,
        (split_groups(queries, groups), keys.transpose(1, 0, 2), values.transpose(1, 0, 2)),
    )
    return (outputs.transpose(1, 0, 2, 3).reshape(token_rows, -1), lse)


def attend_backward(queries, keys, values, allowed, lse, attended, grad_attended):
    groups = keys.shape[1]
    token_rows, heads, width = queries.shape
    scale = width ** (-0.5)

    def one_group(operands):
        q_part, k_part, v_part, lse_part, out_part, grad_part = operands
        scores = jnp.where(allowed[None], product("tpd,sd->pts", q_part, k_part) * scale, -1e30)
        probs = jnp.exp(scores - lse_part[:, :, None])
        grad_v = product("pts,tpd->sd", probs.astype(jnp.bfloat16), grad_part)
        grad_p = product("tpd,sd->pts", grad_part, v_part)
        delta = jnp.sum(
            out_part.astype(jnp.float32) * grad_part.astype(jnp.float32), axis=2
        ).transpose(1, 0)
        grad_score = (probs * (grad_p - delta[:, :, None]) * scale).astype(jnp.bfloat16)
        return (
            product("pts,sd->tpd", grad_score, k_part),
            product("pts,tpd->sd", grad_score, q_part),
            grad_v,
        )

    shaped_out = split_groups(attended.reshape(token_rows, heads, width), groups)
    shaped_grad = split_groups(grad_attended.reshape(token_rows, heads, width), groups)
    grad_q, grad_k, grad_v = lax.map(
        one_group,
        (
            split_groups(queries, groups),
            keys.transpose(1, 0, 2),
            values.transpose(1, 0, 2),
            lse,
            shaped_out,
            shaped_grad,
        ),
    )
    return (
        grad_q.transpose(1, 0, 2, 3).reshape(token_rows, heads, width),
        grad_k.transpose(1, 0, 2),
        grad_v.transpose(1, 0, 2),
    )


def route_gates(normed, router, routes):
    logits = jnp.dot(normed, router, preferred_element_type=jnp.float32)
    weights = jax.nn.softmax(logits, axis=-1)
    chosen = (
        routes[:, :, None] == jnp.arange(router.shape[1], dtype=jnp.int32)[None, None, :]
    ).astype(jnp.float32)
    picked = jnp.sum(chosen * weights[:, None, :], axis=2)
    total = jnp.sum(picked, axis=1, keepdims=True)
    return (weights, chosen, picked, total, picked / total)


def route_gates_back(normed, router, weights, chosen, picked, total, grad_gates):
    grad_picked = grad_gates / total - jnp.sum(grad_gates * picked, axis=1, keepdims=True) / (
        total * total
    )
    grad_weights = jnp.sum(chosen * grad_picked[:, :, None], axis=1)
    grad_logits = weights * (grad_weights - jnp.sum(grad_weights * weights, axis=1, keepdims=True))
    grad_normed = jnp.dot(
        grad_logits, router.astype(jnp.float32).T, precision=lax.Precision.HIGHEST
    )
    grad_router = jnp.dot(
        normed.astype(jnp.float32).T, grad_logits, precision=lax.Precision.HIGHEST
    )
    return (grad_normed, grad_router)


def route_index(routes, experts, capacity):
    flat = routes.reshape(-1)
    onehot = (flat[:, None] == jnp.arange(experts, dtype=jnp.int32)[None, :]).astype(jnp.int32)
    before = jnp.cumsum(onehot, axis=0) - onehot
    return flat * capacity + jnp.sum(before * onehot, axis=1)


def dispatch(rows_per_route, index, experts, capacity):
    width = rows_per_route.shape[1]
    empty = jnp.zeros((experts * capacity, width), rows_per_route.dtype)
    return empty.at[index].set(rows_per_route).reshape(experts, capacity, width)


def collect(buffer, index):
    return buffer.reshape(-1, buffer.shape[-1])[index]


def expert_forward(inputs, weights):
    gate_pre = product("ecd,edf->ecf", inputs, weights[:, 0])
    up_pre = product("ecd,edf->ecf", inputs, weights[:, 1])
    hidden = (jax.nn.silu(gate_pre) * up_pre).astype(jnp.bfloat16)
    result = product("ecf,edf->ecd", hidden, weights[:, 2]).astype(jnp.bfloat16)
    return (gate_pre, up_pre, hidden, result)


def expert_backward(weights, gate_pre, up_pre, grad_result):
    grad_hidden = product("ecd,edf->ecf", grad_result, weights[:, 2])
    sig = jax.nn.sigmoid(gate_pre)
    grad_gate = (grad_hidden * up_pre * sig * (1.0 + gate_pre * (1.0 - sig))).astype(jnp.bfloat16)
    grad_up = (grad_hidden * gate_pre * sig).astype(jnp.bfloat16)
    grad_inputs = product("ecf,edf->ecd", grad_gate, weights[:, 0]) + product(
        "ecf,edf->ecd", grad_up, weights[:, 1]
    )
    return (grad_gate, grad_up, grad_inputs.astype(jnp.bfloat16))


def expert_weight_grads(inputs, hidden, grad_gate, grad_up, grad_result):
    return jnp.stack(
        [
            product("ecd,ecf->edf", inputs, grad_gate),
            product("ecd,ecf->edf", inputs, grad_up),
            product("ecd,ecf->edf", grad_result, hidden),
        ],
        axis=1,
    )


def plain_body(
    block_in,
    segments,
    routes,
    attn_gain,
    query_key_value_weight,
    q_gain,
    k_gain,
    w_out,
    ffn_gain,
    router,
    expert_weights,
    cotangent,
):
    tok = block_in.shape[0]
    width = block_in.shape[1]
    top = routes.shape[1]
    rep_count = lax.axis_size("rep")
    shard_count = lax.axis_size("shard")
    experts = expert_weights.shape[0] * rep_count * shard_count
    capacity = tok * top * 2 // experts
    shard_pos = lax.axis_index("shard")
    qkv_whole, out_whole = (
        lax.all_gather(query_key_value_weight, "shard", axis=0, tiled=True),
        lax.all_gather(w_out, "shard", axis=0, tiled=True),
    )
    inputs = block_in.astype(jnp.float32)
    scale_one = rms_scale(inputs)
    normed_one = (inputs * scale_one * attn_gain).astype(jnp.bfloat16)
    query_key_value = jnp.dot(normed_one, qkv_whole, preferred_element_type=jnp.float32)
    q_raw, unrotated_key, projected_value = split_heads(query_key_value)
    positions = shard_pos * tok + jnp.arange(tok, dtype=jnp.int32)
    cosine, sine = rope_tables(positions)
    q_scale, q_rot = norm_rope(q_raw, q_gain, cosine, sine)
    k_scale, k_rot = norm_rope(unrotated_key, k_gain, cosine, sine)
    keys_all, values_all = (
        lax.all_gather(k_rot, "shard", axis=0, tiled=True),
        lax.all_gather(projected_value.astype(jnp.bfloat16), "shard", axis=0, tiled=True),
    )
    query_seg = lax.dynamic_slice_in_dim(segments, shard_pos * tok, tok)
    key_pos = jnp.arange(segments.shape[0], dtype=jnp.int32)
    allowed = (query_seg[:, None] == segments[None, :]) & (key_pos[None, :] <= positions[:, None])
    attended_f, lse = attend_forward(q_rot, keys_all, values_all, allowed)
    attended = attended_f.astype(jnp.bfloat16)
    middle = inputs + jnp.dot(attended, out_whole, preferred_element_type=jnp.float32)
    scale_two = rms_scale(middle)
    normed_two = (middle * scale_two * ffn_gain).astype(jnp.bfloat16)
    weights, chosen, picked, total, gates = route_gates(normed_two, router, routes)
    index = route_index(routes, experts, capacity)
    upstream = cotangent.astype(jnp.float32)
    grad_rows = (
        (gates[:, :, None] * upstream[:, None, :]).astype(jnp.bfloat16).reshape(tok * top, width)
    )
    paired = jnp.concatenate([jnp.repeat(normed_two, top, axis=0), grad_rows], axis=1)
    buffer = dispatch(paired, index, experts, capacity)
    received = lax.all_to_all(buffer, ("rep", "shard"), split_axis=0, concat_axis=1, tiled=True)
    token_rows = received[:, :, :width]
    grads = received[:, :, width:]
    gate_pre, up_pre, hidden, result = expert_forward(token_rows, expert_weights)
    grad_gate, grad_up, grad_inner = expert_backward(expert_weights, gate_pre, up_pre, grads)
    grad_experts = expert_weight_grads(token_rows, hidden, grad_gate, grad_up, grads)
    outgoing = jnp.concatenate([result, grad_inner], axis=2)
    returned = lax.all_to_all(outgoing, ("rep", "shard"), split_axis=1, concat_axis=0, tiled=True)
    fetched = collect(returned, index).reshape(tok, top, 2 * width)
    expert_rows = fetched[:, :, :width].astype(jnp.float32)
    grad_from_experts = jnp.sum(fetched[:, :, width:].astype(jnp.float32), axis=1)
    block_out = (middle + jnp.sum(gates[:, :, None] * expert_rows, axis=1)).astype(jnp.bfloat16)
    grad_gates = jnp.sum(expert_rows * upstream[:, None, :], axis=2)
    grad_from_router, grad_router = route_gates_back(
        normed_two, router, weights, chosen, picked, total, grad_gates
    )
    grad_norm_two, grad_ffn_gain = rms_back(
        middle, scale_two, ffn_gain, grad_from_experts + grad_from_router
    )
    grad_middle = upstream + grad_norm_two
    grad_middle_b = grad_middle.astype(jnp.bfloat16)
    columns = attended
    grad_out = lax.psum_scatter(
        lax.dot_general(
            columns, grad_middle_b, (((0,), (0,)), ((), ())), preferred_element_type=jnp.float32
        ).astype(jnp.bfloat16),
        "shard",
        scatter_dimension=0,
        tiled=True,
    ).astype(jnp.float32)
    grad_attended = jnp.dot(grad_middle_b, out_whole.T, preferred_element_type=jnp.float32).astype(
        jnp.bfloat16
    )
    grad_q_rot, grad_k_all, grad_v_all = attend_backward(
        q_rot, keys_all, values_all, allowed, lse, attended, grad_attended
    )
    grad_k_rot, grad_v = (
        lax.psum_scatter(
            grad_k_all.astype(jnp.bfloat16), "shard", scatter_dimension=0, tiled=True
        ).astype(jnp.float32),
        lax.psum_scatter(
            grad_v_all.astype(jnp.bfloat16), "shard", scatter_dimension=0, tiled=True
        ).astype(jnp.float32),
    )
    grad_q_raw, grad_q_gain = norm_rope_back(q_raw, q_scale, q_gain, cosine, sine, grad_q_rot)
    grad_k_raw, grad_k_gain = norm_rope_back(
        unrotated_key, k_scale, k_gain, cosine, sine, grad_k_rot
    )
    grad_qkv_b = jnp.concatenate(
        [grad_q_raw.reshape(tok, -1), grad_k_raw.reshape(tok, -1), grad_v.reshape(tok, -1)], axis=1
    ).astype(jnp.bfloat16)
    columns = normed_one
    grad_qkv = lax.psum_scatter(
        lax.dot_general(
            columns, grad_qkv_b, (((0,), (0,)), ((), ())), preferred_element_type=jnp.float32
        ).astype(jnp.bfloat16),
        "shard",
        scatter_dimension=0,
        tiled=True,
    ).astype(jnp.float32)
    grad_norm_one = jnp.dot(grad_qkv_b, qkv_whole.T, preferred_element_type=jnp.float32)
    grad_inputs, grad_attn_gain = rms_back(inputs, scale_one, attn_gain, grad_norm_one)
    grad_input = (grad_middle + grad_inputs).astype(jnp.bfloat16)
    grad_attn_gain, grad_q_gain, grad_k_gain, grad_ffn_gain, grad_router = lax.psum(
        (grad_attn_gain, grad_q_gain, grad_k_gain, grad_ffn_gain, grad_router), ("rep", "shard")
    )
    grad_qkv, grad_out = (
        lax.psum(grad_qkv.astype(jnp.bfloat16), "rep").astype(jnp.float32),
        lax.psum(grad_out.astype(jnp.bfloat16), "rep").astype(jnp.float32),
    )
    return (
        block_out,
        grad_input,
        grad_attn_gain,
        grad_qkv,
        grad_q_gain,
        grad_k_gain,
        grad_out,
        grad_ffn_gain,
        grad_router,
        grad_experts,
    )


MESH_ID = pl.DeviceIdType.MESH
PLANES = 4


def place():
    rep, shard = lax.axis_index("rep"), lax.axis_index("shard")
    return rep // 2, rep % 2, shard // 2, shard % 2


def device(z, core, y, x):
    return (z * 2 + core, y * 2 + x)


def block_of(z, core, y, x):
    return (z * 2 + core) * 4 + y * 2 + x


def greet(targets):
    barrier = pltpu.get_barrier_semaphore()
    for condition, target in targets:
        if condition is None:
            pl.semaphore_signal(barrier, inc=1, device_id=target, device_id_type=MESH_ID)
        else:

            @pl.when(condition)
            def _():
                pl.semaphore_signal(barrier, inc=1, device_id=target, device_id_type=MESH_ID)

    peers = 0
    for condition, _ in targets:
        peers = peers + (1 if condition is None else condition.astype(jnp.int32))
    pl.semaphore_wait(barrier, peers)


def experts_kernel(
    x_ref,
    table_ref,
    upstream_ref,
    w_ref,
    x_all,
    table_all,
    out_ref,
    grad_ref,
    gg_ref,
    rows_out,
    hidden_out,
    gs,
    rows_hold,
    hidden_hold,
    x_hold,
    g_hold,
    t_hold,
    out_hold,
    grad_hold,
    send_sem,
    recv_sem,
    own_sem,
    load_sem,
    store_sem,
):
    ins, outs = (x_ref, table_ref), (x_all, table_all)
    rows = (x_ref.shape[0], table_ref.shape[0])
    count = len(ins)
    tok = rows[0]
    experts = rows[1] // 2
    z, core, y, x = place()
    partner = device(z, 1 - core, y, x)
    x_next, y_next = device(z, core, y, 1 - x), device(z, core, 1 - y, x)
    up, down = device(z + 1, core, y, x), device(z - 1, core, y, x)
    can_up, can_down = z < PLANES - 1, z > 0
    greet(
        [
            (None, partner),
            (None, x_next),
            (None, y_next),
            (can_up, up),
            (can_down, down),
        ]
    )
    tables = ((0, 1, 2, 3), (1, 0, 2, 3), (2, 3, 1, 0), (3, 2, 1, 0))
    order = [
        sum((z == level).astype(jnp.int32) * tables[level][n] for level in range(PLANES))
        for n in range(PLANES)
    ]
    pending, used = [], [0]

    def region(array, block, part):
        size = rows[array]
        if part is None:
            return pl.ds(pl.multiple_of(block * size, size), size)
        return pl.ds(pl.multiple_of(block * size + part * (size // 2), size // 2), size // 2)

    def copy_of(array, block, part, target, index, own=False):
        where = region(array, block, part)
        source = ins[array] if own else outs[array].at[where]
        return remote(
            source,
            outs[array].at[where],
            send_sem.at[array, index],
            recv_sem.at[array, block * 2 + (part or 0)],
            target,
        )

    def plan(block, part, target, condition=None, own=False):
        index = used[0]
        used[0] += 1

        def start():
            for array in range(count):
                copy_of(array, block, part, target, index, own).start()

        def finish():
            for array in range(count):
                copy_of(array, block, part, target, index, own).wait_send()

        pending.append((condition, finish))
        return lambda: start() if condition is None else pl.when(condition)(start)

    def arrived(block, part):
        for array in range(count):
            copy_of(array, block, part, partner, 0).wait_recv()

    own = block_of(z, core, y, x)
    for target, condition in (
        (up, can_up),
        (down, can_down),
        (x_next, None),
        (y_next, None),
        (partner, None),
    ):
        plan(own, None, target, condition, own=True)()
    locals_ = [
        pltpu.make_async_copy(ins[n], outs[n].at[region(n, own, None)], own_sem.at[n])
        for n in range(count)
    ]
    for copy in locals_:
        copy.start()

    def along(n):
        plane = order[n]
        block = block_of(plane, core, y, x)
        moves = [
            plan(block, None, up, jnp.logical_and(plane < z, can_up)),
            plan(block, None, down, jnp.logical_and(plane > z, can_down)),
            plan(block, None, x_next),
            plan(block, None, y_next),
            plan(block, None, partner),
        ]

        def run():
            arrived(block, None)
            for move in moves:
                move()

        return run

    def across(n):
        plane = order[n]
        from_x, from_y = block_of(plane, core, y, 1 - x), block_of(plane, core, 1 - y, x)
        moves = [
            plan(from_x, 1, y_next),
            plan(from_x, None, partner),
            plan(from_y, 0, x_next),
            plan(from_y, None, partner),
        ]

        def run():
            arrived(from_x, None)
            moves[0]()
            moves[1]()
            arrived(from_y, None)
            moves[2]()
            moves[3]()

        return run

    def diagonal(n):
        block = block_of(order[n], core, 1 - y, 1 - x)
        moves = [plan(block, part, partner) for part in range(2)]

        def run():
            for part in range(2):
                arrived(block, part)
                moves[part]()

        return run

    def paired(n):
        plane = order[n]

        def run():
            for where_y, where_x in ((y, x), (y, 1 - x), (1 - y, x)):
                arrived(block_of(plane, 1 - core, where_y, where_x), None)
            for part in range(2):
                arrived(block_of(plane, 1 - core, 1 - y, 1 - x), part)

        return run

    def settled():
        for copy in locals_:
            copy.wait()

    inside = jnp.logical_and(can_up, can_down)
    steps_along = [along(n) for n in range(1, PLANES)]

    def hop(n, condition):
        return lambda: pl.when(condition)(steps_along[n - 1])

    outside = jnp.logical_not(inside)
    work = (
        (across(0), steps_along[0], hop(2, inside), diagonal(0), settled),
        (across(1), hop(2, outside), hop(3, inside), paired(0)),
        (hop(3, outside), diagonal(1)),
        (across(2), paired(1)),
        (across(3), diagonal(2)),
        (diagonal(3), paired(2)),
        (),
        (paired(3),),
    )
    group = 4 * tok
    steps = len(work)
    cap = gs.shape[0] // 4
    me = block_of(z, core, y, x)

    def group_of(i):
        if isinstance(i, int):
            plane = order[i // 2]
        else:
            plane = sum((i // 2 == n).astype(jnp.int32) * order[n] for n in range(PLANES))
        return plane * 2 + (core + i % 2) % 2

    def group_rows(ref, i):
        return ref.at[pl.ds(pl.multiple_of(group_of(i) * group, group), group)]

    def load_g(i):
        return pltpu.make_async_copy(
            group_rows(upstream_ref, i), g_hold.at[i % 2], load_sem.at[i % 2]
        )

    def load_x(i):
        return pltpu.make_async_copy(group_rows(x_all, i), x_hold, load_sem.at[2])

    def load_t(i):
        size = 4 * rows[1]
        return pltpu.make_async_copy(
            table_all.at[pl.ds(pl.multiple_of(group_of(i) * size, size), size)],
            t_hold,
            load_sem.at[3],
        )

    def store(i):
        held = pl.ds(pl.multiple_of(i * 4 * cap, 4 * cap), 4 * cap)
        return [
            pltpu.make_async_copy(hold.at[i % 2], target, store_sem.at[n, i % 2])
            for n, (hold, target) in enumerate(
                (
                    (out_hold, group_rows(out_ref, i)),
                    (grad_hold, group_rows(grad_ref, i)),
                    (rows_hold, rows_out.at[:, held]),
                    (hidden_hold, hidden_out.at[:, held]),
                )
            )
        ]

    def dot(left, right, dims):
        return lax.dot_general(
            left, right, ((dims[:1], dims[1:]), ((), ())), preferred_element_type=jnp.float32
        )

    load_g(0).start()

    @pl.loop(0, steps)
    def _(i):
        for n in range(steps):
            if work[n]:

                @pl.when(i == n)
                def _():
                    for run in work[n]:
                        run()

        load_x(i).start()
        load_t(i).start()

        @pl.when(i + 1 < steps)
        def _():
            load_g(i + 1).start()

        @pl.when(i >= 2)
        def _():
            for copy in store(i - 2):
                copy.wait()

        load_t(i).wait()
        load_x(i).wait()
        load_g(i).wait()
        slot = i % 2
        chosen, gate_cols = [], []
        for pair in range(2):
            first = [(pair * 2 + j) * 2 * experts + me for j in range(2)]
            gate_row = jnp.concatenate([t_hold[pl.ds(at, 1), :] for at in first], axis=1)
            slot_row = jnp.concatenate(
                [
                    t_hold[pl.ds(at + experts, 1), :] + float(cap * j)
                    for j, at in enumerate(first)
                ],
                axis=1,
            )
            ids = lax.broadcasted_iota(jnp.int32, (2 * cap, 2 * tok), 0).astype(jnp.float32)
            mask = jnp.where(ids == slot_row, 1.0, 0.0)
            pick = mask.astype(jnp.bfloat16)
            held = pl.ds(pair * 2 * cap, 2 * cap)
            tokens = pl.ds(pair * 2 * tok, 2 * tok)
            gate = jnp.sum(mask * gate_row, axis=1, keepdims=True)
            rows_hold[slot, 0, held] = dot(pick, x_hold[tokens], (1, 0)).astype(jnp.bfloat16)
            upstream = dot(pick, g_hold[slot, tokens], (1, 0))
            gs[held] = upstream.astype(jnp.bfloat16)
            rows_hold[slot, 1, held] = (upstream * gate).astype(jnp.bfloat16)
            chosen.append(pick)
            gate_cols.append(gate)
        rows_x = rows_hold[slot, 0]
        rows_g = rows_hold[slot, 1]
        gate_pre = dot(rows_x, w_ref[0], (1, 0))
        up_pre = dot(rows_x, w_ref[1], (1, 0))
        sig = jax.nn.sigmoid(gate_pre)
        silu = gate_pre * sig
        hidden = (silu * up_pre).astype(jnp.bfloat16)
        grad_hidden = dot(rows_g, w_ref[2], (1, 0))
        grad_gate = (grad_hidden * up_pre * sig * (1.0 + gate_pre * (1.0 - sig))).astype(
            jnp.bfloat16
        )
        grad_up = (grad_hidden * silu).astype(jnp.bfloat16)
        result = dot(hidden, w_ref[2], (1, 1)).astype(jnp.bfloat16)
        grad_in = (dot(grad_gate, w_ref[0], (1, 1)) + dot(grad_up, w_ref[1], (1, 1))).astype(
            jnp.bfloat16
        )
        hidden_hold[slot, 0] = grad_gate
        hidden_hold[slot, 1] = grad_up
        hidden_hold[slot, 2] = hidden
        result_f = result.astype(jnp.float32)
        share = jnp.sum(gs[...].astype(jnp.float32) * result_f, axis=1, keepdims=True)
        for pair in range(2):
            tokens = pl.ds(pair * 2 * tok, 2 * tok)
            low, high = pair * 2 * cap, (pair + 1) * 2 * cap
            pick = chosen[pair]
            scaled = (result_f[low:high] * gate_cols[pair]).astype(jnp.bfloat16)
            out_hold[slot, tokens] = dot(pick, scaled, (0, 0)).astype(jnp.bfloat16)
            grad_hold[slot, tokens] = dot(pick, grad_in[low:high], (0, 0)).astype(jnp.bfloat16)
            row = jnp.sum(pick.astype(jnp.float32) * share[low:high], axis=0, keepdims=True)
            for j in range(2):
                gg_ref[pl.ds(group_of(i) * 4 + pair * 2 + j, 1), :] = row[
                    :, j * tok : (j + 1) * tok
                ]
        for copy in store(i):
            copy.start()

    for i in (steps - 2, steps - 1):
        for copy in store(i):
            copy.wait()
    for condition, finish in pending:
        if condition is None:
            finish()
        else:
            pl.when(condition)(finish)


def run_experts(tokens, table, upstream, weights, cap, collective_id):
    tok, width = tokens.shape
    _, three, _, ff = weights.shape
    devices = 32
    total = tok * devices
    held = 4 * cap
    group = 4 * tok
    return pl.pallas_call(
        experts_kernel,
        out_shape=[
            jax.ShapeDtypeStruct((total, width), tokens.dtype),
            jax.ShapeDtypeStruct((table.shape[0] * devices, tok), table.dtype),
            jax.ShapeDtypeStruct((total, width), jnp.bfloat16),
            jax.ShapeDtypeStruct((total, width), jnp.bfloat16),
            jax.ShapeDtypeStruct((devices, tok), jnp.float32),
            jax.ShapeDtypeStruct((2, 8 * held, width), jnp.bfloat16),
            jax.ShapeDtypeStruct((3, 8 * held, ff), jnp.bfloat16),
        ],
        in_specs=[
            pl.BlockSpec(memory_space=pltpu.VMEM),
            pl.BlockSpec(memory_space=pltpu.VMEM),
            pl.BlockSpec(memory_space=pltpu.HBM),
            pl.BlockSpec(memory_space=pltpu.VMEM),
        ],
        out_specs=[pl.BlockSpec(memory_space=pltpu.HBM)] * 4
        + [pl.BlockSpec(memory_space=pltpu.VMEM)]
        + [pl.BlockSpec(memory_space=pltpu.HBM)] * 2,
        scratch_shapes=[
            pltpu.VMEM((held, width), jnp.bfloat16),
            pltpu.VMEM((2, 2, held, width), jnp.bfloat16),
            pltpu.VMEM((2, 3, held, ff), jnp.bfloat16),
            pltpu.VMEM((group, width), jnp.bfloat16),
            pltpu.VMEM((2, group, width), jnp.bfloat16),
            pltpu.VMEM((4 * table.shape[0], tok), jnp.float32),
            pltpu.VMEM((2, group, width), jnp.bfloat16),
            pltpu.VMEM((2, group, width), jnp.bfloat16),
            pltpu.SemaphoreType.DMA((2, 44)),
            pltpu.SemaphoreType.DMA((2, 64)),
            pltpu.SemaphoreType.DMA((2,)),
            pltpu.SemaphoreType.DMA((4,)),
            pltpu.SemaphoreType.DMA((4, 2)),
        ],
        compiler_params=pltpu.CompilerParams(
            collective_id=collective_id, has_side_effects=True, vmem_limit_bytes=63 << 20
        ),
        name="run_experts",
    )(tokens, table, upstream, weights.reshape(three, width, ff))


def add_rows(target, sources, rows=128, step=16):
    @pl.loop(0, rows // step)
    def _(i):
        where = pl.ds(pl.multiple_of(i * step, step), step)
        total = target[where].astype(jnp.float32)
        for source in sources:
            total += source[where].astype(jnp.float32)
        target[where] = total.astype(target.dtype)


def rolled(values):
    return pltpu.roll(values, HEAD_SIZE // 2, 1)


def inverse_rms(values):
    return lax.rsqrt(jnp.mean(values * values, axis=1, keepdims=True) + epsilon)


def mm(left, right, dims):
    return lax.dot_general(
        left, right, ((dims[:1], dims[1:]), ((), ())), preferred_element_type=jnp.float32
    )


def fill_bias(bias, seg_col, seg_row):
    seq = bias.shape[0]
    key = lax.broadcasted_iota(jnp.int32, (seq, seq), 0)
    query = lax.broadcasted_iota(jnp.int32, (seq, seq), 1)
    same = seg_col[...] == seg_row[...]
    bias[...] = jnp.where(jnp.logical_and(same, key <= query), 0.0, -1e30)


def attend_kernel(
    x_ref,
    weight_ref,
    w_out_ref,
    gain_ref,
    q_gain_ref,
    k_gain_ref,
    cos_ref,
    sin_ref,
    seg_col,
    seg_row,
    normed_ref,
    raw_ref,
    q_ref,
    k_ref,
    v_ref,
    attended_ref,
    lse_ref,
    part_ref,
    bias,
):
    seq = x_ref.shape[0]
    size = HEAD_SIZE
    heads = q_ref.shape[1] // size
    scale = size ** (-0.5)

    @pl.loop(0, seq // 64)
    def _(n):
        rows = pl.ds(pl.multiple_of(n * 64, 64), 64)
        x = x_ref[rows].astype(jnp.float32)
        normed_ref[rows] = (x * inverse_rms(x) * gain_ref[...]).astype(jnp.bfloat16)

    fill_bias(bias, seg_col, seg_row)

    @pl.loop(0, raw_ref.shape[1] // 256)
    def _(n):
        columns = pl.ds(pl.multiple_of(n * 256, 256), 256)
        raw_ref[:, columns] = mm(normed_ref[...], weight_ref[:, columns], (1, 0))

    def turned(raw, gain_row):
        normed = raw * inverse_rms(raw) * gain_row
        return (normed * cos_ref[...] + rolled(normed) * sin_ref[...]).astype(jnp.bfloat16)

    k_ref[...] = turned(raw_ref[:, heads * size : (heads + 1) * size], k_gain_ref[...])
    v_ref[...] = raw_ref[:, (heads + 1) * size :].astype(jnp.bfloat16)
    half = seq // 2

    @pl.loop(0, heads)
    def _(h):
        columns = pl.ds(pl.multiple_of(h * size, size), size)
        q_ref[:, columns] = turned(raw_ref[:, columns], q_gain_ref[...])
        for first, keys in ((0, half), (half, seq)):
            queries = pl.ds(first, half)
            score = mm(k_ref[:keys], q_ref[queries, columns], (1, 1)) * scale
            score = score + bias[:keys, first : first + half]
            highest = jnp.max(score, axis=0, keepdims=True)
            power = jnp.exp(score - highest)
            total = jnp.sum(power, axis=0, keepdims=True)
            lse_ref[pl.ds(h, 1), queries] = highest + jnp.log(total)
            probs = (power * (1.0 / total)).astype(jnp.bfloat16)
            attended_ref[queries, columns] = mm(probs, v_ref[:keys], (0, 0)).astype(jnp.bfloat16)

    @pl.loop(0, part_ref.shape[1] // 512)
    def _(n):
        columns = pl.ds(pl.multiple_of(n * 512, 512), 512)
        part_ref[:, columns] = mm(attended_ref[...], w_out_ref[:, columns], (1, 0)).astype(
            jnp.bfloat16
        )


def attend(x, weight, w_out, gain, q_gain, k_gain, cosine, sine, segments):
    seq, width = x.shape
    columns = weight.shape[1]
    heads = w_out.shape[0] // HEAD_SIZE
    bf, f4 = jnp.bfloat16, jnp.float32
    out = jax.ShapeDtypeStruct
    return pl.pallas_call(
        attend_kernel,
        out_shape=[
            out((seq, width), bf),
            out((seq, columns), f4),
            out((seq, heads * HEAD_SIZE), bf),
            out((seq, HEAD_SIZE), bf),
            out((seq, HEAD_SIZE), bf),
            out((seq, heads * HEAD_SIZE), bf),
            out((heads, seq), f4),
            out((seq, width), bf),
        ],
        in_specs=[pl.BlockSpec(memory_space=pltpu.VMEM)] * 10,
        out_specs=[pl.BlockSpec(memory_space=pltpu.VMEM)] * 8,
        scratch_shapes=[pltpu.VMEM((seq, seq), f4)],
        compiler_params=pltpu.CompilerParams(vmem_limit_bytes=56 << 20),
        name="attend",
    )(
        x,
        weight,
        w_out,
        gain[None],
        q_gain[None],
        k_gain[None],
        cosine,
        sine,
        segments[:, None],
        segments[None],
    )


def backward_steps(refs):
    q_ref, k_ref, v_ref, raw_ref, upstream, lse_ref = refs[:6]
    q_gain_ref, k_gain_ref, cos_ref, sin_ref, seg_col, seg_row = refs[6:12]
    grad_ref, gains_ref, bias, grad_k, grad_v = refs[12:]
    seq, size = k_ref.shape
    heads = q_ref.shape[1] // size
    scale = size ** (-0.5)
    half = seq // 2

    def prepare():
        fill_bias(bias, seg_col, seg_row)
        grad_k[...] = jnp.zeros_like(grad_k)
        grad_v[...] = jnp.zeros_like(grad_v)
        gains_ref[...] = jnp.zeros_like(gains_ref)

    def turn_back(grad, queries, columns, gain, line):
        turned = grad * cos_ref[queries] + rolled(grad * sin_ref[queries])
        raw = raw_ref[queries, columns]
        inverse = inverse_rms(raw)
        scaled = turned * gain
        mean = jnp.mean(scaled * raw, axis=1, keepdims=True)
        grad_raw = inverse * scaled - raw * (inverse * inverse * inverse) * mean
        grad_ref[queries, columns] = grad_raw.astype(jnp.bfloat16)
        gains_ref[line : line + 1] += jnp.sum(turned * raw * inverse, axis=0, keepdims=True)

    def head(h):
        columns = pl.ds(pl.multiple_of(h * size, size), size)
        for first, keys in ((0, half), (half, seq)):
            queries = pl.ds(first, half)
            q, above = q_ref[queries, columns], upstream[queries, columns]
            score = mm(k_ref[:keys], q, (1, 1)) * scale + bias[:keys, first : first + half]
            probs = jnp.exp(score - lse_ref[pl.ds(h, 1), queries])
            grad_v[:keys] += mm(probs.astype(jnp.bfloat16), above, (1, 0))
            grad_p = mm(v_ref[:keys], above, (1, 1))
            delta = jnp.sum(probs * grad_p, axis=0, keepdims=True)
            grad_score = (probs * (grad_p - delta) * scale).astype(jnp.bfloat16)
            grad_k[:keys] += mm(grad_score, q, (1, 0))
            grad_q = mm(grad_score, k_ref[:keys], (0, 0))
            turn_back(grad_q, queries, columns, q_gain_ref[...], 0)

    def keys_and_values():
        for first in (0, half):
            queries = pl.ds(first, half)
            turn_back(grad_k[queries], queries, pl.ds(heads * size, size), k_gain_ref[...], 1)
        grad_ref[:, (heads + 1) * size :] = grad_v[...].astype(jnp.bfloat16)

    return prepare, head, keys_and_values


class Sends:
    def __init__(self, send_sem, partner):
        self.send_sem, self.partner, self.used, self.pending = send_sem, partner, 0, []

    def make(self, source, landing, sem, target, *conditions):
        copy = remote(source, landing, self.send_sem.at[self.used], sem, target)
        self.used += 1
        self.pending.append((conditions, copy))
        return copy

    def send(self, source, landing, sem, target):
        self.make(source, landing, sem, target).start()

    def arrived(self, landing, sem):
        remote(landing, landing, self.send_sem.at[0], sem, self.partner).wait_recv()

    def finish(self):
        for conditions, copy in self.pending:
            if not conditions:
                copy.wait_send()
            elif len(conditions) == 1:
                pl.when(conditions[0])(copy.wait_send)
            else:
                pl.when(jnp.logical_and(*conditions))(copy.wait_send)


def add_into(target, sources, rows):
    @pl.loop(0, rows // 16)
    def _(n):
        where = pl.ds(pl.multiple_of(n * 16, 16), 16)
        total = sources[0][where].astype(jnp.float32)
        for source in sources[1:]:
            total += source[where].astype(jnp.float32)
        target[where] = total.astype(target.dtype)


def ladder(sends, count, before, piece, from_up, from_down, final, size, sems):
    climb_send, spread_send, close_send, climb_sem, spread_sem, close_sem = sems
    z, core, y, x = place()
    partner = sends.partner
    up, down = device(z + 1, core, y, x), device(z - 1, core, y, x)
    can_up, can_down = z < PLANES - 1, z > 0

    def climb(n, rising):
        landing = from_down(n) if rising else from_up(n)
        side = 1 if rising else 0
        return remote(
            piece(n), landing, climb_send.at[n], climb_sem.at[n, side], up if rising else down
        )

    def gained(n, rising):
        landing = from_down(n) if rising else from_up(n)
        sends.arrived(landing, climb_sem.at[n, 1 if rising else 0])
        return landing

    def spread(n, rising):
        block = final(n, core)
        target = up if rising else down
        return remote(block, block, spread_send.at[n, 1 if rising else 0], spread_sem.at[n], target)

    def hand_over(n):
        block = final(n, core)
        return remote(block, block, close_send.at[n], close_sem.at[n], partner)

    def ends(n, root):
        before(n)
        pl.when(z == 0)(climb(n, True).start)
        pl.when(z == PLANES - 1)(climb(n, False).start)

    def between(n, root):
        for rising, level in ((True, 1), (False, 2)):

            @pl.when(jnp.logical_and(z == level, root == 3 - level))
            def _():
                add_rows(piece(n), (gained(n, rising),), size)
                climb(n, rising).start()

    def settle(n, root):
        @pl.when(z == root)
        def _():
            add_into(final(n, core), (piece(n), gained(n, True), gained(n, False)), size)
            spread(n, True).start()
            spread(n, False).start()
            hand_over(n).start()

    def receive(n, root, distance):
        for rising, there, more in (
            (True, z == root + distance, can_up),
            (False, z == root - distance, can_down),
        ):

            @pl.when(there)
            def _():
                sends.arrived(final(n, core), spread_sem.at[n])
                pl.when(more)(spread(n, rising).start)
                hand_over(n).start()

    stages = (
        ends,
        between,
        settle,
        functools.partial(receive, distance=1),
        functools.partial(receive, distance=2),
    )

    def step(m):
        for stage, run in enumerate(stages):
            n = m - stage * SLACK

            @pl.when(jnp.logical_and(n >= 0, n < count))
            def _():
                run(n, 1 + n % 2)

    def close():
        @pl.loop(0, count)
        def _(n):
            root = 1 + n % 2
            pl.when(z != root)(climb(n, True).wait_send)
            pl.when(jnp.logical_and(z >= root, can_up))(spread(n, True).wait_send)
            pl.when(jnp.logical_and(z <= root, can_down))(spread(n, False).wait_send)
            hand_over(n).wait_send()

    def closed(n):
        sends.arrived(final(n, 1 - core), close_sem.at[n])

    return step, closed, close


SLACK = 2
LADDER_MORE = 4 * SLACK


def ladder_scratch(count):
    return [
        pltpu.SemaphoreType.DMA((count,)),
        pltpu.SemaphoreType.DMA((count, 2)),
        pltpu.SemaphoreType.DMA((count,)),
        pltpu.SemaphoreType.DMA((count, 2)),
        pltpu.SemaphoreType.DMA((count,)),
        pltpu.SemaphoreType.DMA((count,)),
    ]


LADDER = 32
PER = LADDER // 4


def reduce_kernel(with_weight, *refs):
    refs = list(refs)
    part_ref = refs.pop(0)
    weight_ref = refs.pop(0) if with_weight else None
    back = [refs.pop(0) for _ in range(12)] if with_weight else []
    rows_ref, hidden_ref = (None, None) if with_weight else (refs.pop(0), refs.pop(0))
    out_ref = refs.pop(0)
    weight_out = refs.pop(0) if with_weight else None
    grad_w = None if with_weight else refs.pop(0)
    back += [refs.pop(0) for _ in range(2)] if with_weight else []
    kept, paired, x_half, x_full, y_half, y_full, from_up, from_down = refs[:8]
    send_sem, pair_sem, x_sem, y_sem, z_sem, load_sem, step_sem = refs[8:15]
    refs = refs[:8] + refs[9:]
    rows = out_ref.shape[0]
    half = rows // 2
    z, core, y, x = place()
    partner = device(z, 1 - core, y, x)
    x_next, y_next = device(z, core, y, 1 - x), device(z, core, 1 - y, x)
    up, down = device(z + 1, core, y, x), device(z - 1, core, y, x)
    greet(
        [
            (None, partner),
            (None, x_next),
            (None, y_next),
            (z < PLANES - 1, up),
            (z > 0, down),
        ]
    )
    sends = Sends(send_sem, partner)
    tables = ((3, 2, 1, 0), (3, 0, 2, 1), (0, 3, 1, 2), (0, 1, 2, 3))
    order = [
        sum((z == level).astype(jnp.int32) * tables[level][n] for level in range(PLANES))
        for n in range(PLANES)
    ]

    def plane_at(n):
        return sum((n == k).astype(jnp.int32) * order[k] for k in range(PLANES))

    spots = ((1 - y, 1 - x), (y, 1 - x), (1 - y, x), (y, x))

    def slot(plane, spot):
        return plane * 4 + spots[spot][0] * 2 + spots[spot][1]

    def block(plane, which, spot):
        size = pl.multiple_of(block_of(plane, which, *spots[spot]) * rows, rows)
        return part_ref.at[pl.ds(size, rows)]

    def load(plane, spot):
        return pltpu.make_async_copy(
            block(plane, core, spot), kept.at[slot(plane, spot)], load_sem.at[spot * 4 + plane]
        )

    for spot in range(4):
        for plane in order:
            where = slot(plane, spot)
            sends.send(block(plane, 1 - core, spot), paired.at[where], pair_sem.at[where], partner)
            load(plane, spot).start()
    if with_weight:
        out_pair, out_part, out_up, out_down, out_done = refs[14:19]
        out_pair_sem, out_sem = refs[19:21]
        out_half = weight_ref.shape[0] // 2
        out_block = out_half // LADDER
        big = out_half // 4

        def out_rows(n, which, count=1):
            start = pl.multiple_of(which * out_half + n * out_block, out_block)
            return weight_ref.at[pl.ds(start, out_block * count)]

        for n in range(4):
            sends.send(out_rows(n * PER, 1 - core, PER), out_pair.at[n], out_pair_sem.at[n], partner)

        def before(n):
            @pl.when(n % PER == 0)
            def _():
                where = n // PER
                sends.arrived(out_pair.at[where], out_pair_sem.at[where])
                add_into(out_part.at[where], (out_rows(n, core, PER), out_pair.at[where]), big)

        def done_rows(n, which):
            start = pl.multiple_of(which * out_half + n * out_block, out_block)
            return out_done.at[pl.ds(start, out_block)]

        ladder_step, closed, close = ladder(
            sends,
            LADDER,
            before,
            lambda n: out_part.at[
                n // PER, pl.ds(pl.multiple_of((n % PER) * out_block, out_block), out_block)
            ],
            lambda n: out_up.at[n],
            lambda n: out_down.at[n],
            done_rows,
            out_block,
            refs[21:27],
        )
        fill = backward_steps(back + refs[27:])

    else:
        rows_hold, hidden_hold, sums, part_sem, sum_sem = refs[14:]
        held = rows_hold.shape[2]

        def fetch(i):
            span = pl.ds(pl.multiple_of(i * held, held), held)
            return (
                pltpu.make_async_copy(
                    rows_ref.at[:, span], rows_hold.at[i % 2], part_sem.at[0, i % 2]
                ),
                pltpu.make_async_copy(
                    hidden_ref.at[:, span], hidden_hold.at[i % 2], part_sem.at[1, i % 2]
                ),
            )

        parts = rows_ref.shape[1] // held
        for copy in fetch(0):
            copy.start()

        sums[...] = jnp.zeros_like(sums)

        def add_product(i):
            @pl.when(i + 1 < parts)
            def _():
                for copy in fetch(i + 1):
                    copy.start()

            for copy in fetch(i):
                copy.wait()
            stripes = sums.shape[1] // 512

            @pl.loop(0, 3 * stripes)
            def _(n):
                matrix = n // stripes
                span = pl.ds(pl.multiple_of((n % stripes) * 512, 512), 512)
                sums[matrix, span] += mm(
                    rows_hold[i % 2, matrix // 2, :, span], hidden_hold[i % 2, matrix], (0, 0)
                )

        write_sums = pltpu.make_async_copy(sums, grad_w.at[0], sum_sem)

    def joined(plane, spot, more=()):
        where = slot(plane, spot)
        load(plane, spot).wait()
        sends.arrived(paired.at[where], pair_sem.at[where])
        add_rows(kept.at[where], (paired.at[where],) + tuple(more), rows)

    def across_copies(plane):
        source = kept.at[slot(plane, 0)]
        return (
            remote(
                source.at[pl.ds(0, half)],
                x_half.at[plane],
                step_sem.at[0, plane],
                x_sem.at[plane],
                x_next,
            ),
            remote(
                source.at[pl.ds(half, half)],
                y_half.at[plane],
                step_sem.at[1, plane],
                y_sem.at[plane],
                y_next,
            ),
        )

    def beside_copies(plane):
        return (
            remote(
                kept.at[slot(plane, 1)],
                x_full.at[plane],
                step_sem.at[2, plane],
                x_sem.at[4 + plane],
                x_next,
            ),
            remote(
                kept.at[slot(plane, 2)],
                y_full.at[plane],
                step_sem.at[3, plane],
                y_sem.at[4 + plane],
                y_next,
            ),
        )

    def across(plane):
        joined(plane, 0)
        for copy in across_copies(plane):
            copy.start()

    def beside(plane):
        along_x, along_y = beside_copies(plane)
        joined(plane, 1)
        sends.arrived(y_half.at[plane], y_sem.at[plane])
        add_rows(kept.at[slot(plane, 1)].at[pl.ds(half, half)], (y_half.at[plane],), half)
        along_x.start()
        joined(plane, 2)
        sends.arrived(x_half.at[plane], x_sem.at[plane])
        add_rows(kept.at[slot(plane, 2)].at[pl.ds(0, half)], (x_half.at[plane],), half)
        along_y.start()

    def along(plane):
        sends.arrived(x_full.at[plane], x_sem.at[4 + plane])
        sends.arrived(y_full.at[plane], y_sem.at[4 + plane])
        joined(plane, 3, (x_full.at[plane], y_full.at[plane]))

    def onward(plane):
        total = kept.at[slot(plane, 3)]
        return (
            remote(total, from_up.at[plane], step_sem.at[4, plane], z_sem.at[0, plane], down),
            remote(total, from_down.at[plane], step_sem.at[4, plane], z_sem.at[1, plane], up),
        )

    def pass_on(plane, first):
        total = kept.at[slot(plane, 3)]
        fall, rise = onward(plane)
        for copy, way, end, landing, sem in (
            (fall, z > plane, z == PLANES - 1, from_up.at[plane], z_sem.at[0, plane]),
            (rise, z < plane, z == 0, from_down.at[plane], z_sem.at[1, plane]),
        ):
            if first:
                pl.when(jnp.logical_and(way, end))(copy.start)
            else:

                @pl.when(jnp.logical_and(way, jnp.logical_not(end)))
                def _():
                    sends.arrived(landing, sem)
                    add_rows(total, (landing,), rows)
                    copy.start()

    if with_weight:
        fill[0]()
        share = (LADDER + LADDER_MORE) // (2 * PLANES)
    for late, run in enumerate((across, beside)):

        @pl.loop(0, PLANES)
        def _(n):
            run(plane_at(n))
            if with_weight:
                if not late:
                    fill[1](n)
                first = (late * PLANES + n) * share

                @pl.loop(0, share)
                def _(m):
                    ladder_step(first + m)
            else:
                add_product(late * PLANES + n)

    if not with_weight:
        write_sums.start()

    @pl.loop(0, PLANES)
    def _(n):
        plane = plane_at(n)
        along(plane)

        @pl.when(n < PLANES - 1)
        def _():
            pass_on(plane, True)

        @pl.when(n > 0)
        def _():
            pass_on(plane_at(n - 1), False)

        if with_weight:
            fill[1](PLANES + n)

    if with_weight:
        fill[-1]()
    mine = kept.at[slot(z, 3)]

    @pl.when(z < PLANES - 1)
    def _():
        sends.arrived(from_up.at[z], z_sem.at[0, z])
        add_rows(mine, (from_up.at[z],), rows)

    @pl.when(z > 0)
    def _():
        sends.arrived(from_down.at[z], z_sem.at[1, z])
        add_rows(mine, (from_down.at[z],), rows)

    out_ref[...] = mine[...]
    if with_weight:

        @pl.loop(0, LADDER)
        def _(n):
            closed(n)

        write = pltpu.make_async_copy(out_done, weight_out, out_sem)
        write.start()
        close()
        write.wait()
    else:
        write_sums.wait()

    @pl.loop(0, PLANES)
    def _(plane):
        for copy in across_copies(plane) + beside_copies(plane):
            copy.wait_send()
        pl.when(plane != z)(onward(plane)[0].wait_send)

    sends.finish()


def reduce_all(part, collective_id, weight=None, back=(), expert=()):
    total, width = part.shape
    rows = total // 32
    half = rows // 2
    dtype = part.dtype
    out_shape = [jax.ShapeDtypeStruct((rows, width), dtype)]
    in_specs = [pl.BlockSpec(memory_space=pltpu.HBM)]
    out_specs = [pl.BlockSpec(memory_space=pltpu.VMEM)]
    scratch = [
        pltpu.VMEM((16, rows, width), dtype),
        pltpu.VMEM((16, rows, width), dtype),
        pltpu.VMEM((4, half, width), dtype),
        pltpu.VMEM((4, rows, width), dtype),
        pltpu.VMEM((4, half, width), dtype),
        pltpu.VMEM((4, rows, width), dtype),
        pltpu.VMEM((4, rows, width), dtype),
        pltpu.VMEM((4, rows, width), dtype),
        pltpu.SemaphoreType.DMA((20,)),
        pltpu.SemaphoreType.DMA((16,)),
        pltpu.SemaphoreType.DMA((8,)),
        pltpu.SemaphoreType.DMA((8,)),
        pltpu.SemaphoreType.DMA((2, 4)),
        pltpu.SemaphoreType.DMA((16,)),
        pltpu.SemaphoreType.DMA((5, 4)),
    ]
    operands = [part]
    if weight is not None:
        operands.append(weight)
        block = weight.shape[0] // 8
        seq = back[0].shape[0]
        operands += back
        out_shape += [
            jax.ShapeDtypeStruct(weight.shape, dtype),
            jax.ShapeDtypeStruct(back[3].shape, dtype),
            jax.ShapeDtypeStruct((8, HEAD_SIZE), jnp.float32),
        ]
        in_specs += [pl.BlockSpec(memory_space=pltpu.VMEM)] * (1 + len(back))
        out_specs += [
            pl.BlockSpec(memory_space=pltpu.HBM),
            pl.BlockSpec(memory_space=pltpu.VMEM),
            pl.BlockSpec(memory_space=pltpu.VMEM),
        ]
        scratch += [
            pltpu.VMEM((4, block, width), dtype),
            pltpu.VMEM((4, block, width), dtype),
            pltpu.VMEM((LADDER, weight.shape[0] // 2 // LADDER, width), dtype),
            pltpu.VMEM((LADDER, weight.shape[0] // 2 // LADDER, width), dtype),
            pltpu.VMEM(weight.shape, dtype),
            pltpu.SemaphoreType.DMA((4,)),
            pltpu.SemaphoreType.DMA,
        ] + ladder_scratch(LADDER)
        scratch += [
            pltpu.VMEM((seq, seq), jnp.float32),
            pltpu.VMEM((seq, HEAD_SIZE), jnp.float32),
            pltpu.VMEM((seq, HEAD_SIZE), jnp.float32),
        ]
    else:
        rows_held, hidden_held = expert
        held, ff = rows_held.shape[1] // 8, hidden_held.shape[2]
        operands += expert
        in_specs += [pl.BlockSpec(memory_space=pltpu.HBM)] * 2
        out_shape.append(jax.ShapeDtypeStruct((1, 3, width, ff), jnp.float32))
        out_specs.append(pl.BlockSpec(memory_space=pltpu.HBM))
        scratch += [
            pltpu.VMEM((2, 2, held, width), dtype),
            pltpu.VMEM((2, 3, held, ff), dtype),
            pltpu.VMEM((3, width, ff), jnp.float32),
            pltpu.SemaphoreType.DMA((2, 2)),
            pltpu.SemaphoreType.DMA,
        ]
    return pl.pallas_call(
        functools.partial(reduce_kernel, weight is not None),
        out_shape=out_shape,
        in_specs=in_specs,
        out_specs=out_specs,
        scratch_shapes=scratch,
        compiler_params=pltpu.CompilerParams(
            collective_id=collective_id, has_side_effects=True, vmem_limit_bytes=63 << 20
        ),
        name="reduce_all",
    )(*operands)


def others():
    z, core, y, x = place()
    return [
        (device(z, core, yy, xx), yy * 2 + xx)
        for yy, xx in ((y, 1 - x), (1 - y, x), (1 - y, 1 - x))
    ]


def remote(source, landing, send_sem, recv_sem, target):
    return pltpu.make_async_remote_copy(
        src_ref=source,
        dst_ref=landing,
        send_sem=send_sem,
        recv_sem=recv_sem,
        device_id=target,
        device_id_type=MESH_ID,
    )


def start_kernel(
    x_ref, w_ref, x_all, w_own, hold, send_sem, x_sem, w_sem, pair_sem, own_sem
):
    tok = x_ref.shape[0]
    depth = w_ref.shape[0]
    half = depth // 2
    z, core, y, x = place()
    me = y * 2 + x
    partner = device(z, 1 - core, y, x)
    near = others()
    greet([(None, target) for target, _ in near] + [(None, partner)])
    parts = QUERY_HEADS // 4 * HEAD_SIZE
    single = HEAD_SIZE
    widths = (
        (0, parts, 0),
        (QUERY_HEADS * HEAD_SIZE, single, parts),
        ((QUERY_HEADS + KEY_VALUE_HEADS) * HEAD_SIZE, single, parts + single),
    )

    def columns(piece, who):
        base, width, _ = widths[piece]
        return pl.ds(pl.multiple_of(base + who * width, 128), width)

    def landing(piece, who, part, ref=w_own):
        _, width, offset = widths[piece]
        rows = pl.ds(pl.multiple_of(who * depth + part * half, half), half)
        return ref.at[rows, pl.ds(offset, width)]

    sends = []
    for slot, (target, who) in enumerate(near):
        for piece in range(3):
            copy = remote(
                w_ref.at[pl.ds(pl.multiple_of(core * half, half), half), columns(piece, who)],
                landing(piece, me, core),
                send_sem.at[slot * 4 + piece],
                w_sem.at[slot * 3 + piece],
                target,
            )
            copy.start()
            sends.append(copy)
        copy = remote(
            x_ref,
            x_all.at[pl.ds(pl.multiple_of(me * tok, tok), tok)],
            send_sem.at[slot * 4 + 3],
            x_sem.at[slot],
            target,
        )
        copy.start()
        sends.append(copy)
    mine = pltpu.make_async_copy(
        x_ref, x_all.at[pl.ds(pl.multiple_of(me * tok, tok), tok)], own_sem.at[0]
    )
    mine.start()
    loads = []
    for piece in range(3):
        _, width, offset = widths[piece]
        loads.append(
            pltpu.make_async_copy(
                w_ref.at[:, columns(piece, me)], hold.at[:, pl.ds(offset, width)], own_sem.at[1 + piece]
            )
        )
        loads[-1].start()
    for copy in loads:
        copy.wait()
    keep = pltpu.make_async_copy(
        hold, w_own.at[pl.ds(pl.multiple_of(me * depth, depth), depth)], own_sem.at[4]
    )
    keep.start()
    for slot, (target, who) in enumerate(near):
        for piece in range(3):
            where = landing(piece, who, core)
            remote(where, where, send_sem.at[0], w_sem.at[slot * 3 + piece], partner).wait_recv()
        rows = w_own.at[pl.ds(pl.multiple_of(who * depth + core * half, half), half)]
        copy = remote(rows, rows, send_sem.at[12 + slot], pair_sem.at[slot], partner)
        copy.start()
        sends.append(copy)
    for slot, (target, who) in enumerate(near):
        rows = w_own.at[pl.ds(pl.multiple_of(who * depth + (1 - core) * half, half), half)]
        remote(rows, rows, send_sem.at[0], pair_sem.at[slot], partner).wait_recv()
        rows = x_all.at[pl.ds(pl.multiple_of(who * tok, tok), tok)]
        remote(rows, rows, send_sem.at[0], x_sem.at[slot], partner).wait_recv()
    mine.wait()
    keep.wait()
    for copy in sends:
        copy.wait_send()


def start_exchange(block_in, weight, collective_id):
    tok, width = block_in.shape
    depth, columns = weight.shape
    return pl.pallas_call(
        start_kernel,
        out_shape=[
            jax.ShapeDtypeStruct((tok * 4, width), block_in.dtype),
            jax.ShapeDtypeStruct((depth * 4, columns // 4), weight.dtype),
        ],
        in_specs=[
            pl.BlockSpec(memory_space=pltpu.VMEM),
            pl.BlockSpec(memory_space=pltpu.HBM),
        ],
        out_specs=[pl.BlockSpec(memory_space=pltpu.HBM)] * 2,
        scratch_shapes=[
            pltpu.VMEM((depth, columns // 4), weight.dtype),
            pltpu.SemaphoreType.DMA((16,)),
            pltpu.SemaphoreType.DMA((3,)),
            pltpu.SemaphoreType.DMA((9,)),
            pltpu.SemaphoreType.DMA((3,)),
            pltpu.SemaphoreType.DMA((5,)),
        ],
        compiler_params=pltpu.CompilerParams(
            collective_id=collective_id, has_side_effects=True, vmem_limit_bytes=40 << 20
        ),
        name="start_exchange",
    )(block_in, weight)


def spread_kernel(x_ref, x_all, send_sem, x_sem, own_sem):
    tok = x_ref.shape[0]
    z, core, y, x = place()
    me = y * 2 + x
    near = others()
    greet([(None, target) for target, _ in near[:2]])
    sends = Sends(send_sem, near[0][0])

    def rows(who, part=None):
        if part is None:
            return x_all.at[pl.ds(pl.multiple_of(who * tok, tok), tok)]
        start = who * tok + part * (tok // 2)
        return x_all.at[pl.ds(pl.multiple_of(start, tok // 2), tok // 2)]

    for slot in range(2):
        for part in (1 - slot, slot):
            sends.send(
                x_ref.at[pl.ds(part * (tok // 2), tok // 2)],
                rows(me, part),
                x_sem.at[slot, part],
                near[slot][0],
            )
    own_x = pltpu.make_async_copy(x_ref, rows(me), own_sem)
    own_x.start()
    for slot in range(2):
        who, part = near[slot][1], 1 - slot
        sends.arrived(rows(who, part), x_sem.at[slot, part])
        sends.send(rows(who, part), rows(who, part), x_sem.at[2, part], near[1 - slot][0])
    for slot in range(2):
        sends.arrived(rows(near[slot][1], slot), x_sem.at[slot, slot])
    for part in range(2):
        sends.arrived(rows(near[2][1], part), x_sem.at[2, part])
    own_x.wait()
    sends.finish()


def spread_sequence(rows, collective_id):
    tok, width = rows.shape
    return pl.pallas_call(
        spread_kernel,
        out_shape=jax.ShapeDtypeStruct((tok * 4, width), rows.dtype),
        in_specs=[pl.BlockSpec(memory_space=pltpu.VMEM)],
        out_specs=pl.BlockSpec(memory_space=pltpu.HBM),
        scratch_shapes=[
            pltpu.SemaphoreType.DMA((6,)),
            pltpu.SemaphoreType.DMA((3, 2)),
            pltpu.SemaphoreType.DMA,
        ],
        compiler_params=pltpu.CompilerParams(
            collective_id=collective_id, has_side_effects=True, vmem_limit_bytes=40 << 20
        ),
        name="spread_sequence",
    )(rows)


def fold_kernel(part_ref, out_ref, across, beside, summed, send_sem, recv_sem):
    tok = out_ref.shape[0]
    half = tok // 2
    z, core, y, x = place()
    me = y * 2 + x
    near = others()
    greet([(None, target) for target, _ in near[:2]])
    sends = Sends(send_sem, near[0][0])

    def rows(who, part):
        start = who * tok + part * half
        return part_ref.at[pl.ds(pl.multiple_of(start, half), half)]

    def landing(slot, part):
        return beside.at[slot, pl.ds(part * half, half)]

    for slot in range(2):
        sends.send(rows(near[2][1], slot), across.at[slot], recv_sem.at[0, slot], near[slot][0])
    for slot in range(2):
        sends.send(
            rows(near[slot][1], slot), landing(slot, slot), recv_sem.at[1, slot], near[slot][0]
        )
    for slot in range(2):
        part = 1 - slot
        sends.arrived(across.at[part], recv_sem.at[0, part])
        add_into(summed.at[slot], (rows(near[slot][1], part), across.at[part]), half)
        sends.send(summed.at[slot], landing(slot, part), recv_sem.at[2, slot], near[slot][0])
    for slot in range(2):
        sends.arrived(landing(slot, slot), recv_sem.at[1, slot])
        sends.arrived(landing(slot, 1 - slot), recv_sem.at[2, slot])
    own = part_ref.at[pl.ds(pl.multiple_of(me * tok, tok), tok)]
    add_into(out_ref, (own, beside.at[0], beside.at[1]), tok)
    sends.finish()


def fold_sequence(part, collective_id):
    total, width = part.shape
    tok = total // 4
    return pl.pallas_call(
        fold_kernel,
        out_shape=jax.ShapeDtypeStruct((tok, width), jnp.float32),
        in_specs=[pl.BlockSpec(memory_space=pltpu.VMEM)],
        out_specs=pl.BlockSpec(memory_space=pltpu.VMEM),
        scratch_shapes=[
            pltpu.VMEM((2, tok // 2, width), part.dtype),
            pltpu.VMEM((2, tok, width), part.dtype),
            pltpu.VMEM((2, tok // 2, width), part.dtype),
            pltpu.SemaphoreType.DMA((6,)),
            pltpu.SemaphoreType.DMA((3, 2)),
        ],
        compiler_params=pltpu.CompilerParams(
            collective_id=collective_id, has_side_effects=True, vmem_limit_bytes=40 << 20
        ),
        name="fold_sequence",
    )(part)


def weight_kernel(
    grad_ref,
    fold_ref,
    out_ref,
    fold_out,
    pair,
    part,
    landed,
    from_up,
    from_down,
    done,
    folds,
    send_sem,
    pair_sem,
    cross_sem,
    fold_sem,
    write_sem,
    *ladder_sems,
):
    depth = done.shape[1]
    half = depth // 2
    block = half // PER
    tok = fold_out.shape[0]
    z, core, y, x = place()
    me = y * 2 + x
    partner = device(z, 1 - core, y, x)
    up, down = device(z + 1, core, y, x), device(z - 1, core, y, x)
    near = [(device(z, core, y, x), me)] + others()
    greet(
        [(None, partner)]
        + [(None, target) for target, _ in near[1:]]
        + [(z < PLANES - 1, up), (z > 0, down)]
    )
    sends = Sends(send_sem, partner)

    def own_rows(n, which):
        start = pl.multiple_of(near[n][1] * depth + which * half, half)
        return grad_ref.at[pl.ds(start, half)]

    for n in range(4):
        sends.send(own_rows(n, 1 - core), pair.at[n], pair_sem.at[n], partner)
    for n in range(4):
        sends.arrived(pair.at[n], pair_sem.at[n])
        target = part.at[n - 1] if n else landed.at[0]
        add_into(target, (own_rows(n, core), pair.at[n]), half)
        if n:
            sends.send(target, landed.at[n], cross_sem.at[n - 1], near[n][0])
    for n in (1, 2, 3):
        target, who = near[n]
        rows = fold_ref.at[pl.ds(pl.multiple_of(who * tok, tok), tok)]
        sends.send(rows, folds.at[n - 1], fold_sem.at[n - 1], target)

    def before(n):
        @pl.when(jnp.logical_and(n % PER == 0, n > 0))
        def _():
            sends.arrived(landed.at[n // PER], cross_sem.at[n // PER - 1])

    def done_rows(n, which):
        source = n // PER
        who = ((y + source // 2) % 2) * 2 + (x + source % 2) % 2
        start = pl.multiple_of(which * half + (n % PER) * block, block)
        return done.at[who, pl.ds(start, block)]

    ladder_step, closed, close = ladder(
        sends,
        LADDER,
        before,
        lambda n: landed.at[n // PER, pl.ds(pl.multiple_of((n % PER) * block, block), block)],
        lambda n: from_up.at[n],
        lambda n: from_down.at[n],
        done_rows,
        block,
        ladder_sems,
    )

    @pl.loop(0, LADDER + LADDER_MORE)
    def _(m):
        ladder_step(m)

    for n in range(3):
        sends.arrived(folds.at[n], fold_sem.at[n])
    add_into(
        fold_out,
        [fold_ref.at[pl.ds(pl.multiple_of(me * tok, tok), tok)]] + [folds.at[n] for n in range(3)],
        tok,
    )
    single = HEAD_SIZE
    heads = QUERY_HEADS // 4 * HEAD_SIZE
    writes = []
    for n in range(4):
        pl.loop(n * PER, (n + 1) * PER)(closed)
        who = near[n][1]
        for c, (base, width, offset) in enumerate(
            (
                (0, heads, 0),
                (QUERY_HEADS * HEAD_SIZE, single, heads),
                ((QUERY_HEADS + KEY_VALUE_HEADS) * HEAD_SIZE, single, heads + single),
            )
        ):
            copy = pltpu.make_async_copy(
                done.at[who, :, pl.ds(offset, width)],
                out_ref.at[:, pl.ds(pl.multiple_of(base + who * width, 128), width)],
                write_sem.at[n * 3 + c],
            )
            copy.start()
            writes.append(copy)
    close()
    for copy in writes:
        copy.wait()
    sends.finish()


def weight_reduce(grad, fold, collective_id):
    rows, columns = grad.shape
    depth = rows // 4
    half = depth // 2
    tok, width = fold.shape[0] // 4, fold.shape[1]
    dtype = grad.dtype
    return pl.pallas_call(
        weight_kernel,
        out_shape=[
            jax.ShapeDtypeStruct((depth, columns * 4), dtype),
            jax.ShapeDtypeStruct((tok, width), jnp.float32),
        ],
        in_specs=[pl.BlockSpec(memory_space=pltpu.VMEM)] * 2,
        out_specs=[pl.BlockSpec(memory_space=pltpu.HBM), pl.BlockSpec(memory_space=pltpu.VMEM)],
        scratch_shapes=[
            pltpu.VMEM((4, half, columns), dtype),
            pltpu.VMEM((3, half, columns), dtype),
            pltpu.VMEM((4, half, columns), dtype),
            pltpu.VMEM((LADDER, half // PER, columns), dtype),
            pltpu.VMEM((LADDER, half // PER, columns), dtype),
            pltpu.VMEM((4, depth, columns), dtype),
            pltpu.VMEM((3, tok, width), dtype),
            pltpu.SemaphoreType.DMA((10,)),
            pltpu.SemaphoreType.DMA((4,)),
            pltpu.SemaphoreType.DMA((3,)),
            pltpu.SemaphoreType.DMA((3,)),
            pltpu.SemaphoreType.DMA((12,)),
        ]
        + ladder_scratch(LADDER),
        compiler_params=pltpu.CompilerParams(
            collective_id=collective_id, has_side_effects=True, vmem_limit_bytes=56 << 20
        ),
        name="weight_reduce",
    )(grad, fold)


def project_back_kernel(
    grad_ref,
    weight_ref,
    normed_ref,
    x_ref,
    experts_ref,
    part_ref,
    grad_weight_ref,
    gain_ref,
    experts_out,
    inverse,
    ring,
    load_sem,
    store_sem,
):
    stripes = x_ref.shape[1] // 256
    chunk = ring.shape[1]
    slots = ring.shape[0]
    each = experts_ref.shape[2] // chunk
    chunks = 3 * each
    per = chunks // stripes

    def rows(ref, c):
        return ref.at[0, c // each, pl.ds(pl.multiple_of((c % each) * chunk, chunk), chunk)]

    def load(c):
        return pltpu.make_async_copy(
            rows(experts_ref, c), ring.at[c % slots], load_sem.at[c % slots]
        )

    def store(c):
        return pltpu.make_async_copy(
            ring.at[c % slots], rows(experts_out, c), store_sem.at[c % slots]
        )

    for c in range(slots):
        load(c).start()

    @pl.loop(0, x_ref.shape[0] // 64)
    def _(n):
        span = pl.ds(pl.multiple_of(n * 64, 64), 64)
        inverse[span] = inverse_rms(x_ref[span].astype(jnp.float32))

    @pl.loop(0, stripes)
    def _(i):
        for k in range(per):
            load(i * per + k).wait()
            store(i * per + k).start()
        span = pl.ds(pl.multiple_of(i * 256, 256), 256)
        part = mm(grad_ref[...], weight_ref[span], (1, 1))
        part_ref[:, span] = part.astype(jnp.bfloat16)
        scaled = part * x_ref[:, span].astype(jnp.float32) * inverse[...]
        gain_ref[:, span] = jnp.sum(scaled, axis=0, keepdims=True)
        grad_weight_ref[span] = mm(normed_ref[:, span], grad_ref[...], (0, 0)).astype(jnp.bfloat16)
        for k in range(per):
            store(i * per + k).wait()

            @pl.when(i * per + k + slots < chunks)
            def _():
                load(i * per + k + slots).start()


def project_back(grad, weight, normed, x, experts):
    seq, width = x.shape
    bf, f4 = jnp.bfloat16, jnp.float32
    return pl.pallas_call(
        project_back_kernel,
        out_shape=[
            jax.ShapeDtypeStruct((seq, width), bf),
            jax.ShapeDtypeStruct(weight.shape, bf),
            jax.ShapeDtypeStruct((1, width), f4),
            jax.ShapeDtypeStruct(experts.shape, f4),
        ],
        in_specs=[pl.BlockSpec(memory_space=pltpu.VMEM)] * 4
        + [pl.BlockSpec(memory_space=pltpu.HBM)],
        out_specs=[pl.BlockSpec(memory_space=pltpu.VMEM)] * 3
        + [pl.BlockSpec(memory_space=pltpu.HBM)],
        scratch_shapes=[
            pltpu.VMEM((seq, 1), f4),
            pltpu.VMEM((6, 256, experts.shape[3]), f4),
            pltpu.SemaphoreType.DMA((6,)),
            pltpu.SemaphoreType.DMA((6,)),
        ],
        compiler_params=pltpu.CompilerParams(vmem_limit_bytes=48 << 20),
        name="project_back",
    )(grad, weight, normed, x, experts)


def split_body(
    block_in,
    segments,
    routes,
    attn_gain,
    query_key_value_weight,
    q_gain,
    k_gain,
    w_out,
    ffn_gain,
    router,
    expert_weights,
    cotangent,
):
    tok, width = block_in.shape
    seq = segments.shape[0]
    experts = router.shape[1]
    capacity = tok * routes.shape[1] * 2 // experts
    heads = QUERY_HEADS // 4
    both = ("rep", "shard")
    upstream_all = lax.all_gather(cotangent, both, axis=0, tiled=True)
    x_all, weight = start_exchange(block_in, query_key_value_weight, 0)

    mask = jnp.any(
        routes[:, :, None] == jnp.arange(experts, dtype=jnp.int32)[None, None, :], axis=1
    )
    mask_f = mask.astype(jnp.float32)
    earlier = (jnp.arange(tok)[:, None] > jnp.arange(tok)[None, :]).astype(jnp.bfloat16)
    slot = jnp.dot(earlier, mask.astype(jnp.bfloat16), preferred_element_type=jnp.float32)
    slot_table = jnp.where(mask, slot, -4096.0).T

    cosine, sine = rope_tables(jnp.arange(seq, dtype=jnp.int32))
    cosine = cosine[:, 0]
    sine = sine[:, 0] * jnp.where(jnp.arange(HEAD_SIZE) < HEAD_SIZE // 2, -1.0, 1.0)
    normed_one, raw, q_rot, k_rot, values, attended, lse, partial = attend(
        x_all, weight, w_out, attn_gain, q_gain, k_gain, cosine, sine, segments
    )
    inputs = block_in.astype(jnp.float32)
    middle = inputs + fold_sequence(partial, 1)
    scale_two = rms_scale(middle)
    normed_two = (middle * scale_two * ffn_gain).astype(jnp.bfloat16)
    logits = jnp.dot(normed_two, router, preferred_element_type=jnp.float32)
    weights = jax.nn.softmax(logits, axis=-1)
    picked = weights * mask_f
    total = jnp.sum(picked, axis=1, keepdims=True)
    gates = picked / total
    table = jnp.concatenate([gates.T, slot_table], axis=0)
    tokens_all, _, out_part, grad_part, gate_part, rows_held, hidden_held = run_experts(
        normed_two, table, upstream_all, expert_weights, capacity, 2
    )
    grad_gates = lax.all_to_all(gate_part, both, split_axis=0, concat_axis=0, tiled=True).T
    grad_from_experts, grad_experts = reduce_all(grad_part, 3, expert=[rows_held, hidden_held])
    grad_from_experts = grad_from_experts.astype(jnp.float32)

    upstream = cotangent.astype(jnp.float32)
    grad_picked = grad_gates / total - jnp.sum(grad_gates * picked, axis=1, keepdims=True) / (
        total * total
    )
    grad_weights = grad_picked * mask_f
    grad_logits = weights * (grad_weights - jnp.sum(grad_weights * weights, axis=1, keepdims=True))
    grad_from_router = jnp.dot(
        grad_logits, router.astype(jnp.float32).T, precision=lax.Precision.HIGHEST
    )
    grad_norm_two, grad_ffn_gain = rms_back(
        middle, scale_two, ffn_gain, grad_from_experts + grad_from_router
    )
    grad_middle = upstream + grad_norm_two
    grad_middle_all = spread_sequence(grad_middle.astype(jnp.bfloat16), 5)
    grad_out = lax.dot_general(
        attended, grad_middle_all, (((0,), (0,)), ((), ())), preferred_element_type=jnp.float32
    ).astype(jnp.bfloat16)
    grad_attended = jnp.dot(
        grad_middle_all, w_out.T, preferred_element_type=jnp.float32
    ).astype(jnp.bfloat16)
    expert_sum, grad_out, grad_qkv_b, grad_gains = reduce_all(
        out_part,
        4,
        grad_out,
        [
            q_rot,
            k_rot,
            values,
            raw,
            grad_attended,
            lse,
            q_gain[None],
            k_gain[None],
            cosine,
            sine,
            segments[:, None],
            segments[None],
        ],
    )
    block_out = (middle + expert_sum.astype(jnp.float32)).astype(jnp.bfloat16)
    grad_out = grad_out.astype(jnp.float32)
    grad_q_gain, grad_k_gain = grad_gains[0], grad_gains[1]
    norm_part, grad_weight, grad_attn_gain, grad_experts = project_back(
        grad_qkv_b, weight, normed_one, x_all, grad_experts
    )
    grad_attn_gain = grad_attn_gain[0]
    gains = jnp.concatenate([grad_attn_gain, grad_ffn_gain, grad_q_gain, grad_k_gain])
    lines = gains.shape[0] // tok
    spare = -(lines + experts) % 16
    small = jnp.concatenate(
        [grad_logits.T, gains.reshape(lines, tok), jnp.zeros((spare, tok), jnp.float32)], axis=0
    )
    small_all = lax.all_gather(small, both)
    grad_qkv, grad_norm_one = weight_reduce(grad_weight, norm_part, 7)
    grad_qkv = grad_qkv.astype(jnp.float32)
    grad_inputs, _ = rms_back(inputs, rms_scale(inputs), attn_gain, grad_norm_one)
    grad_input = (grad_middle + grad_inputs).astype(jnp.bfloat16)
    gains = jnp.sum(small_all[:, experts : experts + lines], axis=0).reshape(-1)
    grad_attn_gain, grad_ffn_gain, grad_q_gain, grad_k_gain = jnp.split(
        gains, (width, 2 * width, 2 * width + HEAD_SIZE)
    )
    logits_all = small_all[:, :experts].transpose(1, 0, 2).reshape(experts, -1)
    high = lax.reduce_precision(logits_all, 8, 7)
    middle_part = lax.reduce_precision(logits_all - high, 8, 7)
    low = logits_all - high - middle_part
    pieces = jnp.concatenate([high, middle_part, low], axis=0).astype(jnp.bfloat16)
    pieces = jnp.dot(pieces, tokens_all, preferred_element_type=jnp.float32)
    grad_router = jnp.sum(pieces.reshape(3, experts, width), axis=0).T
    return (
        block_out,
        grad_input,
        grad_attn_gain,
        grad_qkv,
        grad_q_gain,
        grad_k_gain,
        grad_out,
        grad_ffn_gain,
        grad_router,
        grad_experts,
    )


def solution(mesh):
    placed = (
        P(("rep", "shard"), None),
        P("rep"),
        P(("rep", "shard"), None),
        P(),
        P("shard", None),
        P(),
        P(),
        P("shard", None),
        P(),
        P(),
        P(("rep", "shard"), None, None, None),
        P(("rep", "shard"), None),
    )
    body = split_body if dict(mesh.shape) == {"rep": 8, "shard": 4} else plain_body
    return jax.shard_map(
        body,
        mesh=mesh,
        in_specs=placed,
        out_specs=(
            P(("rep", "shard"), None),
            P(("rep", "shard"), None),
            P(),
            P("shard", None),
            P(),
            P(),
            P("shard", None),
            P(),
            P(),
            P(("rep", "shard"), None, None, None),
        ),
        check_vma=False,
    )
```
